32 devices in a mesh: dp: 16 (over z, y, x), tensor: 2 (over core).
Axes of the slice: x: 2, y: 2, z: 4, core: 2. Of those that a mesh axis runs over, the one named last changes fastest.
Arguments:
- tokens: bfloat16 [16384, 768], P(('dp', 'tensor')), may hold values from -6 to 6
- lengths: int32 [16], P('dp'), may hold values from 256 to 1024, as said below
- qkv_weight: bfloat16 [3, 768, 768], P(None, 'dp', 'tensor'), may hold values from -0.21875 to 0.21875
- qv_bias: bfloat16 [2, 768], P(None, ('tensor', 'dp')), may hold values from -3 to 3
- out_weight: bfloat16 [768, 768], P('tensor', 'dp'), may hold values from -0.4375 to 0.4375
- in_weight: bfloat16 [2, 768, 3072], P(None, 'dp', 'tensor'), may hold values from -0.21875 to 0.21875
- in_bias: bfloat16 [2, 3072], P(None, ('tensor', 'dp')), may hold values from -3 to 3
- down_weight: bfloat16 [3072, 768], P('tensor', 'dp'), may hold values from -0.21875 to 0.21875
- norm_gains: float32 [2, 768], P(None, ('dp', 'tensor')), may hold values from 0.1 to 1.9
- offsets: float32 [4, 768], P(None, ('dp', 'tensor')), may hold values from -3 to 3
- cotangent: bfloat16 [16384, 768], P(('dp', 'tensor')), may hold values from -6 to 6
Outputs:
- output: bfloat16 [16384, 768], P(('dp', 'tensor'))
- grad_tokens: float32 [16384, 768], P(('dp', 'tensor'))
- grad_qkv_weight: float32 [3, 768, 768], P(None, 'dp', 'tensor')
- grad_qv_bias: float32 [2, 768], P(None, ('tensor', 'dp'))
- grad_out_weight: float32 [768, 768], P('tensor', 'dp')
- grad_in_weight: float32 [2, 768, 3072], P(None, 'dp', 'tensor')
- grad_in_bias: float32 [2, 3072], P(None, ('tensor', 'dp'))
- grad_down_weight: float32 [3072, 768], P('tensor', 'dp')
- grad_norm_gains: float32 [2, 768], P(None, ('dp', 'tensor'))
- grad_offsets: float32 [4, 768], P(None, ('dp', 'tensor'))
The draws below stay inside these ranges and needn't reach their ends.
Inputs may be any that keep to these rules, and one draw needn't show every extreme that they name: `lengths`: the number of valid leading slots of each sequence; some sequence is full and some holds exactly 256.
All inputs are finite; a program needn't handle non-finite values.
Results may differ from the reference program's by a relative error of at most 0.02.
Values may be sent and summed in bfloat16 or wider, within the bound.
A program may use at most 128 MiB of HBM per device.

```python
import jax
import jax.numpy as jnp
from jax import lax

HEADS = 12
HEAD = 64
D = 768
FF = 3072
SEQ = 1024
SEQS = 16
TOKENS = 16384


def draw_lengths(key, part):
    seq_count = SEQS
    drawn = jax.random.randint(jax.random.fold_in(key, 1), (seq_count,), SEQ // 4, SEQ + 1)
    chosen = jax.random.randint(jax.random.fold_in(key, 2), (), 0, seq_count)
    second_pick = (chosen + 1 + jax.random.randint(jax.random.fold_in(key, 3), (), 0, seq_count - 1)) % seq_count
    indices = jnp.arange(seq_count, dtype=jnp.int32)
    drawn = jnp.where(indices == chosen, SEQ, drawn)
    drawn = jnp.where(indices == second_pick, SEQ // 4, drawn)
    return drawn.astype(jnp.int32)


def level_of(key, dims, pieces, low, top_value):
    level = 1.0
    for axis_at, shards_of in pieces:
        steps = jax.random.uniform(jax.random.fold_in(jax.random.fold_in(key, 6), axis_at), (shards_of,), jnp.float32, low / len(pieces), top_value / len(pieces))
        level = level * jnp.repeat(jnp.exp(steps), dims[axis_at] // shards_of).reshape((-1,) + (1,) * (len(dims) - 1 - axis_at))
    return level


def bell_draw(own_key, dims, scale, most, shards=(), kind=jnp.bfloat16):
    level = level_of(own_key, dims, shards, -0.22, 0.18) if shards else 1.0
    entries = jax.random.normal(own_key, dims, jnp.float32) * scale * level
    return jnp.minimum(jnp.maximum(entries, -most), most).astype(kind)


def setup_inputs(seed: int = 0) -> dict:
    seeds = jax.random.split(jax.random.key(seed), 12)
    tokens = bell_draw(seeds[0], (TOKENS, D), 1.0, 6.0, ((0, 32),))
    lengths = draw_lengths(jax.random.fold_in(seeds[11], 71), 0)
    qkv_weight = bell_draw(seeds[2], (3, D, D), D ** -0.5, 0.21875, ((1, 16), (2, 2)))
    qv_bias = bell_draw(seeds[3], (2, D), 0.5, 3.0, ((1, 32),))
    out_weight = bell_draw(seeds[4], (D, D), (D // 4) ** -0.5, 0.4375, ((0, 2), (1, 16)))
    in_weight = bell_draw(seeds[5], (2, D, FF), D ** -0.5, 0.21875, ((1, 16), (2, 2)))
    in_bias = bell_draw(seeds[6], (2, FF), 0.5, 3.0, ((1, 32),))
    down_weight = bell_draw(seeds[7], (FF, D), (FF // 4) ** -0.5, 0.21875, ((0, 2), (1, 16)))
    norm_gains = jnp.clip(1.0 + 0.18 * jax.random.normal(seeds[8], (2, D), jnp.float32), 0.1, 1.9)
    offsets = bell_draw(seeds[9], (4, D), 0.5, 3.0, ((1, 32),), jnp.float32)
    cotangent = bell_draw(seeds[10], (TOKENS, D), 1.0, 6.0, ((0, 32),))
    return dict(tokens=tokens, lengths=lengths, qkv_weight=qkv_weight, qv_bias=qv_bias, out_weight=out_weight, in_weight=in_weight, in_bias=in_bias, down_weight=down_weight, norm_gains=norm_gains, offsets=offsets, cotangent=cotangent)


highest = lax.Precision.HIGHEST
norm_epsilon = 1e-06

@jax.custom_vjp
def low(v):
    return lax.optimization_barrier(v.astype(jnp.bfloat16)).astype(jnp.float32)

@jax.custom_vjp
def low_back(v):
    return v

def low_keep(v):
    return (low(v), None)

def low_pass(kept, grad):
    return (grad,)

def back_keep(v):
    return (v, None)

def back_low(kept, grad):
    return (low(grad),)
low.defvjp(low_keep, low_pass)
low_back.defvjp(back_keep, back_low)

def layer_norm(values, gain_row, shift_row):
    centred = values - lax.optimization_barrier(jnp.mean(values, axis=-1, keepdims=True))
    variance = lax.optimization_barrier(jnp.mean(centred * centred, axis=-1, keepdims=True))
    return centred * lax.rsqrt(variance + norm_epsilon) * gain_row + shift_row

def forward_sequence(params, inputs, length):
    qkv_weight, qv_bias, out_weight, in_weight, in_bias, down_weight, norm_gains, offsets = params
    slot_count = inputs.shape[0]
    positions = jnp.arange(slot_count, dtype=jnp.int32)
    key_valid = positions < length
    row_valid = key_valid.astype(jnp.float32)[:, None]
    head_ids = jnp.arange(HEADS, dtype=jnp.int32).astype(jnp.float32)
    slopes = jnp.exp2(-8.0 * (head_ids + 1.0) / HEADS)
    queries = low_back(low(jnp.dot(inputs, qkv_weight[0], precision=highest) + qv_bias[0]))
    key_rows = low_back(low(jnp.dot(inputs, qkv_weight[1], precision=highest)))
    value_rows = low_back(low(jnp.dot(inputs, qkv_weight[2], precision=highest) + qv_bias[1]))
    key_heads = key_rows.reshape(slot_count, HEADS, HEAD)
    value_heads = value_rows.reshape(slot_count, HEADS, HEAD)
    block_size = min(512, slot_count)
    block_count = slot_count // block_size
    query_blocks = queries.reshape(block_count, block_size, HEADS, HEAD)
    first_rows = jnp.arange(block_count, dtype=jnp.int32) * block_size

    def attend_block(query_block, first_row):
        query_pos = first_row + jnp.arange(block_size, dtype=jnp.int32)
        distance = jnp.abs(query_pos[:, None] - positions[None, :]).astype(jnp.float32)
        raw_scores = jnp.einsum('qhc,khc->hqk', query_block, key_heads, precision=highest)
        scores = low_back(0.125 * raw_scores - slopes[:, None, None] * distance[None, :, :])
        scores = jnp.where(key_valid[None, None, :], scores, -1e+30)
        weights = low(jax.nn.softmax(scores, axis=-1))
        return jnp.einsum('hqk,khc->qhc', weights, value_heads, precision=highest)
    checked = jax.checkpoint(attend_block)
    mixed_heads = lax.map(lambda block_pair: checked(block_pair[0], block_pair[1]), (query_blocks, first_rows))
    mixed_heads = low_back(low(mixed_heads.reshape(slot_count, D)))
    branch = low_back(jnp.dot(mixed_heads, out_weight, precision=highest))
    attended = layer_norm(inputs + branch + offsets[0], norm_gains[0], offsets[1])
    attended_low = low(attended)
    gate_pre = low_back(jnp.dot(attended_low, in_weight[0], precision=highest) + in_bias[0])
    up_pre = low_back(jnp.dot(attended_low, in_weight[1], precision=highest) + in_bias[1])
    hidden = low(jax.nn.gelu(gate_pre, approximate=False) * up_pre)
    branch_ff = low_back(jnp.dot(hidden, down_weight, precision=highest))
    final_norm = layer_norm(attended + branch_ff + offsets[2], norm_gains[1], offsets[3])
    return final_norm * row_valid

def reference(tokens, lengths, qkv_weight, qv_bias, out_weight, in_weight, in_bias, down_weight, norm_gains, offsets, cotangent):
    params = (qkv_weight.astype(jnp.float32), qv_bias.astype(jnp.float32), out_weight.astype(jnp.float32), in_weight.astype(jnp.float32), in_bias.astype(jnp.float32), down_weight.astype(jnp.float32), norm_gains.astype(jnp.float32), offsets.astype(jnp.float32))
    inputs = tokens.astype(jnp.float32).reshape(SEQS, SEQ, D)
    cotangents = cotangent.astype(jnp.float32).reshape(SEQS, SEQ, D)
    zero_grads = jax.tree.map(jnp.zeros_like, params)

    def per_sequence(totals, seq_item):
        seq_in, seq_cot, length = seq_item
        outputs, pullback = jax.vjp(lambda weights_now, rows_now: forward_sequence(weights_now, rows_now, length), params, seq_in)
        grad_params, grad_rows = pullback(seq_cot)
        return (jax.tree.map(jnp.add, totals, grad_params), (outputs.astype(jnp.bfloat16), grad_rows))
    totals, (outputs, grad_rows) = lax.scan(per_sequence, zero_grads, (inputs, cotangents, lengths))
    return (outputs.reshape(TOKENS, D), grad_rows.reshape(TOKENS, D), totals[0], totals[1], totals[2], totals[3], totals[4], totals[5], totals[6], totals[7])
```

```python
import functools

import jax
import jax.numpy as jnp
from jax import lax
from jax.experimental import pallas as pl
from jax.experimental.pallas import tpu as pltpu
from jax.sharding import PartitionSpec as P

HEAD = 64
MESH = pl.DeviceIdType.MESH
VMEM_LIMIT = 64 * 1024 * 1024 - 65536


class Grid3:
    def __init__(self, dp):
        self.nx, self.ny = 2, 2
        self.nz = dp // 4

    def here(self):
        me = lax.axis_index("dp")
        return me // 4, (me // 2) % 2, me % 2

    def at(self, z, y, x):
        return (z * 2 + y) * 2 + x

    def up(self, z, k):
        return (z + k) % self.nz


def remote(src, dst, send_sem, recv_sem, **device):
    return pltpu.make_async_remote_copy(
        src_ref=src, dst_ref=dst, send_sem=send_sem, recv_sem=recv_sem, device_id=device, device_id_type=MESH
    )


def greet(grid, z, y, x, partner):
    barrier = pltpu.get_barrier_semaphore()
    peers = [grid.at(grid.up(z, k), y, x) for k in range(1, grid.nz)]
    peers += [grid.at(z, 1 - y, x), grid.at(z, y, 1 - x)]
    for peer in peers:
        pl.semaphore_signal(barrier, inc=1, device_id={"dp": peer}, device_id_type=MESH)
    if partner is not None:
        pl.semaphore_signal(barrier, inc=1, device_id={"tensor": partner}, device_id_type=MESH)
    pl.semaphore_wait(barrier, len(peers) + (partner is not None))


class SmallSum:
    def __init__(self, grid, place, value, out, box, send, recv):
        self.grid, self.place = grid, place
        self.value, self.out, self.box, self.send, self.recv = value, out, box, send, recv
        self.copies = []

    def _post(self, slot, **device):
        copy = remote(self.out, self.box.at[slot], self.send.at[slot], self.recv.at[slot], **device)
        copy.start()
        self.copies.append(copy)

    def stage(self, number):
        z, y, x = self.place
        grid = self.grid
        if number == 0:
            self.out[...] = self.value[...]
            self._post(0, tensor=1 - lax.axis_index("tensor"))
            return
        for copy in self.copies:
            copy.wait()
        self.copies = []
        if number == 1:
            self.out[...] = self.out[...] + self.box[0]
            self._post(1, dp=grid.at(z, y, 1 - x))
        elif number == 2:
            self.out[...] = self.out[...] + self.box[1]
            self._post(2, dp=grid.at(z, 1 - y, x))
        elif number == 3:
            self.out[...] = self.out[...] + self.box[2]
            for k in range(1, grid.nz):
                self._post(2 + k, dp=grid.at(grid.up(z, k), y, x))
        else:
            total = self.out[...]
            for k in range(1, grid.nz):
                total = total + self.box[2 + k]
            self.out[...] = total


def small_slots(grid):
    return 2 + grid.nz


class Gather:
    def __init__(self, grid, place, rows, chunks, send, recv):
        self.grid, self.place, self.rows, self.chunks = grid, place, rows, chunks
        self.send_sem, self.recv_sem = send, recv
        self.copies = []

    def _dst(self, chunk, shard):
        return chunk[1](pl.ds(pl.multiple_of(shard * self.rows, self.rows), self.rows))

    def _send(self, number, shard, peer, slot, first=False):
        chunk = self.chunks[number]
        dst = self._dst(chunk, shard)
        copy = remote(
            chunk[0] if first else dst, dst, self.send_sem.at[number, slot], self.recv_sem.at[number, slot], dp=peer
        )
        copy.start()
        self.copies.append(copy)

    def _arrive(self, number, shard, slot):
        dst = self._dst(self.chunks[number], shard)
        remote(dst, dst, self.send_sem.at[number, slot], self.recv_sem.at[number, slot], dp=shard).wait_recv()

    def peer(self, colour, order):
        z, y, x = self.place
        along_y = (colour == 0) == (order == 0)
        return self.grid.at(z, 1 - y, x) if along_y else self.grid.at(z, y, 1 - x)

    def shard(self, k, colour, order):
        z, y, x = self.place
        low = (z - k) % self.grid.nz
        if order is None:
            return self.grid.at(low, y, x)
        if order == 2:
            return self.grid.at(low, 1 - y, 1 - x)
        along_y = (colour == 0) == (order == 0)
        return self.grid.at(low, 1 - y, x) if along_y else self.grid.at(low, y, 1 - x)

    def begin(self, number):
        nz = self.grid.nz
        colour = self.chunks[number][2]
        z, y, x = self.place
        me = self.grid.at(z, y, x)
        for k in range(1, nz):
            self._send(number, me, self.grid.at(self.grid.up(z, k), y, x), k - 1, True)
        self._send(number, me, self.peer(colour, 0), nz - 1, True)
        self._send(number, me, self.peer(colour, 1), 2 * nz - 1, True)

    def from_line(self, number, k):
        nz = self.grid.nz
        colour = self.chunks[number][2]
        shard = self.shard(k, colour, None)
        self._arrive(number, shard, k - 1)
        self._send(number, shard, self.peer(colour, 0), nz - 1 + k)
        self._send(number, shard, self.peer(colour, 1), 2 * nz - 1 + k)

    def from_first(self, number, k):
        nz = self.grid.nz
        colour = self.chunks[number][2]
        shard = self.shard(k, colour, 0)
        self._arrive(number, shard, nz - 1 + k)
        self._send(number, shard, self.peer(colour, 1), 3 * nz - 1 + k)

    def finish(self, number):
        nz = self.grid.nz
        colour = self.chunks[number][2]
        for k in range(nz):
            self._arrive(number, self.shard(k, colour, 1), 2 * nz - 1 + k)
            self._arrive(number, self.shard(k, colour, 2), 3 * nz - 1 + k)

    def drain(self):
        for copy in self.copies:
            copy.wait_send()
        self.copies = []


def gather_slots(grid):
    return 4 * grid.nz - 1


class Scatter:
    def __init__(self, grid, place, rows, chunks, send, recv):
        self.grid, self.place, self.rows, self.chunks = grid, place, rows, chunks
        self.send_sem, self.recv_sem = send, recv
        self.copies = []

    def peer(self, colour, order):
        z, y, x = self.place
        along_x = (colour == 0) == (order == 0)
        return self.grid.at(z, y, 1 - x) if along_x else self.grid.at(z, 1 - y, x)

    def _part(self, number, shard):
        return self.chunks[number][0](pl.ds(pl.multiple_of(shard * self.rows, self.rows), self.rows))

    def shard(self, k, colour, mine0, mine1):
        z, y, x = self.place
        high = self.grid.up(z, k)
        xs, ys = (mine0, mine1) if colour == 0 else (mine1, mine0)
        return self.grid.at(high, y if ys else 1 - y, x if xs else 1 - x)

    def _send(self, number, source, slot, peer):
        box = self.chunks[number][3]
        copy = remote(
            source, box.at[slot], self.send_sem.at[number, slot], self.recv_sem.at[number, slot], dp=peer
        )
        copy.start()
        self.copies.append(copy)

    def _arrive(self, number, slot):
        box = self.chunks[number][3].at[slot]
        remote(box, box, self.send_sem.at[number, slot], self.recv_sem.at[number, slot], dp=0).wait_recv()

    def begin(self, number):
        nz = self.grid.nz
        colour = self.chunks[number][2]
        peer = self.peer(colour, 0)
        for k in list(range(1, nz)) + [0]:
            self._send(number, self._part(number, self.shard(k, colour, False, False)), k, peer)
        for k in list(range(1, nz)) + [0]:
            self._send(number, self._part(number, self.shard(k, colour, False, True)), nz + k, peer)

    def second(self, number, k):
        nz = self.grid.nz
        colour, box = self.chunks[number][2:4]
        self._arrive(number, k)
        shard = self.shard(k, colour, True, False)
        part = self._part(number, shard)
        box[k] = (part[...].astype(jnp.float32) + box[k].astype(jnp.float32)).astype(jnp.bfloat16)
        self._send(number, box.at[k], 2 * nz + k, self.peer(colour, 1))

    def third(self, number, k):
        nz = self.grid.nz
        colour, box = self.chunks[number][2:4]
        z, y, x = self.place
        self._arrive(number, nz + k)
        self._arrive(number, 2 * nz + k)
        shard = self.shard(k, colour, True, True)
        part = self._part(number, shard)
        total = part[...].astype(jnp.float32) + box[nz + k].astype(jnp.float32) + box[2 * nz + k].astype(jnp.float32)
        box[nz + k] = total.astype(jnp.bfloat16)
        self._send(number, box.at[nz + k], 3 * nz - 1 + k, self.grid.at(self.grid.up(z, k), y, x))

    def last(self, number):
        nz = self.grid.nz
        colour, box = self.chunks[number][2:4]
        self._arrive(number, nz)
        self._arrive(number, 2 * nz)
        part = self._part(number, self.shard(0, colour, True, True))
        total = part[...].astype(jnp.float32) + box[nz].astype(jnp.float32) + box[2 * nz].astype(jnp.float32)
        for k in range(1, nz):
            self._arrive(number, 3 * nz - 1 + k)
            total = total + box[3 * nz - 1 + k].astype(jnp.float32)
        self.chunks[number][1][...] = total

    def drain(self):
        for copy in self.copies:
            copy.wait_send()
        self.copies = []


def scatter_slots(grid):
    return 4 * grid.nz - 1


def gather_chunks(qkv, outw, inw, down, to_qkv, to_out, to_in, to_down):
    half = down.shape[1] // 2
    first, second = pl.ds(0, half), pl.ds(half, half)
    return [
        (qkv.at[0], lambda rows: to_qkv.at[0, rows], 0),
        (qkv.at[1], lambda rows: to_qkv.at[1, rows], 1),
        (qkv.at[2], lambda rows: to_qkv.at[2, rows], 0),
        (outw, lambda rows: to_out.at[rows], 1),
        (inw.at[0], lambda rows: to_in.at[0, rows], 0),
        (inw.at[1], lambda rows: to_in.at[1, rows], 1),
        (down.at[:, first], lambda rows: to_down.at[rows, first], 0),
        (down.at[:, second], lambda rows: to_down.at[rows, second], 1),
    ]


def gather_body(grid, rows, qkv, outw, inw, down, small, to_qkv, to_out, to_in, to_down, to_small, box, send, recv, ssend, srecv, own):
    place = grid.here()
    z, y, x = place
    me = grid.at(z, y, x)
    greet(grid, z, y, x, 1 - lax.axis_index("tensor"))
    chunks = gather_chunks(qkv, outw, inw, down, to_qkv, to_out, to_in, to_down)
    gather = Gather(grid, place, rows, chunks, send, recv)
    sums = SmallSum(grid, place, small, to_small, box, ssend, srecv)
    sums.stage(0)
    for number in range(len(chunks)):
        gather.begin(number)
    mine = pl.ds(pl.multiple_of(me * rows, rows), rows)
    copies = [pltpu.make_async_copy(c[0], c[1](mine), own.at[n]) for n, c in enumerate(chunks)]
    for copy in copies:
        copy.start()
    for number in range(len(chunks)):
        for k in range(1, grid.nz):
            gather.from_line(number, k)
        for k in range(grid.nz):
            gather.from_first(number, k)
        if number < 4:
            sums.stage(number + 1)
    for number in range(len(chunks)):
        gather.finish(number)
    gather.drain()
    for copy in copies:
        copy.wait()


def gather_call(grid, qkv, outw, inw, down, small):
    rows = qkv.shape[1]
    count = rows * grid.nz * 4
    chunks = 8
    shapes = [
        jax.ShapeDtypeStruct((3, count, qkv.shape[2]), qkv.dtype),
        jax.ShapeDtypeStruct((count, outw.shape[1]), outw.dtype),
        jax.ShapeDtypeStruct((2, count, inw.shape[2]), inw.dtype),
        jax.ShapeDtypeStruct((count, down.shape[1]), down.dtype),
        jax.ShapeDtypeStruct(small.shape, small.dtype),
    ]
    vmem = pl.BlockSpec(memory_space=pltpu.VMEM)
    slots = gather_slots(grid)
    return pl.pallas_call(
        functools.partial(gather_body, grid, rows),
        out_shape=shapes,
        in_specs=[vmem] * 5,
        out_specs=[vmem] * 5,
        scratch_shapes=[
            pltpu.VMEM((small_slots(grid), *small.shape), small.dtype),
            pltpu.SemaphoreType.DMA((chunks, slots)),
            pltpu.SemaphoreType.DMA((chunks, slots)),
            pltpu.SemaphoreType.DMA((small_slots(grid),)),
            pltpu.SemaphoreType.DMA((small_slots(grid),)),
            pltpu.SemaphoreType.DMA((chunks,)),
        ],
        compiler_params=pltpu.CompilerParams(collective_id=0, has_side_effects=True, vmem_limit_bytes=VMEM_LIMIT),
        name="gather",
    )(qkv, outw, inw, down, small)


def scatter_chunks(qkv, outw, inw, down, to_qkv, to_out, to_in, to_down, box_a, box_b, box_c):
    half = down.shape[1] // 2
    first, second = pl.ds(0, half), pl.ds(half, half)
    return [
        (lambda rows: inw.at[0, rows], to_in.at[0], 0, box_a.at[0]),
        (lambda rows: inw.at[1, rows], to_in.at[1], 1, box_a.at[1]),
        (lambda rows: down.at[rows, first], to_down.at[:, first], 0, box_b.at[0]),
        (lambda rows: down.at[rows, second], to_down.at[:, second], 1, box_b.at[1]),
        (lambda rows: outw.at[rows], to_out, 1, box_c.at[3]),
        (lambda rows: qkv.at[0, rows], to_qkv.at[0], 0, box_c.at[0]),
        (lambda rows: qkv.at[1, rows], to_qkv.at[1], 1, box_c.at[1]),
        (lambda rows: qkv.at[2, rows], to_qkv.at[2], 0, box_c.at[2]),
    ]


def scatter_body(grid, rows, qkv, outw, inw, down, small, to_qkv, to_out, to_in, to_down, to_small,
                 box_a, box_b, box_c, box, send, recv, ssend, srecv):
    place = grid.here()
    greet(grid, *place, 1 - lax.axis_index("tensor"))
    chunks = scatter_chunks(qkv, outw, inw, down, to_qkv, to_out, to_in, to_down, box_a, box_b, box_c)
    scatter = Scatter(grid, place, rows, chunks, send, recv)
    sums = SmallSum(grid, place, small, to_small, box, ssend, srecv)
    sums.stage(0)
    for number in range(len(chunks)):
        scatter.begin(number)
    for number in range(len(chunks)):
        for k in list(range(1, grid.nz)) + [0]:
            scatter.second(number, k)
        if number < 4:
            sums.stage(number + 1)
        if number >= 2:
            for k in range(1, grid.nz):
                scatter.third(number - 2, k)
    for number in range(len(chunks) - 2, len(chunks)):
        for k in range(1, grid.nz):
            scatter.third(number, k)
    for number in range(len(chunks)):
        scatter.last(number)
    scatter.drain()


def scatter_call(grid, qkv, outw, inw, down, small):
    count = qkv.shape[1]
    rows = count // (grid.nz * 4)
    chunks = 8
    slots = scatter_slots(grid)
    f32 = jnp.float32
    shapes = [
        jax.ShapeDtypeStruct((3, rows, qkv.shape[2]), f32),
        jax.ShapeDtypeStruct((rows, outw.shape[1]), f32),
        jax.ShapeDtypeStruct((2, rows, inw.shape[2]), f32),
        jax.ShapeDtypeStruct((rows, down.shape[1]), f32),
        jax.ShapeDtypeStruct(small.shape, small.dtype),
    ]
    vmem = pl.BlockSpec(memory_space=pltpu.VMEM)
    return pl.pallas_call(
        functools.partial(scatter_body, grid, rows),
        out_shape=shapes,
        in_specs=[vmem] * 5,
        out_specs=[vmem] * 5,
        scratch_shapes=[
            pltpu.VMEM((2, slots, rows, inw.shape[2]), jnp.bfloat16),
            pltpu.VMEM((2, slots, rows, down.shape[1] // 2), jnp.bfloat16),
            pltpu.VMEM((4, slots, rows, qkv.shape[2]), jnp.bfloat16),
            pltpu.VMEM((small_slots(grid), *small.shape), small.dtype),
            pltpu.SemaphoreType.DMA((chunks, slots)),
            pltpu.SemaphoreType.DMA((chunks, slots)),
            pltpu.SemaphoreType.DMA((small_slots(grid),)),
            pltpu.SemaphoreType.DMA((small_slots(grid),)),
        ],
        input_output_aliases={},
        compiler_params=pltpu.CompilerParams(collective_id=1, has_side_effects=True, vmem_limit_bytes=VMEM_LIMIT),
        name="scatter",
    )(qkv, outw, inw, down, small)


norm_epsilon = 1e-06


def norm_forward(values, gain_row, shift_row):
    centred = values - jnp.mean(values, axis=-1, keepdims=True)
    variance = jnp.mean(centred * centred, axis=-1, keepdims=True)
    inv_scale = lax.rsqrt(variance + norm_epsilon)
    unit_vals = centred * inv_scale
    return (unit_vals * gain_row + shift_row, unit_vals, inv_scale)


def norm_backward(grad_out, unit_vals, inv_scale, gain_row):
    grad_unit = grad_out * gain_row
    inner_term = (
        grad_unit
        - jnp.mean(grad_unit, axis=-1, keepdims=True)
        - unit_vals * jnp.mean(grad_unit * unit_vals, axis=-1, keepdims=True)
    )
    return (
        inner_term * inv_scale,
        jnp.sum(grad_out * unit_vals, axis=0),
        jnp.sum(grad_out, axis=0),
    )


def score_block(query_block, first_row, key_heads, slopes, key_valid):
    block_size = query_block.shape[0]
    heads_here = slopes.shape[0]
    query_heads = query_block.reshape(block_size, heads_here, HEAD)
    raw_scores = jnp.einsum(
        "qhc,khc->hqk", query_heads, key_heads, preferred_element_type=jnp.float32
    )
    query_pos = first_row + lax.iota(jnp.int32, block_size)
    key_pos = lax.iota(jnp.int32, key_heads.shape[0])
    distance = jnp.abs(query_pos[:, None] - key_pos[None, :]).astype(jnp.float32)
    scores = 0.125 * raw_scores - slopes[:, None, None] * distance[None, :, :]
    return (jnp.where(key_valid[None, None, :], scores, -1e30), query_heads)


def attend(queries, key_rows, value_rows, slopes, key_valid):
    slot_count, width_here = queries.shape
    heads_here = width_here // HEAD
    block_size = min(512, slot_count)
    key_heads = key_rows.reshape(slot_count, heads_here, HEAD)
    value_heads = value_rows.reshape(slot_count, heads_here, HEAD)

    def one_block(first_row):
        query_block = lax.dynamic_slice_in_dim(queries, first_row, block_size, 0)
        scores, query_heads = score_block(query_block, first_row, key_heads, slopes, key_valid)
        row_max = jnp.max(scores, axis=-1, keepdims=True)
        exp_scores = jnp.exp(scores - row_max)
        row_total = jnp.sum(exp_scores, axis=-1, keepdims=True)
        weights = (exp_scores / row_total).astype(jnp.bfloat16)
        mixed_block = jnp.einsum(
            "hqk,khc->qhc", weights, value_heads, preferred_element_type=jnp.float32
        )
        return (
            mixed_block.reshape(block_size, width_here).astype(jnp.bfloat16),
            (row_max + jnp.log(row_total))[..., 0],
        )

    first_rows = lax.iota(jnp.int32, slot_count // block_size) * block_size
    mixed_heads, logsum = lax.map(one_block, first_rows)
    return (mixed_heads.reshape(slot_count, width_here), logsum)


def attend_back(queries, key_rows, value_rows, grad_mixed, logsum, slopes, key_valid):
    slot_count, width_here = queries.shape
    heads_here = width_here // HEAD
    block_size = min(512, slot_count)
    key_heads = key_rows.reshape(slot_count, heads_here, HEAD)
    value_heads = value_rows.reshape(slot_count, heads_here, HEAD)

    def one_block(running, block_item):
        grad_keys, grad_values = running
        first_row, block_lse = block_item
        query_block = lax.dynamic_slice_in_dim(queries, first_row, block_size, 0)
        grad_block = lax.dynamic_slice_in_dim(grad_mixed, first_row, block_size, 0)
        scores, query_heads = score_block(query_block, first_row, key_heads, slopes, key_valid)
        probs = jnp.exp(scores - block_lse[..., None])
        grad_heads = grad_block.reshape(block_size, heads_here, HEAD)
        grad_probs = jnp.einsum(
            "qhc,khc->hqk", grad_heads, value_heads, preferred_element_type=jnp.float32
        )
        row_dot = jnp.sum(probs * grad_probs, axis=-1, keepdims=True)
        grad_scores = (probs * (grad_probs - row_dot)).astype(jnp.bfloat16)
        grad_query = 0.125 * jnp.einsum(
            "hqk,khc->qhc", grad_scores, key_heads, preferred_element_type=jnp.float32
        )
        grad_keys = grad_keys + 0.125 * jnp.einsum(
            "hqk,qhc->khc", grad_scores, query_heads, preferred_element_type=jnp.float32
        )
        grad_values = grad_values + jnp.einsum(
            "hqk,qhc->khc",
            probs.astype(jnp.bfloat16),
            grad_heads,
            preferred_element_type=jnp.float32,
        )
        return ((grad_keys, grad_values), grad_query.reshape(block_size, width_here))

    first_rows = lax.iota(jnp.int32, slot_count // block_size) * block_size
    zero_grads = jnp.zeros((slot_count, heads_here, HEAD), jnp.float32)
    (grad_keys, grad_values), grad_queries = lax.scan(
        one_block, (zero_grads, zero_grads), (first_rows, logsum)
    )
    return (
        grad_queries.reshape(slot_count, width_here),
        grad_keys.reshape(slot_count, width_here),
        grad_values.reshape(slot_count, width_here),
    )


def spread(part, index, count):
    wide = jnp.tile(part, (1, count))
    owner = lax.broadcasted_iota(jnp.int32, wide.shape, 1) // part.shape[1]
    return jnp.where(owner == index, wide.astype(jnp.float32), 0.0)


def pick(whole, index, count):
    size = whole.shape[1] // count
    return lax.dynamic_slice_in_dim(whole, index * size, size, 1)


def pack_small(biases_qv, biases_in, rows_all, piece, pieces):
    width = rows_all.shape[1]
    halves = [b if pieces == 1 else spread(b, piece, pieces) for b in (biases_qv, biases_in)]
    rows = [rows_all] + [h.reshape(-1, width) for h in halves]
    packed = jnp.concatenate(rows, axis=0)
    return jnp.pad(packed, ((0, -packed.shape[0] % 8), (0, 0)))


def unpack_small(packed, width_qv, width_in, piece, pieces):
    width = packed.shape[1]
    count_qv = 2 * width_qv * pieces // width
    count_in = 2 * width_in * pieces // width
    whole_qv = packed[6 : 6 + count_qv].reshape(2, -1)
    whole_in = packed[6 + count_qv : 6 + count_qv + count_in].reshape(2, -1)
    return packed[:6], pick(whole_qv, piece, pieces), pick(whole_in, piece, pieces)


def per_device(
    direct,
    tokens,
    lengths,
    qkv_weight,
    qv_bias,
    out_weight,
    in_weight,
    in_bias,
    down_weight,
    norm_gains,
    offsets,
    cotangent,
):
    row_count = tokens.shape[0]
    dp = lax.axis_size("dp")
    pieces = lax.axis_size("tensor")
    piece_index = lax.axis_index("tensor")
    dp_index = lax.axis_index("dp")
    flat_index = dp_index * pieces + piece_index
    grid = Grid3(dp)
    slot_count = row_count * pieces
    length = lengths[0]
    heads_here = qkv_weight.shape[2] // HEAD
    head_ids = (piece_index * heads_here + lax.iota(jnp.int32, heads_here)).astype(jnp.float32)
    slopes = jnp.exp2(-8.0 * (head_ids + 1.0) / (heads_here * pieces))
    key_valid = lax.iota(jnp.int32, slot_count) < length
    row_valid = (piece_index * row_count + lax.iota(jnp.int32, row_count) < length).astype(
        jnp.float32
    )[:, None]

    width_qv, width_in = qkv_weight.shape[2], in_weight.shape[2]
    small = pack_small(
        spread(qv_bias, dp_index, dp),
        spread(in_bias, dp_index, dp),
        jnp.concatenate([spread(norm_gains, flat_index, dp * pieces), spread(offsets, flat_index, dp * pieces)]),
        piece_index,
        pieces,
    )
    parts = (qkv_weight, out_weight.T, in_weight, down_weight.T)
    if direct:
        whole_qkv, whole_out_t, whole_in, whole_down_t, small = gather_call(grid, *parts, small)
    else:
        whole_qkv, whole_out_t, whole_in, whole_down_t = (
            lax.all_gather(p, "dp", axis=p.ndim - 2, tiled=True) for p in parts
        )
        small = lax.psum(small, ("dp", "tensor"))
    rows_all, whole_bqv, whole_bin = unpack_small(small, width_qv, width_in, piece_index, pieces)
    gains, shift_rows = rows_all[:2], rows_all[2:6]

    gathered = lax.all_gather(tokens, "tensor", axis=0, tiled=True)
    projected = jnp.einsum("sd,kdc->ksc", gathered, whole_qkv, preferred_element_type=jnp.float32)
    queries = (projected[0] + whole_bqv[0]).astype(jnp.bfloat16)
    key_rows = projected[1].astype(jnp.bfloat16)
    value_rows = (projected[2] + whole_bqv[1]).astype(jnp.bfloat16)
    mixed_heads, logsum = attend(queries, key_rows, value_rows, slopes, key_valid)
    attn_part = jnp.einsum("sc,dc->sd", mixed_heads, whole_out_t, preferred_element_type=jnp.float32)
    attn_total = lax.psum_scatter(
        attn_part.astype(jnp.bfloat16), "tensor", scatter_dimension=0, tiled=True
    ).astype(jnp.float32)
    first_in = tokens.astype(jnp.float32) + attn_total + shift_rows[0]
    attended, unit_one, scale_one = norm_forward(first_in, gains[0], shift_rows[1])
    attended_low = attended.astype(jnp.bfloat16)
    gathered_ff = lax.all_gather(attended_low, "tensor", axis=0, tiled=True)
    pre_acts = jnp.einsum("sd,kdc->ksc", gathered_ff, whole_in, preferred_element_type=jnp.float32)
    pre_acts = pre_acts + whole_bin[:, None, :]
    hidden = (jax.nn.gelu(pre_acts[0], approximate=False) * pre_acts[1]).astype(jnp.bfloat16)
    ff_part = jnp.einsum("sf,df->sd", hidden, whole_down_t, preferred_element_type=jnp.float32)
    ff_total = lax.psum_scatter(
        ff_part.astype(jnp.bfloat16), "tensor", scatter_dimension=0, tiled=True
    ).astype(jnp.float32)
    second_in = attended + ff_total + shift_rows[2]
    final_norm, unit_two, scale_two = norm_forward(second_in, gains[1], shift_rows[3])
    output = (final_norm * row_valid).astype(jnp.bfloat16)
    grad_final = cotangent.astype(jnp.float32) * row_valid
    grad_second, grad_gain_two, grad_shift_two = norm_backward(
        grad_final, unit_two, scale_two, gains[1]
    )
    grad_bdown = jnp.sum(grad_second, axis=0)
    grad_ff_rows = lax.all_gather(grad_second.astype(jnp.bfloat16), "tensor", axis=0, tiled=True)
    grad_down_t = jnp.einsum("sd,sf->df", grad_ff_rows, hidden, preferred_element_type=jnp.float32)
    grad_hidden = jnp.einsum("sd,df->sf", grad_ff_rows, whole_down_t, preferred_element_type=jnp.float32)
    pullback = jax.vjp(
        lambda gate_pre, up_pre: jax.nn.gelu(gate_pre, approximate=False) * up_pre,
        pre_acts[0],
        pre_acts[1],
    )[1]
    grad_gate, grad_up = pullback(grad_hidden)
    grad_pre = jnp.stack([grad_gate, grad_up]).astype(jnp.bfloat16)
    grad_bin = jnp.sum(grad_pre, axis=1, dtype=jnp.float32)
    grad_in = jnp.einsum("sd,ksc->kdc", gathered_ff, grad_pre, preferred_element_type=jnp.float32)
    ff_back = jnp.einsum("ksc,kdc->sd", grad_pre, whole_in, preferred_element_type=jnp.float32)
    grad_attended = grad_second + lax.psum_scatter(
        ff_back.astype(jnp.bfloat16), "tensor", scatter_dimension=0, tiled=True
    ).astype(jnp.float32)
    grad_first, grad_gain_one, grad_shift_one = norm_backward(
        grad_attended, unit_one, scale_one, gains[0]
    )
    grad_bout = jnp.sum(grad_first, axis=0)
    grad_attn_rows = lax.all_gather(grad_first.astype(jnp.bfloat16), "tensor", axis=0, tiled=True)
    grad_out_t = jnp.einsum("sd,sc->dc", grad_attn_rows, mixed_heads, preferred_element_type=jnp.float32)
    grad_mixed = jnp.einsum(
        "sd,dc->sc", grad_attn_rows, whole_out_t, preferred_element_type=jnp.float32
    ).astype(jnp.bfloat16)
    grad_queries, grad_keys, grad_values = attend_back(
        queries, key_rows, value_rows, grad_mixed, logsum, slopes, key_valid
    )
    grad_qkv = jnp.stack([grad_queries, grad_keys, grad_values]).astype(jnp.bfloat16)
    grad_wqkv = jnp.einsum("sd,ksc->kdc", gathered, grad_qkv, preferred_element_type=jnp.float32)
    grad_bqv = jnp.stack(
        [
            jnp.sum(grad_qkv[0], axis=0, dtype=jnp.float32),
            jnp.sum(grad_qkv[2], axis=0, dtype=jnp.float32),
        ]
    )
    input_back = jnp.einsum("ksc,kdc->sd", grad_qkv, whole_qkv, preferred_element_type=jnp.float32)
    grad_tokens = grad_first + lax.psum_scatter(
        input_back.astype(jnp.bfloat16), "tensor", scatter_dimension=0, tiled=True
    ).astype(jnp.float32)

    small_grads = pack_small(
        grad_bqv,
        grad_bin,
        jnp.stack([grad_gain_one, grad_gain_two, grad_bout, grad_shift_one, grad_bdown, grad_shift_two]),
        piece_index,
        pieces,
    )
    grads = tuple(g.astype(jnp.bfloat16) for g in (grad_wqkv, grad_out_t, grad_in, grad_down_t))
    if direct:
        shard_wqkv, shard_out_t, shard_in, shard_down_t, small_grads = scatter_call(grid, *grads, small_grads)
    else:
        shard_wqkv, shard_out_t, shard_in, shard_down_t = (
            lax.psum_scatter(g.astype(jnp.float32), "dp", scatter_dimension=g.ndim - 2, tiled=True) for g in grads
        )
        small_grads = lax.psum(small_grads, ("dp", "tensor"))
    row_grads, bqv_grads, bin_grads = unpack_small(small_grads, width_qv, width_in, piece_index, pieces)
    own_rows = pick(row_grads, flat_index, dp * pieces)
    return (
        output,
        grad_tokens,
        shard_wqkv,
        pick(bqv_grads, dp_index, dp),
        shard_out_t.T,
        shard_in,
        pick(bin_grads, dp_index, dp),
        shard_down_t.T,
        own_rows[:2],
        own_rows[2:],
    )


def solution(mesh):
    placed = (
        P(("dp", "tensor"), None),
        P("dp"),
        P(None, "dp", "tensor"),
        P(None, ("tensor", "dp")),
        P("tensor", "dp"),
        P(None, "dp", "tensor"),
        P(None, ("tensor", "dp")),
        P("tensor", "dp"),
        P(None, ("dp", "tensor")),
        P(None, ("dp", "tensor")),
        P(("dp", "tensor"), None),
    )

    def run(*args):
        dp = mesh.shape["dp"]
        direct = dp % 4 == 0 and (args[2].shape[1] // dp) % 16 == 0 and mesh.shape["tensor"] == 2
        return jax.shard_map(
            functools.partial(per_device, direct),
            mesh=mesh,
            in_specs=placed,
            out_specs=(
                P(("dp", "tensor"), None),
                P(("dp", "tensor"), None),
                P(None, "dp", "tensor"),
                P(None, ("tensor", "dp")),
                P("tensor", "dp"),
                P(None, "dp", "tensor"),
                P(None, ("tensor", "dp")),
                P("tensor", "dp"),
                P(None, ("dp", "tensor")),
                P(None, ("dp", "tensor")),
            ),
            check_vma=False,
        )(*args)

    return run
```

```python
import functools

import jax
import jax.numpy as jnp
from jax import lax
from jax.experimental import pallas as pl
from jax.experimental.pallas import tpu as pltpu
from jax.sharding import PartitionSpec as P

HEAD = 64
MESH = pl.DeviceIdType.MESH
VMEM_LIMIT = 64 * 1024 * 1024 - 65536


class Grid3:
    def __init__(self, dp):
        self.nx, self.ny = 2, 2
        self.nz = dp // 4

    def here(self):
        me = lax.axis_index("dp")
        return me // 4, (me // 2) % 2, me % 2

    def at(self, z, y, x):
        return (z * 2 + y) * 2 + x

    def up(self, z, k):
        return (z + k) % self.nz


def remote(src, dst, send_sem, recv_sem, **device):
    return pltpu.make_async_remote_copy(
        src_ref=src, dst_ref=dst, send_sem=send_sem, recv_sem=recv_sem, device_id=device, device_id_type=MESH
    )


def greet(grid, z, y, x, partner):
    barrier = pltpu.get_barrier_semaphore()
    peers = [grid.at(grid.up(z, k), y, x) for k in range(1, grid.nz)]
    peers += [grid.at(z, 1 - y, x), grid.at(z, y, 1 - x)]
    for peer in peers:
        pl.semaphore_signal(barrier, inc=1, device_id={"dp": peer}, device_id_type=MESH)
    if partner is not None:
        pl.semaphore_signal(barrier, inc=1, device_id={"tensor": partner}, device_id_type=MESH)
    pl.semaphore_wait(barrier, len(peers) + (partner is not None))


class SmallSum:
    def __init__(self, grid, place, value, out, box, send, recv):
        self.grid, self.place = grid, place
        self.value, self.out, self.box, self.send, self.recv = value, out, box, send, recv
        self.copies = []

    def _post(self, slot, **device):
        copy = remote(self.out, self.box.at[slot], self.send.at[slot], self.recv.at[slot], **device)
        copy.start()
        self.copies.append(copy)

    def stage(self, number):
        z, y, x = self.place
        grid = self.grid
        if number == 0:
            self.out[...] = self.value[...]
            self._post(0, tensor=1 - lax.axis_index("tensor"))
            return
        for copy in self.copies:
            copy.wait()
        self.copies = []
        if number == 1:
            self.out[...] = self.out[...] + self.box[0]
            self._post(1, dp=grid.at(z, y, 1 - x))
        elif number == 2:
            self.out[...] = self.out[...] + self.box[1]
            self._post(2, dp=grid.at(z, 1 - y, x))
        elif number == 3:
            self.out[...] = self.out[...] + self.box[2]
            for k in range(1, grid.nz):
                self._post(2 + k, dp=grid.at(grid.up(z, k), y, x))
        else:
            total = self.out[...]
            for k in range(1, grid.nz):
                total = total + self.box[2 + k]
            self.out[...] = total


def small_slots(grid):
    return 2 + grid.nz


class Gather:
    def __init__(self, grid, place, rows, chunks, send, recv):
        self.grid, self.place, self.rows, self.chunks = grid, place, rows, chunks
        self.send_sem, self.recv_sem = send, recv
        self.copies = []

    def _dst(self, chunk, shard):
        return chunk[1](pl.ds(pl.multiple_of(shard * self.rows, self.rows), self.rows))

    def _send(self, number, shard, peer, slot, first=False):
        chunk = self.chunks[number]
        dst = self._dst(chunk, shard)
        copy = remote(
            chunk[0] if first else dst, dst, self.send_sem.at[number, slot], self.recv_sem.at[number, slot], dp=peer
        )
        copy.start()
        self.copies.append(copy)

    def _arrive(self, number, shard, slot):
        dst = self._dst(self.chunks[number], shard)
        remote(dst, dst, self.send_sem.at[number, slot], self.recv_sem.at[number, slot], dp=shard).wait_recv()

    def peer(self, colour, order):
        z, y, x = self.place
        along_y = (colour == 0) == (order == 0)
        return self.grid.at(z, 1 - y, x) if along_y else self.grid.at(z, y, 1 - x)

    def shard(self, k, colour, order):
        z, y, x = self.place
        low = (z - k) % self.grid.nz
        if order is None:
            return self.grid.at(low, y, x)
        if order == 2:
            return self.grid.at(low, 1 - y, 1 - x)
        along_y = (colour == 0) == (order == 0)
        return self.grid.at(low, 1 - y, x) if along_y else self.grid.at(low, y, 1 - x)

    def begin_line(self, number):
        z, y, x = self.place
        me = self.grid.at(z, y, x)
        for k in range(1, self.grid.nz):
            self._send(number, me, self.grid.at(self.grid.up(z, k), y, x), k - 1, True)

    def begin_sides(self, number):
        nz = self.grid.nz
        colour = self.chunks[number][2]
        me = self.grid.at(*self.place)
        self._send(number, me, self.peer(colour, 0), nz - 1, True)
        self._send(number, me, self.peer(colour, 1), 2 * nz - 1, True)

    def from_line(self, number, k):
        nz = self.grid.nz
        colour = self.chunks[number][2]
        shard = self.shard(k, colour, None)
        self._arrive(number, shard, k - 1)
        self._send(number, shard, self.peer(colour, 0), nz - 1 + k)
        self._send(number, shard, self.peer(colour, 1), 2 * nz - 1 + k)

    def from_first(self, number, k):
        nz = self.grid.nz
        colour = self.chunks[number][2]
        shard = self.shard(k, colour, 0)
        self._arrive(number, shard, nz - 1 + k)
        self._send(number, shard, self.peer(colour, 1), 3 * nz - 1 + k)

    def finish(self, number):
        nz = self.grid.nz
        colour = self.chunks[number][2]
        for k in range(nz):
            self._arrive(number, self.shard(k, colour, 1), 2 * nz - 1 + k)
            self._arrive(number, self.shard(k, colour, 2), 3 * nz - 1 + k)

    def drain(self):
        for copy in self.copies:
            copy.wait_send()
        self.copies = []


def gather_slots(grid):
    return 4 * grid.nz - 1


class Scatter:
    def __init__(self, grid, place, rows, chunks, send, recv):
        self.grid, self.place, self.rows, self.chunks = grid, place, rows, chunks
        self.send_sem, self.recv_sem = send, recv
        self.copies = []

    def peer(self, colour, order):
        z, y, x = self.place
        along_x = (colour == 0) == (order == 0)
        return self.grid.at(z, y, 1 - x) if along_x else self.grid.at(z, 1 - y, x)

    def _part(self, number, shard):
        return self.chunks[number][0](pl.ds(pl.multiple_of(shard * self.rows, self.rows), self.rows))

    def shard(self, k, colour, mine0, mine1):
        z, y, x = self.place
        high = self.grid.up(z, k)
        xs, ys = (mine0, mine1) if colour == 0 else (mine1, mine0)
        return self.grid.at(high, y if ys else 1 - y, x if xs else 1 - x)

    def _send(self, number, source, slot, peer):
        box = self.chunks[number][3]
        copy = remote(
            source, box.at[slot], self.send_sem.at[number, slot], self.recv_sem.at[number, slot], dp=peer
        )
        copy.start()
        self.copies.append(copy)

    def _arrive(self, number, slot):
        box = self.chunks[number][3].at[slot]
        remote(box, box, self.send_sem.at[number, slot], self.recv_sem.at[number, slot], dp=0).wait_recv()

    def begin(self, number):
        nz = self.grid.nz
        colour = self.chunks[number][2]
        peer = self.peer(colour, 0)
        for k in list(range(1, nz)) + [0]:
            self._send(number, self._part(number, self.shard(k, colour, False, False)), k, peer)
        for k in list(range(1, nz)) + [0]:
            self._send(number, self._part(number, self.shard(k, colour, False, True)), nz + k, peer)

    def second(self, number, k):
        nz = self.grid.nz
        colour, box = self.chunks[number][2:4]
        self._arrive(number, k)
        shard = self.shard(k, colour, True, False)
        part = self._part(number, shard)
        box[k] = (part[...].astype(jnp.float32) + box[k].astype(jnp.float32)).astype(jnp.bfloat16)
        self._send(number, box.at[k], 2 * nz + k, self.peer(colour, 1))

    def third(self, number, k):
        nz = self.grid.nz
        colour, box = self.chunks[number][2:4]
        z, y, x = self.place
        self._arrive(number, nz + k)
        self._arrive(number, 2 * nz + k)
        shard = self.shard(k, colour, True, True)
        part = self._part(number, shard)
        total = part[...].astype(jnp.float32) + box[nz + k].astype(jnp.float32) + box[2 * nz + k].astype(jnp.float32)
        box[nz + k] = total.astype(jnp.bfloat16)
        self._send(number, box.at[nz + k], 3 * nz - 1 + k, self.grid.at(self.grid.up(z, k), y, x))

    def last(self, number):
        nz = self.grid.nz
        colour, box = self.chunks[number][2:4]
        self._arrive(number, nz)
        self._arrive(number, 2 * nz)
        part = self._part(number, self.shard(0, colour, True, True))
        total = part[...].astype(jnp.float32) + box[nz].astype(jnp.float32) + box[2 * nz].astype(jnp.float32)
        for k in range(1, nz):
            self._arrive(number, 3 * nz - 1 + k)
            total = total + box[3 * nz - 1 + k].astype(jnp.float32)
        self.chunks[number][1][...] = total

    def drain(self):
        for copy in self.copies:
            copy.wait_send()
        self.copies = []


def scatter_slots(grid):
    return 4 * grid.nz - 1


bf16, f32 = jnp.bfloat16, jnp.float32
NORM_EPSILON = 1e-06
ROOT_HALF = 0.7071067811865476
PHI_SCALE = 0.3989422804014327


def nn(a, b):
    return jnp.dot(a, b, preferred_element_type=f32)


def nt(a, b):
    return lax.dot_general(a, b, (((1,), (1,)), ((), ())), preferred_element_type=f32)


def aligned(start, size):
    return pl.ds(pl.multiple_of(start, size), size)


def unit_rows(values):
    centred = values - jnp.mean(values, axis=-1, keepdims=True)
    variance = jnp.mean(centred * centred, axis=-1, keepdims=True)
    scale = lax.rsqrt(variance + NORM_EPSILON)
    return centred * scale, scale


def unit_back(grad_unit, unit, scale):
    inner = (
        grad_unit
        - jnp.mean(grad_unit, axis=-1, keepdims=True)
        - unit * jnp.mean(grad_unit * unit, axis=-1, keepdims=True)
    )
    return inner * scale


def fold(rows):
    return jnp.sum(rows.reshape(rows.shape[0] // 8, 8, rows.shape[1]), axis=0)


class Pump:
    def __init__(self):
        self.steps = []

    def add(self, function, *args):
        self.steps.append((function, args))

    def run(self, count=None):
        count = len(self.steps) if count is None else min(count, len(self.steps))
        for function, args in self.steps[:count]:
            function(*args)
        self.steps = self.steps[count:]


def layer_body(
    grid, rows,
    tokens, cotangent, length, slopes, qkv_part, out_part, in_part, down_part, small,
    output, grad_tokens, to_qkv, to_out, to_in, to_down, small_grads, probs_far,
    w_qkv, w_out, w_in, w_down, every_small, small_box,
    x, qkv, inverse, mixed, work, key_aug, value_aug, query_aug, bias,
    attended, unit_one, scale_one, attended_low, branch_rows, outgoing, incoming, cot, turned,
    pair_a, pair_b, grad_value_t, grad_key_t,
    g_qkv, g_out, g_in, g_down, box_in, box_down, box_rest,
    gather_send, gather_recv, scatter_send, scatter_recv, small_send, small_recv, own_sem, swap_send, swap_recv, local_sem, prob_sem,
):
    place = grid.here()
    z, y, col = place
    me = grid.at(z, y, col)
    side = lax.axis_index("tensor")
    other = 1 - side
    half = tokens.shape[0]
    slots = 2 * half
    width = tokens.shape[1]
    heads_wide = mixed.shape[1]
    units = w_down.shape[1]
    mine = aligned(side * half, half)
    theirs = aligned(other * half, half)
    count = length[0]

    greet(grid, z, y, col, other)

    gate_cols, up_cols = pl.ds(0, units), pl.ds(units, units)
    low, high = pl.ds(0, units // 2), pl.ds(units // 2, units // 2)
    third = [pl.ds(i * heads_wide, heads_wide) for i in range(3)]

    gather = Gather(grid, place, rows, [
        (qkv_part.at[0], lambda r: w_qkv.at[r, third[0]], 0),
        (qkv_part.at[1], lambda r: w_qkv.at[r, third[1]], 1),
        (qkv_part.at[2], lambda r: w_qkv.at[r, third[2]], 0),
        (out_part, lambda r: w_out.at[r], 1),
        (in_part.at[0], lambda r: w_in.at[r, gate_cols], 0),
        (in_part.at[1], lambda r: w_in.at[r, up_cols], 1),
        (down_part.at[:, low], lambda r: w_down.at[r, low], 0),
        (down_part.at[:, high], lambda r: w_down.at[r, high], 1),
    ], gather_send, gather_recv)
    scatter = Scatter(grid, place, rows, [
        (lambda r: g_down.at[r, low], to_down.at[:, low], 0, box_down.at[0]),
        (lambda r: g_down.at[r, high], to_down.at[:, high], 1, box_down.at[1]),
        (lambda r: g_in.at[r, gate_cols], to_in.at[0], 0, box_in.at[0]),
        (lambda r: g_in.at[r, up_cols], to_in.at[1], 1, box_in.at[1]),
        (lambda r: g_out.at[r], to_out, 1, box_rest.at[3]),
        (lambda r: g_qkv.at[r, third[0]], to_qkv.at[0], 0, box_rest.at[0]),
        (lambda r: g_qkv.at[r, third[1]], to_qkv.at[1], 1, box_rest.at[1]),
        (lambda r: g_qkv.at[r, third[2]], to_qkv.at[2], 0, box_rest.at[2]),
    ], scatter_send, scatter_recv)
    nz = grid.nz

    def swap(source, target, slot):
        copy = remote(source, target, swap_send.at[slot], swap_recv.at[slot], tensor=other)
        copy.start()
        return copy

    token_swap = swap(tokens, x.at[mine], 0)
    token_copy = pltpu.make_async_copy(tokens, x.at[mine], local_sem.at[0])
    token_copy.start()
    cot_copy = pltpu.make_async_copy(cotangent, cot, local_sem.at[1])
    cot_copy.start()
    own_rows = aligned(me * rows, rows)
    own_copies = [
        pltpu.make_async_copy(c[0], c[1](own_rows), own_sem.at[n]) for n, c in enumerate(gather.chunks)
    ]
    for copy in own_copies:
        copy.start()
    sums = SmallSum(grid, place, small, every_small, small_box, small_send.at[0], small_recv.at[0])
    for number in range(4):
        gather.begin_line(number)
    sums.stage(0)
    sums.stage(1)
    sums.stage(2)
    sums.stage(3)
    for number in range(4, 8):
        gather.begin_line(number)
    for number in range(4):
        gather.begin_sides(number)
    for number in range(4):
        for k in range(1, nz):
            gather.from_line(number, k)
        if number == 1:
            gather.begin_sides(4)
        if number == 3:
            gather.begin_sides(5)
    for number in range(4):
        for k in range(nz):
            gather.from_first(number, k)
    gather.begin_sides(6)
    gather.begin_sides(7)
    sums.stage(4)
    for copy in own_copies:
        copy.wait()
    token_copy.wait()
    token_swap.wait()
    for number in range(3):
        gather.finish(number)

    bias_q = every_small[6:7, pl.ds(pl.multiple_of(side * heads_wide, 128), heads_wide)]
    bias_v = every_small[7:8, pl.ds(pl.multiple_of(side * heads_wide, 128), heads_wide)]
    row_bias = jnp.concatenate([bias_q, jnp.zeros_like(bias_q), bias_v], axis=1)
    row_scale = jnp.where(lax.broadcasted_iota(jnp.int32, (1, 3 * heads_wide), 1) < heads_wide, 0.125, 1.0)

    @pl.loop(0, slots // 256)
    def _(i):
        r = aligned(i * 256, 256)
        raw = (nn(x[r, :], w_qkv[...]) + row_bias).astype(bf16)
        qkv[r, :] = (raw.astype(f32) * row_scale).astype(bf16)

    pump = Pump()
    for number in (4, 5):
        for k in range(1, nz):
            pump.add(gather.from_line, number, k)
    for number in (4, 5):
        for k in range(nz):
            pump.add(gather.from_first, number, k)
    for number in (6, 7):
        for k in range(1, nz):
            pump.add(gather.from_line, number, k)
    for number in (6, 7):
        for k in range(nz):
            pump.add(gather.from_first, number, k)

    lane = lax.broadcasted_iota(jnp.int32, (slots, 128), 1)
    slot = lax.broadcasted_iota(jnp.int32, (slots, 128), 0)
    key_mask = jnp.where(slot < count, 0.0, -1e30).astype(bf16)
    zero, one = jnp.zeros((), bf16), jnp.ones((), bf16)
    span = bias.shape[1]
    block = bias.shape[0]
    block_lane = lax.broadcasted_iota(jnp.int32, (block, 128), 1)
    head_count = heads_wide // 128 * 2

    def prob_slot(head):
        return work.at[:, pl.ds((head % 2) * slots, slots)]

    prob_out = [pltpu.make_async_copy(prob_slot(h), probs_far.at[h], prob_sem.at[h % 2]) for h in range(head_count)]
    for head in range(head_count):
        pair = pl.ds(head // 2 * 128, 128)
        upper = head % 2 == 1
        own = (lane >= 64) == upper
        spare = 0 if upper else 64
        gap = jnp.abs(
            lax.broadcasted_iota(jnp.int32, (block, span), 0) - (lax.broadcasted_iota(jnp.int32, (block, span), 1) - (span - slots))
        )
        bias[...] = gap.astype(f32) * slopes[head]
        q_pair = qkv[:, pl.ds(head // 2 * 128, 128)]
        k_pair = qkv[:, pl.ds(heads_wide + head // 2 * 128, 128)]
        v_pair = qkv[:, pl.ds(2 * heads_wide + head // 2 * 128, 128)]
        key_aug[...] = jnp.where(own, k_pair, jnp.where(lane == spare, key_mask, zero))
        value_aug[...] = jnp.where(own, v_pair, one)
        query_aug[...] = jnp.where(own, q_pair, jnp.where(lane == spare, one, zero))
        if head >= 2:
            prob_out[head - 2].wait()

        def attend(i, carry, head=head, pair=pair, upper=upper):
            r = aligned(i * block, block)
            scores = nt(query_aug[r, :], key_aug[...]) - bias[:, pl.ds(pl.multiple_of(span - slots - i * block, block), slots)]
            top = jnp.max(scores, axis=1, keepdims=True)
            weights = jnp.exp(scores - top).astype(bf16)
            work[r, pl.ds((head % 2) * slots, slots)] = weights
            sums_and_mixed = nn(weights, value_aug[...])
            total = sums_and_mixed[:, 0:1] if upper else sums_and_mixed[:, 64:65]
            scale = 1.0 / total
            result = (sums_and_mixed * scale).astype(bf16)
            inverse[r, head : head + 1] = scale
            if upper:
                mixed[r, pair] = jnp.where(block_lane < 64, mixed[r, pair], result)
            else:
                mixed[r, pair] = result
            return carry

        lax.fori_loop(0, slots // block, attend, 0, unroll=2)
        prob_out[head].start()
        pump.run(3)

    def project(source, weights, target_rows, sink):
        @pl.loop(0, half // 256)
        def _(i):
            r = aligned(target_rows * half + i * 256, 256)
            sink(i, nt(source[r, :], weights[...]))

    def to_outgoing(i, value):
        outgoing[aligned(i * 256, 256), :] = value.astype(bf16)

    def to_attended(i, value):
        attended[aligned(i * 256, 256), :] = value

    gather.finish(3)
    project(mixed, w_out, other, to_outgoing)
    first_swap = swap(outgoing, incoming.at[0], 1)
    project(mixed, w_out, side, to_attended)
    first_swap.wait()
    gain_one, gain_two = every_small[0:1, :], every_small[1:2, :]
    step = 64

    @pl.loop(0, half // step)
    def _(i):
        r = aligned(i * step, step)
        own = pl.ds(pl.multiple_of(side * half + i * step, step), step)
        total = x[own, :].astype(f32) + attended[r, :] + incoming[0, r, :].astype(f32) + every_small[2:3, :]
        unit, scale = unit_rows(total)
        result = unit * gain_one + every_small[3:4, :]
        unit_one[r, :] = unit
        scale_one[r, :] = jnp.broadcast_to(scale, (step, 128))
        attended[r, :] = result
        attended_low[own, :] = result.astype(bf16)

    low_swap = swap(attended_low.at[mine], attended_low.at[mine], 2)
    for head in (head_count - 2, head_count - 1):
        prob_out[head].wait()
    pump.run(4)
    gather.finish(4)
    gather.finish(5)

    in_wide = [every_small[8 + j : 9 + j, :] for j in range(8)]

    def in_row(index):
        return jnp.concatenate(
            [jnp.where(side == 0, in_wide[4 * index], in_wide[4 * index + 2]), jnp.where(side == 0, in_wide[4 * index + 1], in_wide[4 * index + 3])],
            axis=1,
        )

    turned[0:1, :] = in_row(0)
    turned[1:2, :] = in_row(1)

    def feed(rows_side):
        r = aligned(rows_side * half, half)

        @pl.loop(0, units // 256)
        def _(j):
            c = aligned(j * 256, 256)
            c_up = pl.ds(pl.multiple_of(units + j * 256, 256), 256)
            c_hidden = pl.ds(pl.multiple_of(2 * units + j * 256, 256), 256)
            gate = nn(attended_low[r, :], w_in[:, c]) + turned[0:1, c]
            up = nn(attended_low[r, :], w_in[:, c_up]) + turned[1:2, c]
            below = 0.5 * (1.0 + lax.erf(gate * ROOT_HALF))
            density = PHI_SCALE * jnp.exp(-0.5 * gate * gate)
            bent = gate * below
            work[r, c_hidden] = (bent * up).astype(bf16)
            work[r, c] = (up * (below + gate * density)).astype(bf16)
            work[r, c_up] = bent.astype(bf16)

    feed(side)
    pump.run(6)
    low_swap.wait()
    feed(other)
    pump.run()
    gather.finish(6)
    gather.finish(7)

    hidden = pl.ds(2 * units, units)

    def down(rows_side, sink):
        @pl.loop(0, half // 256)
        def _(i):
            r = aligned(rows_side * half + i * 256, 256)
            sink(i, nt(work[r, hidden], w_down[...]))

    def add_attended(i, value):
        r = aligned(i * 256, 256)
        attended[r, :] = attended[r, :] + value

    down(other, to_outgoing)
    second_swap = swap(outgoing, incoming.at[1], 3)
    down(side, add_attended)
    cot_copy.wait()
    second_swap.wait()
    nothing = jnp.zeros((8, width), f32)

    def second_norm(i, carry):
        sum_gain, sum_shift, sum_branch = carry
        r = aligned(i * step, step)
        own = pl.ds(pl.multiple_of(side * half + i * step, step), step)
        position = side * half + i * step + lax.broadcasted_iota(jnp.int32, (step, 1), 0)
        valid = jnp.where(position < count, 1.0, 0.0)
        unit, scale = unit_rows(attended[r, :] + incoming[1, r, :].astype(f32) + every_small[4:5, :])
        grad = cot[r, :].astype(f32) * valid
        cot[r, :] = ((unit * gain_two + every_small[5:6, :]) * valid).astype(bf16)
        back = unit_back(grad * gain_two, unit, scale)
        attended[r, :] = back
        branch_rows[own, :] = back.astype(bf16)
        return sum_gain + fold(grad * unit), sum_shift + fold(grad), sum_branch + fold(back)

    gain_two_sum, shift_two_sum, down_bias_sum = lax.fori_loop(0, half // step, second_norm, (nothing,) * 3)
    branch_swap = swap(branch_rows.at[mine], branch_rows.at[mine], 4)
    output_copy = pltpu.make_async_copy(cot, output, local_sem.at[2])
    output_copy.start()
    small_grads[...] = jnp.zeros_like(small_grads)
    small_grads[1:2, :] = jnp.sum(gain_two_sum, axis=0, keepdims=True)
    small_grads[5:6, :] = jnp.sum(shift_two_sum, axis=0, keepdims=True)
    small_grads[4:5, :] = jnp.sum(down_bias_sum, axis=0, keepdims=True)
    branch_swap.wait()

    def turn(source):
        @pl.loop(0, slots // 256)
        def _(i):
            r = aligned(i * 256, 256)
            grad_t[:, r] = source[r, :].T

    grad_t = pair_a

    def weight_grad(sink, source, source_start, sink_start, total, tile):
        @pl.loop(0, total // tile)
        def _(j):
            sink[:, pl.ds(pl.multiple_of(sink_start + j * tile, tile), tile)] = nn(
                grad_t[...], source[:, pl.ds(pl.multiple_of(source_start + j * tile, tile), tile)]
            ).astype(bf16)

    turn(branch_rows)
    weight_grad(g_down, work, 2 * units, 0, units // 2, 256)
    scatter.begin(0)
    weight_grad(g_down, work, 2 * units + units // 2, units // 2, units // 2, 256)
    scatter.begin(1)

    def hidden_back(rows_side):
        r = aligned(rows_side * half, half)

        @pl.loop(0, units // 512)
        def _(j):
            c = aligned(j * 512, 512)
            c_up = pl.ds(pl.multiple_of(units + j * 512, 512), 512)
            grad = nn(branch_rows[r, :], w_down[:, c])
            gate_grad = (grad * work[r, c].astype(f32)).astype(bf16)
            up_grad = (grad * work[r, c_up].astype(f32)).astype(bf16)
            work[r, c] = gate_grad
            work[r, c_up] = up_grad
            turned[8:16, c] = turned[8:16, c] + fold(gate_grad.astype(f32))
            turned[16:24, c] = turned[16:24, c] + fold(up_grad.astype(f32))

    turned[8:24, :] = jnp.zeros((16, units), f32)
    hidden_back(0)
    hidden_back(1)
    for index in range(2):
        total = jnp.sum(turned[8 + 8 * index : 16 + 8 * index, :], axis=0, keepdims=True)
        for j in range(units // width):
            small_grads[pl.ds(8 + 4 * index + 2 * side + j, 1), :] = total[:, j * width : (j + 1) * width]

    behind = list(range(1, nz)) + [0]
    pump = Pump()
    for number in (0, 1):
        for k in behind:
            pump.add(scatter.second, number, k)
    for number in (0, 1):
        for k in range(1, nz):
            pump.add(scatter.third, number, k)
    for number in (2, 3):
        for k in behind:
            pump.add(scatter.second, number, k)
    for number in (0, 1):
        pump.add(scatter.last, number)
    for number in (2, 3):
        for k in range(1, nz):
            pump.add(scatter.third, number, k)
    for k in behind:
        pump.add(scatter.second, 4, k)
    for k in range(1, nz):
        pump.add(scatter.third, 4, k)
    for number in (2, 3):
        pump.add(scatter.last, number)

    turn(attended_low)
    weight_grad(g_in, work, 0, 0, units, 512)
    scatter.begin(2)
    pump.run(4)
    weight_grad(g_in, work, units, units, units, 512)
    scatter.begin(3)
    pump.run(4)

    def units_back(rows_side, sink):
        @pl.loop(0, half // 256)
        def _(i):
            r = aligned(rows_side * half + i * 256, 256)
            sink(i, nt(work[r, pl.ds(0, 2 * units)], w_in[...]))

    units_back(other, to_outgoing)
    third_swap = swap(outgoing, incoming.at[0], 5)
    units_back(side, add_attended)
    pump.run(6)
    third_swap.wait()

    def first_norm_back(i, carry):
        sum_gain, sum_shift, sum_branch = carry
        r = aligned(i * step, step)
        own = pl.ds(pl.multiple_of(side * half + i * step, step), step)
        grad = attended[r, :] + incoming[0, r, :].astype(f32)
        unit = unit_one[r, :]
        back = unit_back(grad * gain_one, unit, scale_one[r, 0:1])
        attended[r, :] = back
        branch_rows[own, :] = back.astype(bf16)
        return sum_gain + fold(grad * unit), sum_shift + fold(grad), sum_branch + fold(back)

    prob_in = [pltpu.make_async_copy(probs_far.at[h], prob_slot(h), prob_sem.at[h % 2]) for h in range(head_count)]
    prob_in[0].start()
    prob_in[1].start()
    gain_one_sum, shift_one_sum, out_bias_sum = lax.fori_loop(0, half // step, first_norm_back, (nothing,) * 3)
    attn_swap = swap(branch_rows.at[mine], branch_rows.at[mine], 6)
    small_grads[0:1, :] = jnp.sum(gain_one_sum, axis=0, keepdims=True)
    small_grads[3:4, :] = jnp.sum(shift_one_sum, axis=0, keepdims=True)
    small_grads[2:3, :] = jnp.sum(out_bias_sum, axis=0, keepdims=True)
    attn_swap.wait()

    grad_mixed = attended_low.at[:, pl.ds(0, heads_wide)]
    turn(branch_rows)
    g_out[...] = nn(grad_t[...], mixed[...]).astype(bf16)
    scatter.begin(4)

    @pl.loop(0, slots // 256)
    def _(i):
        r = aligned(i * 256, 256)
        grad_mixed[r, :] = nn(branch_rows[r, :], w_out[...]).astype(bf16)

    grad_t = pair_a
    mixed_t, query_t = pair_b.at[0], pair_b.at[1]
    for head in range(head_count):
        pair = pl.ds(head // 2 * 128, 128)
        k_cols = pl.ds(heads_wide + head // 2 * 128, 128)
        v_cols = pl.ds(2 * heads_wide + head // 2 * 128, 128)
        upper = head % 2 == 1
        own = (lane >= 64) == upper
        spare = 0 if upper else 64
        even, odd = head // 2 * 2, head // 2 * 2 + 1
        shrink = jnp.where(lane < 64, inverse[:, even : even + 1], inverse[:, odd : odd + 1])
        scaled = (grad_mixed[:, pair].astype(f32) * shrink).astype(bf16)
        dots = jnp.sum(jnp.where(own, scaled.astype(f32) * mixed[:, pair].astype(f32), 0.0), axis=1, keepdims=True)
        dots_high = dots.astype(bf16)
        dots_low = (dots - dots_high.astype(f32)).astype(bf16)
        ones = (lane == spare) | (lane == spare + 1)
        value_aug[...] = jnp.where(own, qkv[:, v_cols], jnp.where(ones, one, zero))
        query_aug[...] = jnp.where(
            own, scaled, jnp.where(lane == spare, -dots_high, jnp.where(lane == spare + 1, -dots_low, zero))
        )
        if not upper:
            mixed_t[...] = scaled.T
            query_t[...] = qkv[:, pair].T
        part = pl.ds(64 * (head % 2), 64)
        base = (head % 2) * slots
        prob_in[head].wait()
        for j in range(slots // 512):
            c = pl.ds(j * 512, 512)
            grad_value_t[part, c] = nn(mixed_t[part, :], work[:, pl.ds(base + j * 512, 512)]).astype(bf16)

        def attend_back(i, carry, base=base, k_cols=k_cols, pair=pair, upper=upper):
            r = aligned(i * block, block)
            inner = nt(query_aug[r, :], value_aug[...])
            grads = (work[r, pl.ds(base, slots)].astype(f32) * inner).astype(bf16)
            work[r, pl.ds(base, slots)] = grads
            result = (nn(grads, qkv[:, k_cols]) * 0.125).astype(bf16)
            if upper:
                qkv[r, pair] = jnp.where(block_lane < 64, qkv[r, pair], result)
            else:
                qkv[r, pair] = result
            return carry

        lax.fori_loop(0, slots // block, attend_back, 0, unroll=2)
        for j in range(slots // 512):
            c = pl.ds(j * 512, 512)
            grad_key_t[part, c] = nn(query_t[part, :], work[:, pl.ds(base + j * 512, 512)]).astype(bf16)
        if upper:
            qkv[:, v_cols] = grad_value_t[...].T
            qkv[:, k_cols] = grad_key_t[...].T
        if head + 2 < head_count:
            prob_in[head + 2].start()
        pump.run(4)

    turn(x)
    for part in range(3):
        cols = third[part]
        g_qkv[:, cols] = nn(grad_t[...], qkv[:, cols]).astype(bf16)
        scatter.begin(5 + part)
        pump.run(3)

    def column_sum(cols):
        def add(i, carry):
            return carry + fold(qkv[aligned(i * 128, 128), cols].astype(f32))

        return jnp.sum(lax.fori_loop(0, slots // 128, add, jnp.zeros((8, heads_wide), f32)), axis=0, keepdims=True)

    side_cols = pl.ds(pl.multiple_of(side * heads_wide, 128), heads_wide)
    small_grads[6:7, side_cols] = column_sum(third[0])
    small_grads[7:8, side_cols] = column_sum(third[2])
    sums = SmallSum(grid, place, small_grads, small_grads, small_box, small_send.at[1], small_recv.at[1])
    sums.stage(0)

    def inputs_back(rows_side, sink):
        @pl.loop(0, half // 256)
        def _(i):
            r = aligned(rows_side * half + i * 256, 256)
            sink(i, nt(qkv[r, :], w_qkv[...]))

    inputs_back(other, to_outgoing)
    fourth_swap = swap(outgoing, incoming.at[1], 7)
    sums.stage(1)
    inputs_back(side, add_attended)
    pump.run()
    sums.stage(2)
    fourth_swap.wait()

    @pl.loop(0, half // step)
    def _(i):
        r = aligned(i * step, step)
        attended[r, :] = attended[r, :] + incoming[1, r, :].astype(f32)

    tokens_copy = pltpu.make_async_copy(attended, grad_tokens, local_sem.at[3])
    tokens_copy.start()

    for number in (5, 6, 7):
        for k in behind:
            scatter.second(number, k)
    sums.stage(3)
    for number in (5, 6, 7):
        for k in range(1, nz):
            scatter.third(number, k)
    for number in (4, 5, 6, 7):
        scatter.last(number)
    sums.stage(4)
    output_copy.wait()
    tokens_copy.wait()
    gather.drain()
    scatter.drain()


def layer_call(grid, tokens, cotangent, lengths, slopes, qkv_part, out_part, in_part, down_part, small):
    rows = qkv_part.shape[1]
    width = rows * grid.nz * 4
    half = tokens.shape[0]
    slots = 2 * half
    heads_wide = qkv_part.shape[2]
    units = in_part.shape[2]
    heads = heads_wide // HEAD
    block = 256
    shapes = [
        jax.ShapeDtypeStruct((half, width), bf16),
        jax.ShapeDtypeStruct((half, width), f32),
        jax.ShapeDtypeStruct(qkv_part.shape, f32),
        jax.ShapeDtypeStruct(out_part.shape, f32),
        jax.ShapeDtypeStruct(in_part.shape, f32),
        jax.ShapeDtypeStruct(down_part.shape, f32),
        jax.ShapeDtypeStruct(small.shape, f32),
        jax.ShapeDtypeStruct((heads, slots, slots), bf16),
    ]
    vmem = pl.BlockSpec(memory_space=pltpu.VMEM)
    smem = pl.BlockSpec(memory_space=pltpu.SMEM)
    anywhere = pl.BlockSpec(memory_space=pl.ANY)
    gathers, scatters, smalls = gather_slots(grid), scatter_slots(grid), small_slots(grid)
    dma = pltpu.SemaphoreType.DMA
    scratch = [
        pltpu.VMEM((width, 3 * heads_wide), bf16),
        pltpu.VMEM((width, heads_wide), bf16),
        pltpu.VMEM((width, 2 * units), bf16),
        pltpu.VMEM((width, units), bf16),
        pltpu.VMEM(small.shape, f32),
        pltpu.VMEM((smalls, *small.shape), f32),
        pltpu.VMEM((slots, width), bf16),
        pltpu.VMEM((slots, 3 * heads_wide), bf16),
        pltpu.VMEM((slots, 128), f32),
        pltpu.VMEM((slots, heads_wide), bf16),
        pltpu.VMEM((slots, 3 * units), bf16),
        pltpu.VMEM((slots, 128), bf16),
        pltpu.VMEM((slots, 128), bf16),
        pltpu.VMEM((slots, 128), bf16),
        pltpu.VMEM((block, 2 * slots - block), f32),
        pltpu.VMEM((half, width), f32),
        pltpu.VMEM((half, width), f32),
        pltpu.VMEM((half, 128), f32),
        pltpu.VMEM((slots, width), bf16),
        pltpu.VMEM((slots, width), bf16),
        pltpu.VMEM((half, width), bf16),
        pltpu.VMEM((2, half, width), bf16),
        pltpu.VMEM((half, width), bf16),
        pltpu.VMEM((24, units), f32),
        pltpu.VMEM((width, slots), bf16),
        pltpu.VMEM((2, 128, slots), bf16),
        pltpu.VMEM((128, slots), bf16),
        pltpu.VMEM((128, slots), bf16),
        pltpu.VMEM((width, 3 * heads_wide), bf16),
        pltpu.VMEM((width, heads_wide), bf16),
        pltpu.VMEM((width, 2 * units), bf16),
        pltpu.VMEM((width, units), bf16),
        pltpu.VMEM((2, scatters, rows, units), bf16),
        pltpu.VMEM((2, scatters, rows, units // 2), bf16),
        pltpu.VMEM((4, scatters, rows, heads_wide), bf16),
        dma((8, gathers)),
        dma((8, gathers)),
        dma((8, scatters)),
        dma((8, scatters)),
        dma((2, smalls)),
        dma((2, smalls)),
        dma((8,)),
        dma((8,)),
        dma((8,)),
        dma((4,)),
        dma((2,)),
    ]
    results = pl.pallas_call(
        functools.partial(layer_body, grid, rows),
        out_shape=shapes,
        in_specs=[anywhere, anywhere, smem, smem, anywhere, anywhere, anywhere, anywhere, vmem],
        out_specs=[anywhere] * 2 + [vmem] * 5 + [anywhere],
        scratch_shapes=scratch,
        compiler_params=pltpu.CompilerParams(collective_id=0, has_side_effects=True, vmem_limit_bytes=VMEM_LIMIT),
        name="layer",
    )(tokens, cotangent, lengths, slopes, qkv_part, out_part, in_part, down_part, small)
    return results[:7]


norm_epsilon = 1e-06


def norm_forward(values, gain_row, shift_row):
    centred = values - jnp.mean(values, axis=-1, keepdims=True)
    variance = jnp.mean(centred * centred, axis=-1, keepdims=True)
    inv_scale = lax.rsqrt(variance + norm_epsilon)
    unit_vals = centred * inv_scale
    return (unit_vals * gain_row + shift_row, unit_vals, inv_scale)


def norm_backward(grad_out, unit_vals, inv_scale, gain_row):
    grad_unit = grad_out * gain_row
    inner_term = (
        grad_unit
        - jnp.mean(grad_unit, axis=-1, keepdims=True)
        - unit_vals * jnp.mean(grad_unit * unit_vals, axis=-1, keepdims=True)
    )
    return (
        inner_term * inv_scale,
        jnp.sum(grad_out * unit_vals, axis=0),
        jnp.sum(grad_out, axis=0),
    )


def score_block(query_block, first_row, key_heads, slopes, key_valid):
    block_size = query_block.shape[0]
    heads_here = slopes.shape[0]
    query_heads = query_block.reshape(block_size, heads_here, HEAD)
    raw_scores = jnp.einsum(
        "qhc,khc->hqk", query_heads, key_heads, preferred_element_type=jnp.float32
    )
    query_pos = first_row + lax.iota(jnp.int32, block_size)
    key_pos = lax.iota(jnp.int32, key_heads.shape[0])
    distance = jnp.abs(query_pos[:, None] - key_pos[None, :]).astype(jnp.float32)
    scores = 0.125 * raw_scores - slopes[:, None, None] * distance[None, :, :]
    return (jnp.where(key_valid[None, None, :], scores, -1e30), query_heads)


def attend(queries, key_rows, value_rows, slopes, key_valid):
    slot_count, width_here = queries.shape
    heads_here = width_here // HEAD
    block_size = min(512, slot_count)
    key_heads = key_rows.reshape(slot_count, heads_here, HEAD)
    value_heads = value_rows.reshape(slot_count, heads_here, HEAD)

    def one_block(first_row):
        query_block = lax.dynamic_slice_in_dim(queries, first_row, block_size, 0)
        scores, query_heads = score_block(query_block, first_row, key_heads, slopes, key_valid)
        row_max = jnp.max(scores, axis=-1, keepdims=True)
        exp_scores = jnp.exp(scores - row_max)
        row_total = jnp.sum(exp_scores, axis=-1, keepdims=True)
        weights = (exp_scores / row_total).astype(jnp.bfloat16)
        mixed_block = jnp.einsum(
            "hqk,khc->qhc", weights, value_heads, preferred_element_type=jnp.float32
        )
        return (
            mixed_block.reshape(block_size, width_here).astype(jnp.bfloat16),
            (row_max + jnp.log(row_total))[..., 0],
        )

    first_rows = lax.iota(jnp.int32, slot_count // block_size) * block_size
    mixed_heads, logsum = lax.map(one_block, first_rows)
    return (mixed_heads.reshape(slot_count, width_here), logsum)


def attend_back(queries, key_rows, value_rows, grad_mixed, logsum, slopes, key_valid):
    slot_count, width_here = queries.shape
    heads_here = width_here // HEAD
    block_size = min(512, slot_count)
    key_heads = key_rows.reshape(slot_count, heads_here, HEAD)
    value_heads = value_rows.reshape(slot_count, heads_here, HEAD)

    def one_block(running, block_item):
        grad_keys, grad_values = running
        first_row, block_lse = block_item
        query_block = lax.dynamic_slice_in_dim(queries, first_row, block_size, 0)
        grad_block = lax.dynamic_slice_in_dim(grad_mixed, first_row, block_size, 0)
        scores, query_heads = score_block(query_block, first_row, key_heads, slopes, key_valid)
        probs = jnp.exp(scores - block_lse[..., None])
        grad_heads = grad_block.reshape(block_size, heads_here, HEAD)
        grad_probs = jnp.einsum(
            "qhc,khc->hqk", grad_heads, value_heads, preferred_element_type=jnp.float32
        )
        row_dot = jnp.sum(probs * grad_probs, axis=-1, keepdims=True)
        grad_scores = (probs * (grad_probs - row_dot)).astype(jnp.bfloat16)
        grad_query = 0.125 * jnp.einsum(
            "hqk,khc->qhc", grad_scores, key_heads, preferred_element_type=jnp.float32
        )
        grad_keys = grad_keys + 0.125 * jnp.einsum(
            "hqk,qhc->khc", grad_scores, query_heads, preferred_element_type=jnp.float32
        )
        grad_values = grad_values + jnp.einsum(
            "hqk,qhc->khc",
            probs.astype(jnp.bfloat16),
            grad_heads,
            preferred_element_type=jnp.float32,
        )
        return ((grad_keys, grad_values), grad_query.reshape(block_size, width_here))

    first_rows = lax.iota(jnp.int32, slot_count // block_size) * block_size
    zero_grads = jnp.zeros((slot_count, heads_here, HEAD), jnp.float32)
    (grad_keys, grad_values), grad_queries = lax.scan(
        one_block, (zero_grads, zero_grads), (first_rows, logsum)
    )
    return (
        grad_queries.reshape(slot_count, width_here),
        grad_keys.reshape(slot_count, width_here),
        grad_values.reshape(slot_count, width_here),
    )


def spread(part, index, count):
    wide = jnp.tile(part, (1, count))
    owner = lax.broadcasted_iota(jnp.int32, wide.shape, 1) // part.shape[1]
    return jnp.where(owner == index, wide.astype(jnp.float32), 0.0)


def pick(whole, index, count):
    size = whole.shape[1] // count
    return lax.dynamic_slice_in_dim(whole, index * size, size, 1)


def pack_small(biases_qv, biases_in, rows_all, piece, pieces):
    width = rows_all.shape[1]
    halves = [b if pieces == 1 else spread(b, piece, pieces) for b in (biases_qv, biases_in)]
    rows = [rows_all] + [h.reshape(-1, width) for h in halves]
    packed = jnp.concatenate(rows, axis=0)
    return jnp.pad(packed, ((0, -packed.shape[0] % 8), (0, 0)))


def unpack_small(packed, width_qv, width_in, piece, pieces):
    width = packed.shape[1]
    count_qv = 2 * width_qv * pieces // width
    count_in = 2 * width_in * pieces // width
    whole_qv = packed[6 : 6 + count_qv].reshape(2, -1)
    whole_in = packed[6 + count_qv : 6 + count_qv + count_in].reshape(2, -1)
    return packed[:6], pick(whole_qv, piece, pieces), pick(whole_in, piece, pieces)


def per_device(
    direct,
    tokens,
    lengths,
    qkv_weight,
    qv_bias,
    out_weight,
    in_weight,
    in_bias,
    down_weight,
    norm_gains,
    offsets,
    cotangent,
):
    row_count = tokens.shape[0]
    dp = lax.axis_size("dp")
    pieces = lax.axis_size("tensor")
    piece_index = lax.axis_index("tensor")
    dp_index = lax.axis_index("dp")
    flat_index = dp_index * pieces + piece_index
    grid = Grid3(dp)
    slot_count = row_count * pieces
    length = lengths[0]
    heads_here = qkv_weight.shape[2] // HEAD
    head_ids = (piece_index * heads_here + lax.iota(jnp.int32, heads_here)).astype(jnp.float32)
    slopes = jnp.exp2(-8.0 * (head_ids + 1.0) / (heads_here * pieces))
    key_valid = lax.iota(jnp.int32, slot_count) < length
    row_valid = (piece_index * row_count + lax.iota(jnp.int32, row_count) < length).astype(
        jnp.float32
    )[:, None]

    width_qv, width_in = qkv_weight.shape[2], in_weight.shape[2]
    small = pack_small(
        spread(qv_bias, dp_index, dp),
        spread(in_bias, dp_index, dp),
        jnp.concatenate([spread(norm_gains, flat_index, dp * pieces), spread(offsets, flat_index, dp * pieces)]),
        piece_index,
        pieces,
    )
    parts = (qkv_weight, out_weight.T, in_weight, down_weight.T)
    if direct:
        output, grad_tokens, shard_wqkv, shard_out_t, shard_in, shard_down_t, small_grads = layer_call(
            grid, tokens, cotangent, lengths, slopes, *parts, small
        )
        row_grads, bqv_grads, bin_grads = unpack_small(small_grads, width_qv, width_in, piece_index, pieces)
        own_rows = pick(row_grads, flat_index, dp * pieces)
        return (
            output,
            grad_tokens,
            shard_wqkv,
            pick(bqv_grads, dp_index, dp),
            shard_out_t.T,
            shard_in,
            pick(bin_grads, dp_index, dp),
            shard_down_t.T,
            own_rows[:2],
            own_rows[2:],
        )
    whole_qkv, whole_out_t, whole_in, whole_down_t = (
        lax.all_gather(p, "dp", axis=p.ndim - 2, tiled=True) for p in parts
    )
    small = lax.psum(small, ("dp", "tensor"))
    rows_all, whole_bqv, whole_bin = unpack_small(small, width_qv, width_in, piece_index, pieces)
    gains, shift_rows = rows_all[:2], rows_all[2:6]

    gathered = lax.all_gather(tokens, "tensor", axis=0, tiled=True)
    projected = jnp.einsum("sd,kdc->ksc", gathered, whole_qkv, preferred_element_type=jnp.float32)
    queries = (projected[0] + whole_bqv[0]).astype(jnp.bfloat16)
    key_rows = projected[1].astype(jnp.bfloat16)
    value_rows = (projected[2] + whole_bqv[1]).astype(jnp.bfloat16)
    mixed_heads, logsum = attend(queries, key_rows, value_rows, slopes, key_valid)
    attn_part = jnp.einsum("sc,dc->sd", mixed_heads, whole_out_t, preferred_element_type=jnp.float32)
    attn_total = lax.psum_scatter(
        attn_part.astype(jnp.bfloat16), "tensor", scatter_dimension=0, tiled=True
    ).astype(jnp.float32)
    first_in = tokens.astype(jnp.float32) + attn_total + shift_rows[0]
    attended, unit_one, scale_one = norm_forward(first_in, gains[0], shift_rows[1])
    attended_low = attended.astype(jnp.bfloat16)
    gathered_ff = lax.all_gather(attended_low, "tensor", axis=0, tiled=True)
    pre_acts = jnp.einsum("sd,kdc->ksc", gathered_ff, whole_in, preferred_element_type=jnp.float32)
    pre_acts = pre_acts + whole_bin[:, None, :]
    hidden = (jax.nn.gelu(pre_acts[0], approximate=False) * pre_acts[1]).astype(jnp.bfloat16)
    ff_part = jnp.einsum("sf,df->sd", hidden, whole_down_t, preferred_element_type=jnp.float32)
    ff_total = lax.psum_scatter(
        ff_part.astype(jnp.bfloat16), "tensor", scatter_dimension=0, tiled=True
    ).astype(jnp.float32)
    second_in = attended + ff_total + shift_rows[2]
    final_norm, unit_two, scale_two = norm_forward(second_in, gains[1], shift_rows[3])
    output = (final_norm * row_valid).astype(jnp.bfloat16)
    grad_final = cotangent.astype(jnp.float32) * row_valid
    grad_second, grad_gain_two, grad_shift_two = norm_backward(
        grad_final, unit_two, scale_two, gains[1]
    )
    grad_bdown = jnp.sum(grad_second, axis=0)
    grad_ff_rows = lax.all_gather(grad_second.astype(jnp.bfloat16), "tensor", axis=0, tiled=True)
    grad_down_t = jnp.einsum("sd,sf->df", grad_ff_rows, hidden, preferred_element_type=jnp.float32)
    grad_hidden = jnp.einsum("sd,df->sf", grad_ff_rows, whole_down_t, preferred_element_type=jnp.float32)
    pullback = jax.vjp(
        lambda gate_pre, up_pre: jax.nn.gelu(gate_pre, approximate=False) * up_pre,
        pre_acts[0],
        pre_acts[1],
    )[1]
    grad_gate, grad_up = pullback(grad_hidden)
    grad_pre = jnp.stack([grad_gate, grad_up]).astype(jnp.bfloat16)
    grad_bin = jnp.sum(grad_pre, axis=1, dtype=jnp.float32)
    grad_in = jnp.einsum("sd,ksc->kdc", gathered_ff, grad_pre, preferred_element_type=jnp.float32)
    ff_back = jnp.einsum("ksc,kdc->sd", grad_pre, whole_in, preferred_element_type=jnp.float32)
    grad_attended = grad_second + lax.psum_scatter(
        ff_back.astype(jnp.bfloat16), "tensor", scatter_dimension=0, tiled=True
    ).astype(jnp.float32)
    grad_first, grad_gain_one, grad_shift_one = norm_backward(
        grad_attended, unit_one, scale_one, gains[0]
    )
    grad_bout = jnp.sum(grad_first, axis=0)
    grad_attn_rows = lax.all_gather(grad_first.astype(jnp.bfloat16), "tensor", axis=0, tiled=True)
    grad_out_t = jnp.einsum("sd,sc->dc", grad_attn_rows, mixed_heads, preferred_element_type=jnp.float32)
    grad_mixed = jnp.einsum(
        "sd,dc->sc", grad_attn_rows, whole_out_t, preferred_element_type=jnp.float32
    ).astype(jnp.bfloat16)
    grad_queries, grad_keys, grad_values = attend_back(
        queries, key_rows, value_rows, grad_mixed, logsum, slopes, key_valid
    )
    grad_qkv = jnp.stack([grad_queries, grad_keys, grad_values]).astype(jnp.bfloat16)
    grad_wqkv = jnp.einsum("sd,ksc->kdc", gathered, grad_qkv, preferred_element_type=jnp.float32)
    grad_bqv = jnp.stack(
        [
            jnp.sum(grad_qkv[0], axis=0, dtype=jnp.float32),
            jnp.sum(grad_qkv[2], axis=0, dtype=jnp.float32),
        ]
    )
    input_back = jnp.einsum("ksc,kdc->sd", grad_qkv, whole_qkv, preferred_element_type=jnp.float32)
    grad_tokens = grad_first + lax.psum_scatter(
        input_back.astype(jnp.bfloat16), "tensor", scatter_dimension=0, tiled=True
    ).astype(jnp.float32)

    small_grads = pack_small(
        grad_bqv,
        grad_bin,
        jnp.stack([grad_gain_one, grad_gain_two, grad_bout, grad_shift_one, grad_bdown, grad_shift_two]),
        piece_index,
        pieces,
    )
    grads = tuple(g.astype(jnp.bfloat16) for g in (grad_wqkv, grad_out_t, grad_in, grad_down_t))
    shard_wqkv, shard_out_t, shard_in, shard_down_t = (
        lax.psum_scatter(g.astype(jnp.float32), "dp", scatter_dimension=g.ndim - 2, tiled=True) for g in grads
    )
    small_grads = lax.psum(small_grads, ("dp", "tensor"))
    row_grads, bqv_grads, bin_grads = unpack_small(small_grads, width_qv, width_in, piece_index, pieces)
    own_rows = pick(row_grads, flat_index, dp * pieces)
    return (
        output,
        grad_tokens,
        shard_wqkv,
        pick(bqv_grads, dp_index, dp),
        shard_out_t.T,
        shard_in,
        pick(bin_grads, dp_index, dp),
        shard_down_t.T,
        own_rows[:2],
        own_rows[2:],
    )


def solution(mesh):
    placed = (
        P(("dp", "tensor"), None),
        P("dp"),
        P(None, "dp", "tensor"),
        P(None, ("tensor", "dp")),
        P("tensor", "dp"),
        P(None, "dp", "tensor"),
        P(None, ("tensor", "dp")),
        P("tensor", "dp"),
        P(None, ("dp", "tensor")),
        P(None, ("dp", "tensor")),
        P(("dp", "tensor"), None),
    )

    def run(*args):
        dp = mesh.shape["dp"]
        direct = dp % 4 == 0 and (args[2].shape[1] // dp) % 16 == 0 and mesh.shape["tensor"] == 2
        return jax.shard_map(
            functools.partial(per_device, direct),
            mesh=mesh,
            in_specs=placed,
            out_specs=(
                P(("dp", "tensor"), None),
                P(("dp", "tensor"), None),
                P(None, "dp", "tensor"),
                P(None, ("tensor", "dp")),
                P("tensor", "dp"),
                P(None, "dp", "tensor"),
                P(None, ("tensor", "dp")),
                P("tensor", "dp"),
                P(None, ("dp", "tensor")),
                P(None, ("dp", "tensor")),
            ),
            check_vma=False,
        )(*args)

    return run
```

```python
import functools
import itertools

import jax
import jax.numpy as jnp
from jax import lax
from jax.experimental import pallas as pl
from jax.experimental.pallas import tpu as pltpu
from jax.sharding import PartitionSpec as P

HEAD = 64
MESH = pl.DeviceIdType.MESH
VMEM_LIMIT = 64 * 1024 * 1024 - 65536


class Grid3:
    def __init__(self, dp):
        self.nz = dp // 4
        self.slots = dp

    def here(self):
        me = lax.axis_index("dp")
        self.z, self.y, self.x = me // 4, (me // 2) % 2, me % 2
        z, nz = self.z, self.nz
        self.low, self.high = z > 0, z < nz - 1
        near = [sorted(range(1, nz), key=lambda k: (abs((p + k) % nz - p), k)) for p in range(nz)]
        self.by_distance = [(sum(jnp.where(z == p, near[p][j], 0) for p in range(nz)), 0, 0) for j in range(nz - 1)]
        self.line = []
        for d in self.by_distance:
            above = (z + d[0]) % nz > z
            self.line.append((above, jnp.where(above, z, nz - 1 - z) > 0))

    def at(self, dz, dy, dx):
        y = 1 - self.y if dy else self.y
        x = 1 - self.x if dx else self.x
        return (((self.z + dz) % self.nz) * 2 + y) * 2 + x

    def slot(self, d):
        return (d[0] % self.nz) * 4 + d[1] * 2 + d[2]

    def steps(self, axis):
        if axis == "z":
            return [(k, 0, 0) for k in range(1, self.nz)]
        return [(0, 1, 0)] if axis == "y" else [(0, 0, 1)]

    def seen_from(self, d, move):
        return ((d[0] - move[0] + self.nz) % self.nz, d[1] ^ move[1], d[2] ^ move[2])

    def span(self, axis):
        if axis == "z":
            return [(k, 0, 0) for k in range(self.nz)]
        return [(0, 0, 0), (0, 1, 0)] if axis == "y" else [(0, 0, 0), (0, 0, 1)]


def joined(*ds):
    return tuple(sum(part) for part in zip(*ds))


def remote(src, dst, send_sem, recv_sem, **device):
    return pltpu.make_async_remote_copy(
        src_ref=src, dst_ref=dst, send_sem=send_sem, recv_sem=recv_sem, device_id=device, device_id_type=MESH
    )


def greet(grid, partner):
    barrier = pltpu.get_barrier_semaphore()
    moves = [m for axis in "zyx" for m in grid.steps(axis)]
    for move in moves:
        pl.semaphore_signal(barrier, inc=1, device_id={"dp": grid.at(*move)}, device_id_type=MESH)
    pl.semaphore_signal(barrier, inc=1, device_id={"tensor": partner}, device_id_type=MESH)
    pl.semaphore_wait(barrier, len(moves) + 1)


class SmallSum:
    def __init__(self, grid, value, out, box, send, recv):
        self.grid = grid
        self.value, self.out, self.box, self.send, self.recv = value, out, box, send, recv
        self.copies = []

    def _post(self, slot, **device):
        copy = remote(self.out, self.box.at[slot], self.send.at[slot], self.recv.at[slot], **device)
        copy.start()
        self.copies.append(copy)

    def stage(self, number):
        grid = self.grid
        if number == 0:
            self.out[...] = self.value[...]
            self._post(0, tensor=1 - lax.axis_index("tensor"))
            return
        for copy in self.copies:
            copy.wait()
        self.copies = []
        if number == 1:
            self.out[...] = self.out[...] + self.box[0]
            self._post(1, dp=grid.at(0, 0, 1))
        elif number == 2:
            self.out[...] = self.out[...] + self.box[1]
            self._post(2, dp=grid.at(0, 1, 0))
        elif number == 3:
            self.out[...] = self.out[...] + self.box[2]
            for k in range(1, grid.nz):
                self._post(2 + k, dp=grid.at(k, 0, 0))
        else:
            total = self.out[...]
            for k in range(1, grid.nz):
                total = total + self.box[2 + k]
            self.out[...] = total


def small_slots(grid):
    return 2 + grid.nz


class Gather:
    def __init__(self, grid, chunks, send, recv):
        self.grid, self.chunks = grid, chunks
        self.send_sem, self.recv_sem = send, recv
        self.sent = []

    def _dst(self, number, d):
        rows = self.chunks[number][0].shape[0]
        return self.chunks[number][1].at[pl.ds(pl.multiple_of(self.grid.at(*d) * rows, rows), rows)]

    def _copy(self, number, d, move):
        dst = self._dst(number, d)
        if isinstance(move, int):
            move = (jnp.where(self.grid.line[move][0], -1, 1), 0, 0)
        source = self.chunks[number][0] if isinstance(d[0], int) and d == (0, 0, 0) else dst
        slot = self.grid.slot(self.grid.seen_from(d, move))
        return remote(source, dst, self.send_sem.at[number, slot], self.recv_sem.at[number, slot], dp=self.grid.at(*move))

    def _start(self, allowed, *args):
        if allowed is None:
            self._copy(*args).start()
        else:
            pl.when(allowed)(lambda: self._copy(*args).start())
        self.sent.append((allowed, args))

    def send(self, number, d, axis):
        if axis == "z":
            self._start(self.grid.low, number, d, (-1, 0, 0))
            self._start(self.grid.high, number, d, (1, 0, 0))
        else:
            self._start(None, number, d, self.grid.steps(axis)[0])

    def relay(self, number, d, j):
        self._start(self.grid.line[j][1], number, d, j)

    def arrive(self, number, d):
        dst, slot = self._dst(number, d), self.grid.slot(d)
        remote(dst, dst, self.send_sem.at[number, slot], self.recv_sem.at[number, slot], dp=self.grid.at(*d)).wait_recv()

    def moved(self, axis):
        return self.grid.by_distance if axis == "z" else self.grid.steps(axis)

    def first(self, number):
        return [(self.pass_first, number, d, j) for j, d in enumerate(self.moved(self.chunks[number][2][0]))]

    def second(self, number):
        one, two = self.chunks[number][2][:2]
        return [
            (self.pass_second, number, joined(a, b), j) for j, b in enumerate(self.moved(two)) for a in self.grid.span(one)
        ]

    def third(self, number):
        one, two, three = self.chunks[number][2]
        return [joined(a, b, c) for a in self.grid.span(one) for b in self.grid.span(two) for c in self.grid.steps(three)]

    def pass_first(self, number, d, j):
        order = self.chunks[number][2]
        self.arrive(number, d)
        if order[0] == "z":
            self.relay(number, d, j)
        for axis in order[1:]:
            self.send(number, d, axis)

    def pass_second(self, number, d, j):
        order = self.chunks[number][2]
        self.arrive(number, d)
        if order[1] == "z":
            self.relay(number, d, j)
        self.send(number, d, order[2])

    def finish(self, number):
        for d in self.third(number):
            self.arrive(number, d)

    def drain(self):
        for allowed, args in self.sent:
            if allowed is None:
                self._copy(*args).wait_send()
            else:
                pl.when(allowed)(lambda args=args: self._copy(*args).wait_send())
        self.sent = []


class Scatter:
    def __init__(self, grid, rows, chunks, send, recv):
        self.grid, self.rows, self.chunks = grid, rows, chunks
        self.send_sem, self.recv_sem = send, recv
        self.sent = []
        self.far_first = [2, 1, 3] if grid.nz == 4 else list(range(1, grid.nz))
        self.second, self.line = 2 * grid.nz, 3 * grid.nz - 1

    def part(self, number, d):
        return self.chunks[number][0].at[pl.ds(pl.multiple_of(self.grid.at(*d) * self.rows, self.rows), self.rows)]

    def box(self, number, slot):
        return self.chunks[number][3].at[slot]

    def other(self, number):
        return "y" if self.chunks[number][2] == "x" else "x"

    def place(self, number, dz, e):
        return (dz, e, 0) if self.other(number) == "y" else (dz, 0, e)

    def _copy(self, number, kind, dz, e=0):
        grid = self.grid
        if kind == "own":
            move = grid.steps(self.chunks[number][2])[0]
            source, slot = self.part(number, joined(self.place(number, dz, e), move)), dz * 2 + e
        elif kind == "side":
            move = grid.steps(self.other(number))[0]
            source, slot = self.box(number, dz * 2 + 1), self.second + dz
        else:
            move = (dz, 0, 0)
            source, slot = self.box(number, dz * 2), self.line + dz
        return remote(
            source, self.box(number, slot), self.send_sem.at[number, slot], self.recv_sem.at[number, slot], dp=grid.at(*move)
        )

    def _send(self, *args):
        self._copy(*args).start()
        self.sent.append(args)

    def _arrive(self, number, slot):
        box = self.box(number, slot)
        remote(box, box, self.send_sem.at[number, slot], self.recv_sem.at[number, slot], dp=0).wait_recv()

    def begin(self, number, *halves):
        for e in halves or (1, 0):
            for dz in self.far_first + [0]:
                self._send(number, "own", dz, e)

    def held(self, number, dz, e):
        slot = dz * 2 + e
        self._arrive(number, slot)
        return self.part(number, self.place(number, dz, e))[...].astype(jnp.float32) + self.box(number, slot)[...].astype(jnp.float32)

    def side(self, number, dz):
        self.box(number, dz * 2 + 1)[...] = self.held(number, dz, 1).astype(jnp.bfloat16)
        self._send(number, "side", dz)

    def both(self, number, dz):
        value = self.held(number, dz, 0)
        self._arrive(number, self.second + dz)
        return value + self.box(number, self.second + dz)[...].astype(jnp.float32)

    def along(self, number, dz):
        self.box(number, dz * 2)[...] = self.both(number, dz).astype(jnp.bfloat16)
        self._send(number, "line", dz)

    def sides(self, *numbers):
        return [(self.side, n, dz) for dz in self.far_first + [0] for n in numbers]

    def lines(self, *numbers):
        return [(self.along, n, dz) for dz in self.far_first for n in numbers]

    def lasts(self, *numbers):
        return [(self.last, n) for n in numbers]

    def last(self, number):
        total = self.both(number, 0)
        for dz in self.far_first:
            self._arrive(number, self.line + dz)
            total = total + self.box(number, self.line + dz)[...].astype(jnp.float32)
        self.chunks[number][1][...] = total

    def drain(self):
        for args in self.sent:
            self._copy(*args).wait_send()
        self.sent = []


def scatter_slots(grid):
    return 4 * grid.nz - 1
bf16, f32 = jnp.bfloat16, jnp.float32
NORM_EPSILON = 1e-06
EARLY = 4
AFTER_PROJECTION = 4
GATHER_STEPS = 4
AFTER_OUT = 4
AFTER_NORM = 4
ROOT_HALF = 0.7071067811865476
PHI_SCALE = 0.3989422804014327


def nn(a, b):
    return jnp.dot(a, b, preferred_element_type=f32)


def nt(a, b):
    return lax.dot_general(a, b, (((1,), (1,)), ((), ())), preferred_element_type=f32)


def aligned(start, size):
    return pl.ds(pl.multiple_of(start, size), size)


def unit_rows(values):
    centred = values - jnp.mean(values, axis=-1, keepdims=True)
    variance = jnp.mean(centred * centred, axis=-1, keepdims=True)
    scale = lax.rsqrt(variance + NORM_EPSILON)
    return centred * scale, scale


def unit_back(grad_unit, unit, scale):
    inner = (
        grad_unit
        - jnp.mean(grad_unit, axis=-1, keepdims=True)
        - unit * jnp.mean(grad_unit * unit, axis=-1, keepdims=True)
    )
    return inner * scale


def fold(rows):
    return jnp.sum(rows.reshape(rows.shape[0] // 8, 8, rows.shape[1]), axis=0)


def merged(*lists):
    return [entry for row in itertools.zip_longest(*lists) for entry in row if entry is not None]


class Pump:
    def __init__(self, steps=()):
        self.steps = list(steps)

    def take(self, count=None):
        count = len(self.steps) if count is None else min(count, len(self.steps))
        taken, self.steps = self.steps[:count], self.steps[count:]
        return taken

    def run(self, count=None):
        for function, *args in self.take(count):
            function(*args)


def at_trips(*shares):
    def run(index):
        for trip, share in enumerate(shares):

            @pl.when(index == trip)
            def _(share=share):
                Pump(share).run()

    return run


def layer_body(
    grid, rows,
    tokens, cotangent, length, slopes, qv_part, ko_part, in_part, low_part, high_part, small,
    output, grad_tokens, to_qv, to_ko, to_in, to_low, to_high, small_grads, probs_far,
    w_qv, w_ko, w_gate, w_up, w_low, w_high, small_pair, small_tiles, every_small, small_box,
    x, qkv, inverse, mixed, work, key_aug, value_aug, query_aug,
    rows_f32, attended_low, branch_rows, outgoing, incoming, cot, turned,
    grad_t, pair_b, grad_value_t, grad_key_t,
    g_qv, g_ko, g_gate, g_up, g_low, g_high, box_qv, box_ko, box_gate, box_up, box_low, box_high,
    gather_send, gather_recv, scatter_send, scatter_recv, small_send, small_recv, own_sem, swap_send, swap_recv, local_sem, prob_sem,
):
    grid.here()
    side = lax.axis_index("tensor")
    other = 1 - side
    half = tokens.shape[0]
    slots = 2 * half
    width = tokens.shape[1]
    heads_wide = mixed.shape[1]
    units = w_gate.shape[1]
    mine = aligned(side * half, half)
    count = length[0]
    attended, unit_one = rows_f32.at[:, pl.ds(0, width)], rows_f32.at[:, pl.ds(width, width)]
    scale_one = rows_f32.at[:, pl.ds(2 * width, 128)]
    block = 256
    span = 2 * slots - block
    bias = rows_f32.at[pl.ds(0, block), pl.ds(0, span)]

    greet(grid, other)

    gather = Gather(grid, [
        (qv_part, w_qv, "zyx"),
        (ko_part, w_ko, "zxy"),
        (in_part.at[0], w_gate, "yzx"),
        (in_part.at[1], w_up, "xzy"),
        (low_part, w_low, "zyx"),
        (high_part, w_high, "zxy"),
        (small_pair, small_tiles, "zyx"),
    ], gather_send, gather_recv)
    scatter = Scatter(grid, rows, [
        (g_qv, to_qv, "x", box_qv),
        (g_ko, to_ko, "y", box_ko),
        (g_gate, to_in.at[0], "x", box_gate),
        (g_up, to_in.at[1], "y", box_up),
        (g_low, to_low, "x", box_low),
        (g_high, to_high, "y", box_high),
    ], scatter_send, scatter_recv)
    QV, KO, GATE, UP, LOW, HIGH, SMALL = range(7)

    def swap(source, target, slot):
        copy = remote(source, target, swap_send.at[slot], swap_recv.at[slot], tensor=other)
        copy.start()
        return copy

    token_swap = swap(tokens, x.at[mine], 0)
    token_copy = pltpu.make_async_copy(tokens, x.at[mine], local_sem.at[0])
    token_copy.start()
    cot_copy = pltpu.make_async_copy(cotangent, cot, local_sem.at[1])
    cot_copy.start()
    my_small = small_pair.at[:, pl.ds(pl.multiple_of(side * 128, 128), 128)]
    small_copy = pltpu.make_async_copy(small, my_small, local_sem.at[4])
    small_copy.start()
    small_swap = swap(small, my_small, 8)
    own_copies = []
    for n, (source, target, _) in enumerate(gather.chunks[:SMALL]):
        copy = pltpu.make_async_copy(source, target.at[aligned(grid.at(0, 0, 0) * rows, rows)], own_sem.at[n])
        copy.start()
        own_copies.append(copy)
        for axis in gather.chunks[n][2]:
            gather.send(n, (0, 0, 0), axis)
        if n == KO:
            small_copy.wait()
            small_swap.wait()
            for axis in gather.chunks[SMALL][2]:
                gather.send(SMALL, (0, 0, 0), axis)
            small_tiles[aligned(grid.at(0, 0, 0) * 16, 16), :] = small_pair[...]
    near_units = merged(gather.second(GATE), gather.second(UP))
    ends_first = merged(gather.first(LOW), gather.first(HIGH))
    ends_second = merged(gather.second(LOW), gather.second(HIGH))
    early = (
        merged(gather.first(QV), gather.first(SMALL), gather.first(KO))
        + merged(gather.first(GATE), gather.first(UP))
        + merged(merged(gather.second(QV), gather.second(SMALL), gather.second(KO)), near_units[:EARLY])
    )
    pump = Pump(early)
    pump.run()
    pump = Pump(merged(near_units[EARLY:], ends_first) + ends_second)
    for copy in own_copies:
        copy.wait()
    token_copy.wait()
    token_swap.wait()
    for number in (SMALL, QV, KO):
        gather.finish(number)

    norm_rows = jnp.zeros((8, width), f32)
    head_rows = jnp.zeros((8, heads_wide), f32)
    unit_rows_in = jnp.zeros((8, units), f32)

    def at_lanes(tile, lanes, start):
        wide = jnp.concatenate([tile, jnp.zeros((8, lanes - 128), f32)], axis=1)
        return pltpu.roll(wide, start, 1) if start else wide

    for i in range(grid.slots):
        pair_tile = [small_tiles[16 * i : 16 * i + 8, 128 * s : 128 * s + 128] for s in range(2)]
        unit_tile = [small_tiles[16 * i + 8 : 16 * i + 16, 128 * s : 128 * s + 128] for s in range(2)]
        for s in range(2):
            norm_rows = norm_rows + at_lanes(pair_tile[s], width, (2 * i + s) * (rows // 2))
        units_here = jnp.where(side == 0, unit_tile[0], unit_tile[1])
        unit_rows_in = unit_rows_in + at_lanes(units_here, units, i * (units // grid.slots))
        head_rows = head_rows + at_lanes(pltpu.roll(units_here, 6, 0), heads_wide, i * (heads_wide // grid.slots))
    every_small[0:8, :] = norm_rows
    every_small[8:9, pl.ds(0, heads_wide)] = head_rows[0:1, :]
    every_small[8:9, pl.ds(heads_wide, heads_wide)] = head_rows[1:2, :]
    turned[0:8, :] = unit_rows_in

    q_cols, v_cols, k_cols = (pl.ds(i * heads_wide, heads_wide) for i in range(3))
    side_cols = pl.ds(pl.multiple_of(side * heads_wide, 128), heads_wide)
    row_bias = every_small[8:9, :]
    row_scale = jnp.where(lax.broadcasted_iota(jnp.int32, (1, 2 * heads_wide), 1) < heads_wide, 0.125, 1.0)

    @pl.loop(0, slots // 256)
    def _(i):
        r = aligned(i * 256, 256)
        raw = (nn(x[r, :], w_qv[...]) + row_bias).astype(bf16)
        qkv[r, pl.ds(0, 2 * heads_wide)] = (raw.astype(f32) * row_scale).astype(bf16)
        qkv[r, k_cols] = nn(x[r, :], w_ko[:, pl.ds(0, heads_wide)]).astype(bf16)

    pump.run(AFTER_PROJECTION)

    lane = lax.broadcasted_iota(jnp.int32, (slots, 128), 1)
    slot = lax.broadcasted_iota(jnp.int32, (slots, 128), 0)
    key_mask = jnp.where(slot < count, 0.0, -1e30).astype(bf16)
    zero, one = jnp.zeros((), bf16), jnp.ones((), bf16)
    block_lane = lax.broadcasted_iota(jnp.int32, (block, 128), 1)
    pairs = heads_wide // 128

    def prob_slot(upper):
        return work.at[:, pl.ds(upper * slots, slots)]

    def prob_out(pair, upper):
        return pltpu.make_async_copy(prob_slot(upper), probs_far.at[2 * pair + upper], prob_sem.at[upper])

    def prob_in(pair, upper):
        return pltpu.make_async_copy(probs_far.at[2 * pair + upper], prob_slot(upper), prob_sem.at[upper])

    def pair_cols(pair, start=0):
        return pl.ds(pl.multiple_of(start + pair * 128, 128), 128)

    def attend_pair(pair):
        cols = pair_cols(pair)
        for upper in (0, 1):
            own = (lane >= 64) == (upper == 1)
            spare = 0 if upper else 64
            gap = jnp.abs(
                lax.broadcasted_iota(jnp.int32, (block, span), 0)
                - (lax.broadcasted_iota(jnp.int32, (block, span), 1) - (span - slots))
            )
            bias[...] = gap.astype(f32) * slopes[2 * pair + upper]
            key_aug[...] = jnp.where(own, qkv[:, pair_cols(pair, 2 * heads_wide)], jnp.where(lane == spare, key_mask, zero))
            value_aug[...] = jnp.where(own, qkv[:, pair_cols(pair, heads_wide)], one)
            query_aug[...] = jnp.where(own, qkv[:, cols], jnp.where(lane == spare, one, zero))

            @pl.when(pair > 0)
            def _(upper=upper):
                prob_out(pair - 1, upper).wait()

            def attend(i, inner_carry, upper=upper):
                r = aligned(i * block, block)
                scores = nt(query_aug[r, :], key_aug[...]) - bias[:, pl.ds(pl.multiple_of(span - slots - i * block, block), slots)]
                top = jnp.max(scores, axis=1, keepdims=True)
                weights = jnp.exp(scores - top).astype(bf16)
                work[r, pl.ds(upper * slots, slots)] = weights
                product = nn(weights, value_aug[...])
                scale = 1.0 / (product[:, 0:1] if upper else product[:, 64:65])
                result = (product * scale).astype(bf16)
                inverse[r, :] = jnp.where(block_lane == 2 * pair + upper, scale, inverse[r, :])
                mixed[r, cols] = jnp.where(block_lane < 64, mixed[r, cols], result) if upper else result
                return inner_carry

            lax.fori_loop(0, slots // block, attend, 0, unroll=2)
            prob_out(pair, upper).start()
        between_pairs(pair)

    inverse[...] = jnp.zeros_like(inverse)
    between_pairs = at_trips(*(pump.take(GATHER_STEPS) for _ in range(pairs)))
    pl.loop(0, pairs)(attend_pair)

    def project(source, weights, target_rows, sink):
        @pl.loop(0, half // 256)
        def _(i):
            r = aligned(target_rows * half + i * 256, 256)
            sink(i, nt(source[r, :], weights[...]))

    def to_outgoing(i, value):
        outgoing[aligned(i * 256, 256), :] = value.astype(bf16)

    def to_attended(i, value):
        attended[aligned(i * 256, 256), :] = value

    w_out = w_ko.at[:, pl.ds(heads_wide, heads_wide)]
    project(mixed, w_out, other, to_outgoing)
    first_swap = swap(outgoing, incoming.at[0], 1)
    pump.run(AFTER_OUT)
    project(mixed, w_out, side, to_attended)
    first_swap.wait()
    gain_one, gain_two = every_small[0:1, :], every_small[1:2, :]
    step = 64

    @pl.loop(0, half // step)
    def _(i):
        r = aligned(i * step, step)
        own = pl.ds(pl.multiple_of(side * half + i * step, step), step)
        total = x[own, :].astype(f32) + attended[r, :] + incoming[0, r, :].astype(f32) + every_small[2:3, :]
        unit, scale = unit_rows(total)
        result = unit * gain_one + every_small[3:4, :]
        unit_one[r, :] = unit
        scale_one[r, :] = jnp.broadcast_to(scale, (step, 128))
        attended[r, :] = result
        attended_low[own, :] = result.astype(bf16)

    low_swap = swap(attended_low.at[mine], attended_low.at[mine], 2)
    for upper in (0, 1):
        prob_out(pairs - 1, upper).wait()
    pump.run(AFTER_NORM)
    gather.finish(GATE)
    gather.finish(UP)

    def feed(rows_side):
        r = aligned(rows_side * half, half)

        @pl.loop(0, units // 256)
        def _(j):
            c = aligned(j * 256, 256)
            c_up = pl.ds(pl.multiple_of(units + j * 256, 256), 256)
            c_hidden = pl.ds(pl.multiple_of(2 * units + j * 256, 256), 256)
            gate = nn(attended_low[r, :], w_gate[:, c]) + turned[0:1, c]
            up = nn(attended_low[r, :], w_up[:, c]) + turned[1:2, c]
            below = 0.5 * (1.0 + lax.erf(gate * ROOT_HALF))
            density = PHI_SCALE * jnp.exp(-0.5 * gate * gate)
            bent = gate * below
            work[r, c_hidden] = (bent * up).astype(bf16)
            work[r, c] = (up * (below + gate * density)).astype(bf16)
            work[r, c_up] = bent.astype(bf16)

    feed(side)
    pump.run()
    low_swap.wait()
    feed(other)
    pump.run()
    gather.finish(LOW)
    gather.finish(HIGH)

    hidden_low, hidden_high = pl.ds(2 * units, units // 2), pl.ds(2 * units + units // 2, units // 2)

    def down(rows_side, sink):
        @pl.loop(0, half // 256)
        def _(i):
            r = aligned(rows_side * half + i * 256, 256)
            sink(i, nt(work[r, hidden_low], w_low[...]) + nt(work[r, hidden_high], w_high[...]))

    def add_attended(i, value):
        r = aligned(i * 256, 256)
        attended[r, :] = attended[r, :] + value

    down(other, to_outgoing)
    second_swap = swap(outgoing, incoming.at[1], 3)
    down(side, add_attended)
    cot_copy.wait()
    second_swap.wait()
    nothing = jnp.zeros((8, width), f32)

    def second_norm(i, carry):
        sum_gain, sum_shift, sum_branch = carry
        r = aligned(i * step, step)
        own = pl.ds(pl.multiple_of(side * half + i * step, step), step)
        position = side * half + i * step + lax.broadcasted_iota(jnp.int32, (step, 1), 0)
        valid = jnp.where(position < count, 1.0, 0.0)
        unit, scale = unit_rows(attended[r, :] + incoming[1, r, :].astype(f32) + every_small[4:5, :])
        grad = cot[r, :].astype(f32) * valid
        cot[r, :] = ((unit * gain_two + every_small[5:6, :]) * valid).astype(bf16)
        back = unit_back(grad * gain_two, unit, scale)
        attended[r, :] = back
        branch_rows[own, :] = back.astype(bf16)
        return sum_gain + fold(grad * unit), sum_shift + fold(grad), sum_branch + fold(back)

    gain_two_sum, shift_two_sum, down_bias_sum = lax.fori_loop(0, half // step, second_norm, (nothing,) * 3)
    branch_swap = swap(branch_rows.at[mine], branch_rows.at[mine], 4)
    output_copy = pltpu.make_async_copy(cot, output, local_sem.at[2])
    output_copy.start()
    small_grads[...] = jnp.zeros_like(small_grads)
    small_grads[1:2, :] = jnp.sum(gain_two_sum, axis=0, keepdims=True)
    small_grads[5:6, :] = jnp.sum(shift_two_sum, axis=0, keepdims=True)
    small_grads[4:5, :] = jnp.sum(down_bias_sum, axis=0, keepdims=True)
    branch_swap.wait()

    def turn(source):
        @pl.loop(0, slots // 256)
        def _(i):
            r = aligned(i * 256, 256)
            grad_t[:, r] = source[r, :].T

    def weight_grad(sink, source, source_start, tile):
        @pl.loop(0, sink.shape[1] // tile)
        def _(j):
            sink[:, aligned(j * tile, tile)] = nn(
                grad_t[...], source[:, pl.ds(pl.multiple_of(source_start + j * tile, tile), tile)]
            ).astype(bf16)

    turn(branch_rows)
    weight_grad(g_low, work, 2 * units, 256)
    scatter.begin(LOW)
    weight_grad(g_high, work, 2 * units + units // 2, 256)
    scatter.begin(HIGH)

    turned[8:24, :] = jnp.zeros((16, units), f32)
    for index, weights in enumerate((w_low, w_high)):
        @pl.loop(0, units // 2 // 256)
        def _(j, index=index, weights=weights):
            c = pl.ds(pl.multiple_of(index * (units // 2) + j * 256, 256), 256)
            c_up = pl.ds(pl.multiple_of(units + index * (units // 2) + j * 256, 256), 256)
            for part in range(2):
                r = pl.ds(part * half, half)
                grad = nn(branch_rows[r, :], weights[:, aligned(j * 256, 256)])
                gate_grad = (grad * work[r, c].astype(f32)).astype(bf16)
                up_grad = (grad * work[r, c_up].astype(f32)).astype(bf16)
                work[r, c] = gate_grad
                work[r, c_up] = up_grad
                turned[8:16, c] = turned[8:16, c] + fold(gate_grad.astype(f32))
                turned[16:24, c] = turned[16:24, c] + fold(up_grad.astype(f32))

    for index in range(2):
        total = jnp.sum(turned[8 + 8 * index : 16 + 8 * index, :], axis=0, keepdims=True)
        for j in range(units // width):
            small_grads[pl.ds(8 + 4 * index + 2 * side + j, 1), :] = total[:, j * width : (j + 1) * width]

    Pump(scatter.sides(LOW, HIGH)).run()
    turn(attended_low)
    weight_grad(g_gate, work, 0, 512)
    scatter.begin(GATE, 1)
    weight_grad(g_up, work, units, 512)
    scatter.begin(UP, 1)
    scatter.begin(GATE, 0)

    gate_cols, up_cols = pl.ds(0, units), pl.ds(units, units)

    def units_back(rows_side, sink):
        @pl.loop(0, half // 256)
        def _(i):
            r = aligned(rows_side * half + i * 256, 256)
            sink(i, nt(work[r, gate_cols], w_gate[...]) + nt(work[r, up_cols], w_up[...]))

    units_back(other, to_outgoing)
    third_swap = swap(outgoing, incoming.at[0], 5)
    units_back(side, add_attended)
    Pump(scatter.lines(LOW, HIGH)).run()
    third_swap.wait()

    def first_norm_back(i, carry):
        sum_gain, sum_shift, sum_branch = carry
        r = aligned(i * step, step)
        own = pl.ds(pl.multiple_of(side * half + i * step, step), step)
        grad = attended[r, :] + incoming[0, r, :].astype(f32)
        unit = unit_one[r, :]
        back = unit_back(grad * gain_one, unit, scale_one[r, 0:1])
        attended[r, :] = back
        branch_rows[own, :] = back.astype(bf16)
        return sum_gain + fold(grad * unit), sum_shift + fold(grad), sum_branch + fold(back)

    prob_in(0, 0).start()
    prob_in(0, 1).start()
    gain_one_sum, shift_one_sum, out_bias_sum = lax.fori_loop(0, half // step, first_norm_back, (nothing,) * 3)
    attn_swap = swap(branch_rows.at[mine], branch_rows.at[mine], 6)
    small_grads[0:1, :] = jnp.sum(gain_one_sum, axis=0, keepdims=True)
    small_grads[3:4, :] = jnp.sum(shift_one_sum, axis=0, keepdims=True)
    small_grads[2:3, :] = jnp.sum(out_bias_sum, axis=0, keepdims=True)
    attn_swap.wait()

    grad_mixed = attended_low.at[:, pl.ds(0, heads_wide)]
    turn(branch_rows)
    g_ko[:, pl.ds(heads_wide, heads_wide)] = nn(grad_t[...], mixed[...]).astype(bf16)
    sides_gate = Pump(scatter.sides(GATE))
    sides_gate.run(2)

    @pl.loop(0, slots // 256)
    def _(i):
        r = aligned(i * 256, 256)
        grad_mixed[r, :] = nn(branch_rows[r, :], w_out[...]).astype(bf16)

    sides_gate.run()
    scatter.begin(UP, 0)

    mixed_t, query_t = pair_b.at[0], pair_b.at[1]

    def pair_back(pair):
        cols, key_cols, value_cols = pair_cols(pair), pair_cols(pair, 2 * heads_wide), pair_cols(pair, heads_wide)
        scales = inverse[...]
        shrink = jnp.where(
            lane < 64,
            jnp.sum(jnp.where(lane == 2 * pair, scales, 0.0), axis=1, keepdims=True),
            jnp.sum(jnp.where(lane == 2 * pair + 1, scales, 0.0), axis=1, keepdims=True),
        )
        scaled = (grad_mixed[:, cols].astype(f32) * shrink).astype(bf16)
        mixed_t[...] = scaled.T
        query_t[...] = qkv[:, cols].T
        outgoing_pair[...] = scaled
        for upper in (0, 1):
            own = (lane >= 64) == (upper == 1)
            spare = 0 if upper else 64
            scaled = outgoing_pair[...]
            dots = jnp.sum(jnp.where(own, scaled.astype(f32) * mixed[:, cols].astype(f32), 0.0), axis=1, keepdims=True)
            dots_high = dots.astype(bf16)
            dots_low = (dots - dots_high.astype(f32)).astype(bf16)
            ones = (lane == spare) | (lane == spare + 1)
            value_aug[...] = jnp.where(own, qkv[:, value_cols], jnp.where(ones, one, zero))
            query_aug[...] = jnp.where(
                own, scaled, jnp.where(lane == spare, -dots_high, jnp.where(lane == spare + 1, -dots_low, zero))
            )
            part = pl.ds(64 * upper, 64)
            base = upper * slots
            prob_in(pair, upper).wait()
            for j in range(slots // 512):
                c = pl.ds(j * 512, 512)
                grad_value_t[part, c] = nn(mixed_t[part, :], work[:, pl.ds(base + j * 512, 512)]).astype(bf16)

            def attend_back(i, inner_carry, upper=upper, base=base):
                r = aligned(i * block, block)
                inner = nt(query_aug[r, :], value_aug[...])
                grads = (work[r, pl.ds(base, slots)].astype(f32) * inner).astype(bf16)
                work[r, pl.ds(base, slots)] = grads
                result = (nn(grads, qkv[:, key_cols]) * 0.125).astype(bf16)
                qkv[r, cols] = jnp.where(block_lane < 64, qkv[r, cols], result) if upper else result
                return inner_carry

            lax.fori_loop(0, slots // block, attend_back, 0, unroll=2)
            for j in range(slots // 512):
                c = pl.ds(j * 512, 512)
                grad_key_t[part, c] = nn(query_t[part, :], work[:, pl.ds(base + j * 512, 512)]).astype(bf16)

            @pl.when(pair + 1 < pairs)
            def _(upper=upper):
                prob_in(pair + 1, upper).start()

        qkv[:, value_cols] = grad_value_t[...].T
        qkv[:, key_cols] = grad_key_t[...].T
        between_pairs(pair)

    outgoing_pair = key_aug
    between_pairs = at_trips(scatter.sides(UP), scatter.lasts(LOW, HIGH), scatter.lines(GATE))
    pl.loop(0, pairs)(pair_back)

    turn(x)
    g_qv[...] = nn(grad_t[...], qkv[:, pl.ds(0, 2 * heads_wide)]).astype(bf16)
    scatter.begin(QV)
    g_ko[:, pl.ds(0, heads_wide)] = nn(grad_t[...], qkv[:, k_cols]).astype(bf16)
    scatter.begin(KO)
    def column_sum(cols):
        def add(i, carry):
            return carry + fold(qkv[aligned(i * 128, 128), cols].astype(f32))

        return jnp.sum(lax.fori_loop(0, slots // 128, add, jnp.zeros((8, heads_wide), f32)), axis=0, keepdims=True)

    small_grads[6:7, side_cols] = column_sum(q_cols)
    small_grads[7:8, side_cols] = column_sum(v_cols)
    sums = SmallSum(grid, small_grads, small_grads, small_box, small_send, small_recv)
    sums.stage(0)

    def inputs_back(rows_side, sink):
        @pl.loop(0, half // 256)
        def _(i):
            r = aligned(rows_side * half + i * 256, 256)
            sink(
                i,
                nt(qkv[r, pl.ds(0, 2 * heads_wide)], w_qv[...]) + nt(qkv[r, k_cols], w_ko[:, pl.ds(0, heads_wide)]),
            )

    inputs_back(other, to_outgoing)
    fourth_swap = swap(outgoing, incoming.at[1], 7)
    sums.stage(1)
    inputs_back(side, add_attended)
    fourth_swap.wait()

    @pl.loop(0, half // step)
    def _(i):
        r = aligned(i * step, step)
        attended[r, :] = attended[r, :] + incoming[1, r, :].astype(f32)

    tokens_copy = pltpu.make_async_copy(attended, grad_tokens, local_sem.at[3])
    tokens_copy.start()
    sums.stage(2)
    Pump(scatter.lines(UP) + scatter.sides(QV, KO)).run()
    sums.stage(3)
    Pump(scatter.lasts(GATE, UP) + scatter.lines(QV, KO) + scatter.lasts(QV, KO)).run()
    sums.stage(4)
    output_copy.wait()
    tokens_copy.wait()
    gather.drain()
    scatter.drain()


def layer_call(grid, tokens, cotangent, lengths, slopes, qv_part, ko_part, in_part, low_part, high_part, small):
    rows, wide = qv_part.shape
    width = rows * grid.nz * 4
    half = tokens.shape[0]
    slots = 2 * half
    heads_wide = wide // 2
    units = in_part.shape[2]
    heads = heads_wide // HEAD
    shapes = [
        jax.ShapeDtypeStruct((half, width), bf16),
        jax.ShapeDtypeStruct((half, width), f32),
        jax.ShapeDtypeStruct(qv_part.shape, f32),
        jax.ShapeDtypeStruct(ko_part.shape, f32),
        jax.ShapeDtypeStruct(in_part.shape, f32),
        jax.ShapeDtypeStruct(low_part.shape, f32),
        jax.ShapeDtypeStruct(high_part.shape, f32),
        jax.ShapeDtypeStruct((16, width), f32),
        jax.ShapeDtypeStruct((heads, slots, slots), bf16),
    ]
    vmem = pl.BlockSpec(memory_space=pltpu.VMEM)
    smem = pl.BlockSpec(memory_space=pltpu.SMEM)
    anywhere = pl.BlockSpec(memory_space=pl.ANY)
    smalls = small_slots(grid)
    dma = pltpu.SemaphoreType.DMA
    wides = (wide, wide, units, units, units // 2, units // 2)
    scratch = (
        [pltpu.VMEM((width, w), bf16) for w in wides]
        + [
            pltpu.VMEM((16, 256), f32),
            pltpu.VMEM((16 * grid.slots, 256), f32),
            pltpu.VMEM((16, width), f32),
            pltpu.VMEM((smalls, 16, width), f32),
            pltpu.VMEM((slots, width), bf16),
            pltpu.VMEM((slots, 3 * heads_wide), bf16),
            pltpu.VMEM((slots, 128), f32),
            pltpu.VMEM((slots, heads_wide), bf16),
            pltpu.VMEM((slots, 3 * units), bf16),
            pltpu.VMEM((slots, 128), bf16),
            pltpu.VMEM((slots, 128), bf16),
            pltpu.VMEM((slots, 128), bf16),
            pltpu.VMEM((half, max(2 * slots - 256, 2 * width + 128)), f32),
            pltpu.VMEM((slots, width), bf16),
            pltpu.VMEM((slots, width), bf16),
            pltpu.VMEM((half, width), bf16),
            pltpu.VMEM((2, half, width), bf16),
            pltpu.VMEM((half, width), bf16),
            pltpu.VMEM((24, units), f32),
            pltpu.VMEM((width, slots), bf16),
            pltpu.VMEM((2, 128, slots), bf16),
            pltpu.VMEM((128, slots), bf16),
            pltpu.VMEM((128, slots), bf16),
        ]
        + [pltpu.VMEM((width, w), bf16) for w in wides]
        + [pltpu.VMEM((scatter_slots(grid), rows, w), bf16) for w in wides]
        + [
            dma((7, grid.slots)),
            dma((7, grid.slots)),
            dma((6, scatter_slots(grid))),
            dma((6, scatter_slots(grid))),
            dma((smalls,)),
            dma((smalls,)),
            dma((6,)),
            dma((9,)),
            dma((9,)),
            dma((5,)),
            dma((2,)),
        ]
    )
    results = pl.pallas_call(
        functools.partial(layer_body, grid, rows),
        out_shape=shapes,
        in_specs=[anywhere, anywhere, smem, smem] + [anywhere] * 6,
        out_specs=[anywhere] * 2 + [vmem] * 6 + [anywhere],
        scratch_shapes=scratch,
        compiler_params=pltpu.CompilerParams(collective_id=0, has_side_effects=True, vmem_limit_bytes=VMEM_LIMIT),
        name="layer",
    )(tokens, cotangent, lengths, slopes, qv_part, ko_part, in_part, low_part, high_part, small)
    return results[:8]


norm_epsilon = 1e-06


def norm_forward(values, gain_row, shift_row):
    centred = values - jnp.mean(values, axis=-1, keepdims=True)
    variance = jnp.mean(centred * centred, axis=-1, keepdims=True)
    inv_scale = lax.rsqrt(variance + norm_epsilon)
    unit_vals = centred * inv_scale
    return (unit_vals * gain_row + shift_row, unit_vals, inv_scale)


def norm_backward(grad_out, unit_vals, inv_scale, gain_row):
    grad_unit = grad_out * gain_row
    inner_term = (
        grad_unit
        - jnp.mean(grad_unit, axis=-1, keepdims=True)
        - unit_vals * jnp.mean(grad_unit * unit_vals, axis=-1, keepdims=True)
    )
    return (
        inner_term * inv_scale,
        jnp.sum(grad_out * unit_vals, axis=0),
        jnp.sum(grad_out, axis=0),
    )


def score_block(query_block, first_row, key_heads, slopes, key_valid):
    block_size = query_block.shape[0]
    heads_here = slopes.shape[0]
    query_heads = query_block.reshape(block_size, heads_here, HEAD)
    raw_scores = jnp.einsum(
        "qhc,khc->hqk", query_heads, key_heads, preferred_element_type=jnp.float32
    )
    query_pos = first_row + lax.iota(jnp.int32, block_size)
    key_pos = lax.iota(jnp.int32, key_heads.shape[0])
    distance = jnp.abs(query_pos[:, None] - key_pos[None, :]).astype(jnp.float32)
    scores = 0.125 * raw_scores - slopes[:, None, None] * distance[None, :, :]
    return (jnp.where(key_valid[None, None, :], scores, -1e30), query_heads)


def attend(queries, key_rows, value_rows, slopes, key_valid):
    slot_count, width_here = queries.shape
    heads_here = width_here // HEAD
    block_size = min(512, slot_count)
    key_heads = key_rows.reshape(slot_count, heads_here, HEAD)
    value_heads = value_rows.reshape(slot_count, heads_here, HEAD)

    def one_block(first_row):
        query_block = lax.dynamic_slice_in_dim(queries, first_row, block_size, 0)
        scores, query_heads = score_block(query_block, first_row, key_heads, slopes, key_valid)
        row_max = jnp.max(scores, axis=-1, keepdims=True)
        exp_scores = jnp.exp(scores - row_max)
        row_total = jnp.sum(exp_scores, axis=-1, keepdims=True)
        weights = (exp_scores / row_total).astype(jnp.bfloat16)
        mixed_block = jnp.einsum(
            "hqk,khc->qhc", weights, value_heads, preferred_element_type=jnp.float32
        )
        return (
            mixed_block.reshape(block_size, width_here).astype(jnp.bfloat16),
            (row_max + jnp.log(row_total))[..., 0],
        )

    first_rows = lax.iota(jnp.int32, slot_count // block_size) * block_size
    mixed_heads, logsum = lax.map(one_block, first_rows)
    return (mixed_heads.reshape(slot_count, width_here), logsum)


def attend_back(queries, key_rows, value_rows, grad_mixed, logsum, slopes, key_valid):
    slot_count, width_here = queries.shape
    heads_here = width_here // HEAD
    block_size = min(512, slot_count)
    key_heads = key_rows.reshape(slot_count, heads_here, HEAD)
    value_heads = value_rows.reshape(slot_count, heads_here, HEAD)

    def one_block(running, block_item):
        grad_keys, grad_values = running
        first_row, block_lse = block_item
        query_block = lax.dynamic_slice_in_dim(queries, first_row, block_size, 0)
        grad_block = lax.dynamic_slice_in_dim(grad_mixed, first_row, block_size, 0)
        scores, query_heads = score_block(query_block, first_row, key_heads, slopes, key_valid)
        probs = jnp.exp(scores - block_lse[..., None])
        grad_heads = grad_block.reshape(block_size, heads_here, HEAD)
        grad_probs = jnp.einsum(
            "qhc,khc->hqk", grad_heads, value_heads, preferred_element_type=jnp.float32
        )
        row_dot = jnp.sum(probs * grad_probs, axis=-1, keepdims=True)
        grad_scores = (probs * (grad_probs - row_dot)).astype(jnp.bfloat16)
        grad_query = 0.125 * jnp.einsum(
            "hqk,khc->qhc", grad_scores, key_heads, preferred_element_type=jnp.float32
        )
        grad_keys = grad_keys + 0.125 * jnp.einsum(
            "hqk,qhc->khc", grad_scores, query_heads, preferred_element_type=jnp.float32
        )
        grad_values = grad_values + jnp.einsum(
            "hqk,qhc->khc",
            probs.astype(jnp.bfloat16),
            grad_heads,
            preferred_element_type=jnp.float32,
        )
        return ((grad_keys, grad_values), grad_query.reshape(block_size, width_here))

    first_rows = lax.iota(jnp.int32, slot_count // block_size) * block_size
    zero_grads = jnp.zeros((slot_count, heads_here, HEAD), jnp.float32)
    (grad_keys, grad_values), grad_queries = lax.scan(
        one_block, (zero_grads, zero_grads), (first_rows, logsum)
    )
    return (
        grad_queries.reshape(slot_count, width_here),
        grad_keys.reshape(slot_count, width_here),
        grad_values.reshape(slot_count, width_here),
    )


def spread(part, index, count):
    wide = jnp.tile(part, (1, count))
    owner = lax.broadcasted_iota(jnp.int32, wide.shape, 1) // part.shape[1]
    return jnp.where(owner == index, wide.astype(jnp.float32), 0.0)


def pick(whole, index, count):
    size = whole.shape[1] // count
    return lax.dynamic_slice_in_dim(whole, index * size, size, 1)


def pack_small(biases_qv, biases_in, rows_all, piece, pieces):
    width = rows_all.shape[1]
    halves = [b if pieces == 1 else spread(b, piece, pieces) for b in (biases_qv, biases_in)]
    rows = [rows_all] + [h.reshape(-1, width) for h in halves]
    packed = jnp.concatenate(rows, axis=0)
    return jnp.pad(packed, ((0, -packed.shape[0] % 8), (0, 0)))


def small_tile(norm_gains, offsets, qv_bias, in_bias):
    def rows(part, count):
        return jnp.pad(part.astype(f32), ((0, count - part.shape[0]), (0, 128 - part.shape[1])))

    return jnp.concatenate(
        [rows(norm_gains, 2), rows(offsets, 6), rows(in_bias, 2), rows(qv_bias, 6)], axis=0
    )


def unpack_small(packed, width_qv, width_in, piece, pieces):
    width = packed.shape[1]
    count_qv = 2 * width_qv * pieces // width
    count_in = 2 * width_in * pieces // width
    whole_qv = packed[6 : 6 + count_qv].reshape(2, -1)
    whole_in = packed[6 + count_qv : 6 + count_qv + count_in].reshape(2, -1)
    return packed[:6], pick(whole_qv, piece, pieces), pick(whole_in, piece, pieces)


def per_device(
    direct,
    tokens,
    lengths,
    qkv_weight,
    qv_bias,
    out_weight,
    in_weight,
    in_bias,
    down_weight,
    norm_gains,
    offsets,
    cotangent,
):
    row_count = tokens.shape[0]
    dp = lax.axis_size("dp")
    pieces = lax.axis_size("tensor")
    piece_index = lax.axis_index("tensor")
    dp_index = lax.axis_index("dp")
    flat_index = dp_index * pieces + piece_index
    grid = Grid3(dp)
    slot_count = row_count * pieces
    length = lengths[0]
    heads_here = qkv_weight.shape[2] // HEAD
    head_ids = (piece_index * heads_here + lax.iota(jnp.int32, heads_here)).astype(jnp.float32)
    slopes = jnp.exp2(-8.0 * (head_ids + 1.0) / (heads_here * pieces))
    key_valid = lax.iota(jnp.int32, slot_count) < length
    row_valid = (piece_index * row_count + lax.iota(jnp.int32, row_count) < length).astype(
        jnp.float32
    )[:, None]

    width_qv, width_in = qkv_weight.shape[2], in_weight.shape[2]
    if direct:
        middle = down_weight.shape[0] // 2
        output, grad_tokens, shard_qv, shard_ko, shard_in, shard_low, shard_high, small_grads = layer_call(
            grid,
            tokens,
            cotangent,
            lengths,
            slopes,
            jnp.concatenate([qkv_weight[0], qkv_weight[2]], axis=1),
            jnp.concatenate([qkv_weight[1], out_weight.T], axis=1),
            in_weight,
            down_weight[:middle].T,
            down_weight[middle:].T,
            small_tile(norm_gains, offsets, qv_bias, in_bias),
        )
        shard_wqkv = jnp.stack([shard_qv[:, :width_qv], shard_ko[:, :width_qv], shard_qv[:, width_qv:]])
        shard_out_t = shard_ko[:, width_qv:]
        shard_down_t = jnp.concatenate([shard_low, shard_high], axis=1)
        row_grads, bqv_grads, bin_grads = unpack_small(small_grads, width_qv, width_in, piece_index, pieces)
        own_rows = pick(row_grads, flat_index, dp * pieces)
        return (
            output,
            grad_tokens,
            shard_wqkv,
            pick(bqv_grads, dp_index, dp),
            shard_out_t.T,
            shard_in,
            pick(bin_grads, dp_index, dp),
            shard_down_t.T,
            own_rows[:2],
            own_rows[2:],
        )
    parts = (qkv_weight, out_weight.T, in_weight, down_weight.T)
    small = pack_small(
        spread(qv_bias, dp_index, dp),
        spread(in_bias, dp_index, dp),
        jnp.concatenate([spread(norm_gains, flat_index, dp * pieces), spread(offsets, flat_index, dp * pieces)]),
        piece_index,
        pieces,
    )
    whole_qkv, whole_out_t, whole_in, whole_down_t = (
        lax.all_gather(p, "dp", axis=p.ndim - 2, tiled=True) for p in parts
    )
    small = lax.psum(small, ("dp", "tensor"))
    rows_all, whole_bqv, whole_bin = unpack_small(small, width_qv, width_in, piece_index, pieces)
    gains, shift_rows = rows_all[:2], rows_all[2:6]

    gathered = lax.all_gather(tokens, "tensor", axis=0, tiled=True)
    projected = jnp.einsum("sd,kdc->ksc", gathered, whole_qkv, preferred_element_type=jnp.float32)
    queries = (projected[0] + whole_bqv[0]).astype(jnp.bfloat16)
    key_rows = projected[1].astype(jnp.bfloat16)
    value_rows = (projected[2] + whole_bqv[1]).astype(jnp.bfloat16)
    mixed_heads, logsum = attend(queries, key_rows, value_rows, slopes, key_valid)
    attn_part = jnp.einsum("sc,dc->sd", mixed_heads, whole_out_t, preferred_element_type=jnp.float32)
    attn_total = lax.psum_scatter(
        attn_part.astype(jnp.bfloat16), "tensor", scatter_dimension=0, tiled=True
    ).astype(jnp.float32)
    first_in = tokens.astype(jnp.float32) + attn_total + shift_rows[0]
    attended, unit_one, scale_one = norm_forward(first_in, gains[0], shift_rows[1])
    attended_low = attended.astype(jnp.bfloat16)
    gathered_ff = lax.all_gather(attended_low, "tensor", axis=0, tiled=True)
    pre_acts = jnp.einsum("sd,kdc->ksc", gathered_ff, whole_in, preferred_element_type=jnp.float32)
    pre_acts = pre_acts + whole_bin[:, None, :]
    hidden = (jax.nn.gelu(pre_acts[0], approximate=False) * pre_acts[1]).astype(jnp.bfloat16)
    ff_part = jnp.einsum("sf,df->sd", hidden, whole_down_t, preferred_element_type=jnp.float32)
    ff_total = lax.psum_scatter(
        ff_part.astype(jnp.bfloat16), "tensor", scatter_dimension=0, tiled=True
    ).astype(jnp.float32)
    second_in = attended + ff_total + shift_rows[2]
    final_norm, unit_two, scale_two = norm_forward(second_in, gains[1], shift_rows[3])
    output = (final_norm * row_valid).astype(jnp.bfloat16)
    grad_final = cotangent.astype(jnp.float32) * row_valid
    grad_second, grad_gain_two, grad_shift_two = norm_backward(
        grad_final, unit_two, scale_two, gains[1]
    )
    grad_bdown = jnp.sum(grad_second, axis=0)
    grad_ff_rows = lax.all_gather(grad_second.astype(jnp.bfloat16), "tensor", axis=0, tiled=True)
    grad_down_t = jnp.einsum("sd,sf->df", grad_ff_rows, hidden, preferred_element_type=jnp.float32)
    grad_hidden = jnp.einsum("sd,df->sf", grad_ff_rows, whole_down_t, preferred_element_type=jnp.float32)
    pullback = jax.vjp(
        lambda gate_pre, up_pre: jax.nn.gelu(gate_pre, approximate=False) * up_pre,
        pre_acts[0],
        pre_acts[1],
    )[1]
    grad_gate, grad_up = pullback(grad_hidden)
    grad_pre = jnp.stack([grad_gate, grad_up]).astype(jnp.bfloat16)
    grad_bin = jnp.sum(grad_pre, axis=1, dtype=jnp.float32)
    grad_in = jnp.einsum("sd,ksc->kdc", gathered_ff, grad_pre, preferred_element_type=jnp.float32)
    ff_back = jnp.einsum("ksc,kdc->sd", grad_pre, whole_in, preferred_element_type=jnp.float32)
    grad_attended = grad_second + lax.psum_scatter(
        ff_back.astype(jnp.bfloat16), "tensor", scatter_dimension=0, tiled=True
    ).astype(jnp.float32)
    grad_first, grad_gain_one, grad_shift_one = norm_backward(
        grad_attended, unit_one, scale_one, gains[0]
    )
    grad_bout = jnp.sum(grad_first, axis=0)
    grad_attn_rows = lax.all_gather(grad_first.astype(jnp.bfloat16), "tensor", axis=0, tiled=True)
    grad_out_t = jnp.einsum("sd,sc->dc", grad_attn_rows, mixed_heads, preferred_element_type=jnp.float32)
    grad_mixed = jnp.einsum(
        "sd,dc->sc", grad_attn_rows, whole_out_t, preferred_element_type=jnp.float32
    ).astype(jnp.bfloat16)
    grad_queries, grad_keys, grad_values = attend_back(
        queries, key_rows, value_rows, grad_mixed, logsum, slopes, key_valid
    )
    grad_qkv = jnp.stack([grad_queries, grad_keys, grad_values]).astype(jnp.bfloat16)
    grad_wqkv = jnp.einsum("sd,ksc->kdc", gathered, grad_qkv, preferred_element_type=jnp.float32)
    grad_bqv = jnp.stack(
        [
            jnp.sum(grad_qkv[0], axis=0, dtype=jnp.float32),
            jnp.sum(grad_qkv[2], axis=0, dtype=jnp.float32),
        ]
    )
    input_back = jnp.einsum("ksc,kdc->sd", grad_qkv, whole_qkv, preferred_element_type=jnp.float32)
    grad_tokens = grad_first + lax.psum_scatter(
        input_back.astype(jnp.bfloat16), "tensor", scatter_dimension=0, tiled=True
    ).astype(jnp.float32)

    small_grads = pack_small(
        grad_bqv,
        grad_bin,
        jnp.stack([grad_gain_one, grad_gain_two, grad_bout, grad_shift_one, grad_bdown, grad_shift_two]),
        piece_index,
        pieces,
    )
    grads = tuple(g.astype(jnp.bfloat16) for g in (grad_wqkv, grad_out_t, grad_in, grad_down_t))
    shard_wqkv, shard_out_t, shard_in, shard_down_t = (
        lax.psum_scatter(g.astype(jnp.float32), "dp", scatter_dimension=g.ndim - 2, tiled=True) for g in grads
    )
    small_grads = lax.psum(small_grads, ("dp", "tensor"))
    row_grads, bqv_grads, bin_grads = unpack_small(small_grads, width_qv, width_in, piece_index, pieces)
    own_rows = pick(row_grads, flat_index, dp * pieces)
    return (
        output,
        grad_tokens,
        shard_wqkv,
        pick(bqv_grads, dp_index, dp),
        shard_out_t.T,
        shard_in,
        pick(bin_grads, dp_index, dp),
        shard_down_t.T,
        own_rows[:2],
        own_rows[2:],
    )


def solution(mesh):
    placed = (
        P(("dp", "tensor"), None),
        P("dp"),
        P(None, "dp", "tensor"),
        P(None, ("tensor", "dp")),
        P("tensor", "dp"),
        P(None, "dp", "tensor"),
        P(None, ("tensor", "dp")),
        P("tensor", "dp"),
        P(None, ("dp", "tensor")),
        P(None, ("dp", "tensor")),
        P(("dp", "tensor"), None),
    )

    def run(*args):
        dp = mesh.shape["dp"]
        direct = dp % 4 == 0 and (args[2].shape[1] // dp) % 16 == 0 and mesh.shape["tensor"] == 2
        return jax.shard_map(
            functools.partial(per_device, direct),
            mesh=mesh,
            in_specs=placed,
            out_specs=(
                P(("dp", "tensor"), None),
                P(("dp", "tensor"), None),
                P(None, "dp", "tensor"),
                P(None, ("tensor", "dp")),
                P("tensor", "dp"),
                P(None, "dp", "tensor"),
                P(None, ("tensor", "dp")),
                P("tensor", "dp"),
                P(None, ("dp", "tensor")),
                P(None, ("dp", "tensor")),
            ),
            check_vma=False,
        )(*args)

    return run
```

```python
import functools
import itertools

import jax
import jax.numpy as jnp
from jax import lax
from jax.experimental import pallas as pl
from jax.experimental.pallas import tpu as pltpu
from jax.sharding import PartitionSpec as P

HEAD = 64
MESH = pl.DeviceIdType.MESH
VMEM_LIMIT = 64 * 1024 * 1024 - 65536


class Grid3:
    def __init__(self, dp):
        self.nz = dp // 4
        self.slots = dp

    def here(self):
        me = lax.axis_index("dp")
        self.z, self.y, self.x = me // 4, (me // 2) % 2, me % 2
        z, nz = self.z, self.nz
        self.low, self.high = z > 0, z < nz - 1
        near = [sorted(range(1, nz), key=lambda k: (abs((p + k) % nz - p), k)) for p in range(nz)]
        self.by_distance = [(sum(jnp.where(z == p, near[p][j], 0) for p in range(nz)), 0, 0) for j in range(nz - 1)]
        self.line = []
        for d in self.by_distance:
            above = (z + d[0]) % nz > z
            self.line.append((above, jnp.where(above, z, nz - 1 - z) > 0))

    def at(self, dz, dy, dx):
        y = 1 - self.y if dy else self.y
        x = 1 - self.x if dx else self.x
        return (((self.z + dz) % self.nz) * 2 + y) * 2 + x

    def slot(self, d):
        return (d[0] % self.nz) * 4 + d[1] * 2 + d[2]

    def steps(self, axis):
        if axis == "z":
            return [(k, 0, 0) for k in range(1, self.nz)]
        return [(0, 1, 0)] if axis == "y" else [(0, 0, 1)]

    def seen_from(self, d, move):
        return ((d[0] - move[0] + self.nz) % self.nz, d[1] ^ move[1], d[2] ^ move[2])

    def span(self, axis):
        if axis == "z":
            return [(k, 0, 0) for k in range(self.nz)]
        return [(0, 0, 0), (0, 1, 0)] if axis == "y" else [(0, 0, 0), (0, 0, 1)]


def joined(*ds):
    return tuple(sum(part) for part in zip(*ds))


def remote(src, dst, send_sem, recv_sem, **device):
    return pltpu.make_async_remote_copy(
        src_ref=src, dst_ref=dst, send_sem=send_sem, recv_sem=recv_sem, device_id=device, device_id_type=MESH
    )


def greet(grid, partner):
    barrier = pltpu.get_barrier_semaphore()
    moves = [m for axis in "zyx" for m in grid.steps(axis)]
    for move in moves:
        pl.semaphore_signal(barrier, inc=1, device_id={"dp": grid.at(*move)}, device_id_type=MESH)
    pl.semaphore_signal(barrier, inc=1, device_id={"tensor": partner}, device_id_type=MESH)
    pl.semaphore_wait(barrier, len(moves) + 1)


class SmallSum:
    def __init__(self, grid, value, out, box, send, recv):
        self.grid = grid
        self.value, self.out, self.box, self.send, self.recv = value, out, box, send, recv
        self.copies = []

    def _post(self, slot, **device):
        copy = remote(self.out, self.box.at[slot], self.send.at[slot], self.recv.at[slot], **device)
        copy.start()
        self.copies.append(copy)

    def stage(self, number):
        grid = self.grid
        if number == 0:
            self.out[...] = self.value[...]
            self._post(0, tensor=1 - lax.axis_index("tensor"))
            return
        for copy in self.copies:
            copy.wait()
        self.copies = []
        if number == 1:
            self.out[...] = self.out[...] + self.box[0]
            self._post(1, dp=grid.at(0, 0, 1))
        elif number == 2:
            self.out[...] = self.out[...] + self.box[1]
            self._post(2, dp=grid.at(0, 1, 0))
        elif number == 3:
            self.out[...] = self.out[...] + self.box[2]
            for k in range(1, grid.nz):
                self._post(2 + k, dp=grid.at(k, 0, 0))
        else:
            total = self.out[...]
            for k in range(1, grid.nz):
                total = total + self.box[2 + k]
            self.out[...] = total


def small_slots(grid):
    return 2 + grid.nz


class Gather:
    def __init__(self, grid, chunks, send, recv):
        self.grid, self.chunks = grid, chunks
        self.send_sem, self.recv_sem = send, recv
        self.sent = []

    def _dst(self, number, d):
        rows = self.chunks[number][0].shape[0]
        return self.chunks[number][1].at[pl.ds(pl.multiple_of(self.grid.at(*d) * rows, rows), rows)]

    def _copy(self, number, d, move):
        dst = self._dst(number, d)
        if isinstance(move, int):
            move = (jnp.where(self.grid.line[move][0], -1, 1), 0, 0)
        source = self.chunks[number][0] if isinstance(d[0], int) and d == (0, 0, 0) else dst
        slot = self.grid.slot(self.grid.seen_from(d, move))
        return remote(source, dst, self.send_sem.at[number, slot], self.recv_sem.at[number, slot], dp=self.grid.at(*move))

    def _start(self, allowed, *args):
        if allowed is None:
            self._copy(*args).start()
        else:
            pl.when(allowed)(lambda: self._copy(*args).start())
        self.sent.append((allowed, args))

    def send(self, number, d, axis):
        if axis == "z":
            self._start(self.grid.low, number, d, (-1, 0, 0))
            self._start(self.grid.high, number, d, (1, 0, 0))
        else:
            self._start(None, number, d, self.grid.steps(axis)[0])

    def relay(self, number, d, j):
        self._start(self.grid.line[j][1], number, d, j)

    def arrive(self, number, d):
        dst, slot = self._dst(number, d), self.grid.slot(d)
        remote(dst, dst, self.send_sem.at[number, slot], self.recv_sem.at[number, slot], dp=self.grid.at(*d)).wait_recv()

    def moved(self, axis):
        return self.grid.by_distance if axis == "z" else self.grid.steps(axis)

    def first(self, number):
        return [(self.pass_first, number, d, j) for j, d in enumerate(self.moved(self.chunks[number][2][0]))]

    def second(self, number):
        one, two = self.chunks[number][2][:2]
        return [
            (self.pass_second, number, joined(a, b), j) for j, b in enumerate(self.moved(two)) for a in self.grid.span(one)
        ]

    def third(self, number):
        one, two, three = self.chunks[number][2]
        return [joined(a, b, c) for a in self.grid.span(one) for b in self.grid.span(two) for c in self.grid.steps(three)]

    def pass_first(self, number, d, j):
        order = self.chunks[number][2]
        self.arrive(number, d)
        if order[0] == "z":
            self.relay(number, d, j)
        for axis in order[1:]:
            self.send(number, d, axis)

    def pass_second(self, number, d, j):
        order = self.chunks[number][2]
        self.arrive(number, d)
        if order[1] == "z":
            self.relay(number, d, j)
        self.send(number, d, order[2])

    def finish(self, number):
        for d in self.third(number):
            self.arrive(number, d)

    def drain(self):
        for allowed, args in self.sent:
            if allowed is None:
                self._copy(*args).wait_send()
            else:
                pl.when(allowed)(lambda args=args: self._copy(*args).wait_send())
        self.sent = []


class Scatter:
    def __init__(self, grid, rows, chunks, send, recv):
        self.grid, self.rows, self.chunks = grid, rows, chunks
        self.send_sem, self.recv_sem = send, recv
        self.sent = []
        self.far_first = [2, 1, 3] if grid.nz == 4 else list(range(1, grid.nz))
        self.second, self.line = 2 * grid.nz, 3 * grid.nz - 1

    def part(self, number, d):
        return self.chunks[number][0].at[pl.ds(pl.multiple_of(self.grid.at(*d) * self.rows, self.rows), self.rows)]

    def box(self, number, slot):
        return self.chunks[number][3].at[slot]

    def other(self, number):
        return "y" if self.chunks[number][2] == "x" else "x"

    def place(self, number, dz, e):
        return (dz, e, 0) if self.other(number) == "y" else (dz, 0, e)

    def _copy(self, number, kind, dz, e=0):
        grid = self.grid
        if kind == "own":
            move = grid.steps(self.chunks[number][2])[0]
            source, slot = self.part(number, joined(self.place(number, dz, e), move)), dz * 2 + e
        elif kind == "side":
            move = grid.steps(self.other(number))[0]
            source, slot = self.box(number, dz * 2 + 1), self.second + dz
        else:
            move = (dz, 0, 0)
            source, slot = self.box(number, dz * 2), self.line + dz
        return remote(
            source, self.box(number, slot), self.send_sem.at[number, slot], self.recv_sem.at[number, slot], dp=grid.at(*move)
        )

    def _send(self, *args):
        self._copy(*args).start()
        self.sent.append(args)

    def _arrive(self, number, slot):
        box = self.box(number, slot)
        remote(box, box, self.send_sem.at[number, slot], self.recv_sem.at[number, slot], dp=0).wait_recv()

    def begin(self, number, *halves):
        for e in halves or (1, 0):
            for dz in self.far_first + [0]:
                self._send(number, "own", dz, e)

    def held(self, number, dz, e):
        slot = dz * 2 + e
        self._arrive(number, slot)
        return self.part(number, self.place(number, dz, e))[...].astype(jnp.float32) + self.box(number, slot)[...].astype(jnp.float32)

    def side(self, number, dz):
        self.box(number, dz * 2 + 1)[...] = self.held(number, dz, 1).astype(jnp.bfloat16)
        self._send(number, "side", dz)

    def both(self, number, dz):
        value = self.held(number, dz, 0)
        self._arrive(number, self.second + dz)
        return value + self.box(number, self.second + dz)[...].astype(jnp.float32)

    def along(self, number, dz):
        self.box(number, dz * 2)[...] = self.both(number, dz).astype(jnp.bfloat16)
        self._send(number, "line", dz)

    def sides(self, *numbers):
        return [(self.side, n, dz) for dz in self.far_first + [0] for n in numbers]

    def lines(self, *numbers):
        return [(self.along, n, dz) for dz in self.far_first for n in numbers]

    def lasts(self, *numbers):
        return [(self.last, n) for n in numbers]

    def last(self, number):
        total = self.both(number, 0)
        for dz in self.far_first:
            self._arrive(number, self.line + dz)
            total = total + self.box(number, self.line + dz)[...].astype(jnp.float32)
        self.chunks[number][1](total)

    def drain(self):
        for args in self.sent:
            self._copy(*args).wait_send()
        self.sent = []


def scatter_slots(grid):
    return 4 * grid.nz - 1
bf16, f32 = jnp.bfloat16, jnp.float32
NORM_EPSILON = 1e-06
EARLY = 12
AFTER_PROJECTION = 4
GATHER_STEPS = 4
AFTER_OUT = 4
AFTER_NORM = 4
ROOT_HALF = 0.7071067811865476
PHI_SCALE = 0.3989422804014327


def nn(a, b):
    return jnp.dot(a, b, preferred_element_type=f32)


def nt(a, b):
    return lax.dot_general(a, b, (((1,), (1,)), ((), ())), preferred_element_type=f32)


def aligned(start, size):
    return pl.ds(pl.multiple_of(start, size), size)


def unit_rows(values):
    centred = values - jnp.mean(values, axis=-1, keepdims=True)
    variance = jnp.mean(centred * centred, axis=-1, keepdims=True)
    scale = lax.rsqrt(variance + NORM_EPSILON)
    return centred * scale, scale


def unit_back(grad_unit, unit, scale):
    inner = (
        grad_unit
        - jnp.mean(grad_unit, axis=-1, keepdims=True)
        - unit * jnp.mean(grad_unit * unit, axis=-1, keepdims=True)
    )
    return inner * scale


def fold(rows):
    return jnp.sum(rows.reshape(rows.shape[0] // 8, 8, rows.shape[1]), axis=0)


def merged(*lists):
    return [entry for row in itertools.zip_longest(*lists) for entry in row if entry is not None]


class Pump:
    def __init__(self, steps=()):
        self.steps = list(steps)

    def take(self, count=None):
        count = len(self.steps) if count is None else min(count, len(self.steps))
        taken, self.steps = self.steps[:count], self.steps[count:]
        return taken

    def run(self, count=None):
        for function, *args in self.take(count):
            function(*args)


def at_trips(*shares):
    def run(index):
        for trip, share in enumerate(shares):

            @pl.when(index == trip)
            def _(share=share):
                Pump(share).run()

    return run


def layer_body(
    grid, rows,
    tokens, cotangent, length, qv_part, ko_part, in_part, low_part, high_part, gains_part, offsets_part, qv_bias, in_bias,
    output, grad_tokens, to_qkv, to_out, to_in, to_down, to_gains, to_offsets, to_qv_bias, to_in_bias, probs_far,
    w_qv, w_ko, w_gate, w_up, w_low, w_high, small_mine, small_pair, small_tiles, every_small, small_box, small_grads,
    x, qkv, inverse, mixed, work, key_aug, value_aug, query_aug,
    rows_f32, attended_low, branch_rows, outgoing, incoming, cot, turned,
    grad_t, pair_b, grad_value_t, grad_key_t,
    g_qv, g_ko, g_gate, g_up, g_low, g_high, box_qv, box_ko, box_gate, box_up, box_low, box_high,
    gather_send, gather_recv, scatter_send, scatter_recv, small_send, small_recv, own_sem, swap_send, swap_recv, local_sem, prob_sem,
):
    grid.here()
    side = lax.axis_index("tensor")
    other = 1 - side
    half = tokens.shape[0]
    slots = 2 * half
    width = tokens.shape[1]
    heads_wide = mixed.shape[1]
    units = w_gate.shape[1]
    mine = aligned(side * half, half)
    count = length[0]
    attended, unit_one = rows_f32.at[:, pl.ds(0, width)], rows_f32.at[:, pl.ds(width, width)]
    scale_one = rows_f32.at[:, pl.ds(2 * width, 128)]
    block = 256
    span = 2 * slots - block
    bias = rows_f32.at[pl.ds(0, block), pl.ds(0, span)]

    greet(grid, other)

    gather = Gather(grid, [
        (qv_part, w_qv, "zyx"),
        (ko_part, w_ko, "zxy"),
        (in_part.at[0], w_gate, "yzx"),
        (in_part.at[1], w_up, "xzy"),
        (low_part, w_low, "zyx"),
        (high_part, w_high, "zxy"),
        (small_pair, small_tiles, "zyx"),
    ], gather_send, gather_recv)
    def sink_qv(total):
        to_qkv[0], to_qkv[2] = total[:, :heads_wide], total[:, heads_wide:]

    def sink_ko(total):
        to_qkv[1] = total[:, :heads_wide]
        to_out[...] = total[:, heads_wide:].T

    def sink_gate(total):
        to_in[0] = total

    def sink_up(total):
        to_in[1] = total

    def sink_low(total):
        to_down[: units // 2, :] = total.T

    def sink_high(total):
        to_down[units // 2 :, :] = total.T

    scatter = Scatter(grid, rows, [
        (g_qv, sink_qv, "x", box_qv),
        (g_ko, sink_ko, "y", box_ko),
        (g_gate, sink_gate, "x", box_gate),
        (g_up, sink_up, "y", box_up),
        (g_low, sink_low, "x", box_low),
        (g_high, sink_high, "y", box_high),
    ], scatter_send, scatter_recv)
    QV, KO, GATE, UP, LOW, HIGH, SMALL = range(7)

    def swap(source, target, slot):
        copy = remote(source, target, swap_send.at[slot], swap_recv.at[slot], tensor=other)
        copy.start()
        return copy

    token_swap = swap(tokens, x.at[mine], 0)
    token_copy = pltpu.make_async_copy(tokens, x.at[mine], local_sem.at[0])
    token_copy.start()
    cot_copy = pltpu.make_async_copy(cotangent, cot, local_sem.at[1])
    cot_copy.start()
    my_lanes = pl.ds(pl.multiple_of(side * 128, 128), 128)
    small_mine[...] = jnp.zeros_like(small_mine)
    small_mine[0:2, 0 : gains_part.shape[1]] = gains_part[...]
    small_mine[2:6, 0 : offsets_part.shape[1]] = offsets_part[...]
    small_mine[8:10, 0 : in_bias.shape[1]] = in_bias[...].astype(f32)
    small_mine[10:12, 0 : qv_bias.shape[1]] = qv_bias[...].astype(f32)
    small_pair[:, my_lanes] = small_mine[...]
    small_swap = swap(small_mine, small_pair.at[:, my_lanes], 8)
    own_copies = []
    for n, (source, target, _) in enumerate(gather.chunks[:SMALL]):
        copy = pltpu.make_async_copy(source, target.at[aligned(grid.at(0, 0, 0) * rows, rows)], own_sem.at[n])
        copy.start()
        own_copies.append(copy)
        for axis in gather.chunks[n][2]:
            gather.send(n, (0, 0, 0), axis)
        if n == KO:
            small_swap.wait()
            for axis in gather.chunks[SMALL][2]:
                gather.send(SMALL, (0, 0, 0), axis)
            small_tiles[aligned(grid.at(0, 0, 0) * 16, 16), :] = small_pair[...]
    near_units = merged(gather.second(GATE), gather.second(UP))
    ends_first = merged(gather.first(LOW), gather.first(HIGH))
    ends_second = merged(gather.second(LOW), gather.second(HIGH))
    early = (
        merged(gather.first(QV), gather.first(SMALL), gather.first(KO))
        + merged(gather.first(GATE), gather.first(UP))
        + merged(merged(gather.second(QV), gather.second(SMALL), gather.second(KO)), near_units[:EARLY])
    )
    pump = Pump(early)
    pump.run()
    pump = Pump(merged(near_units[EARLY:], ends_first) + ends_second)
    for copy in own_copies:
        copy.wait()
    token_copy.wait()
    token_swap.wait()
    for number in (SMALL, QV, KO):
        gather.finish(number)

    norm_rows = jnp.zeros((8, width), f32)
    head_rows = jnp.zeros((8, heads_wide), f32)
    unit_rows_in = jnp.zeros((8, units), f32)

    def at_lanes(tile, lanes, start):
        wide = jnp.concatenate([tile, jnp.zeros((8, lanes - 128), f32)], axis=1)
        return pltpu.roll(wide, start, 1) if start else wide

    for i in range(grid.slots):
        pair_tile = [small_tiles[16 * i : 16 * i + 8, 128 * s : 128 * s + 128] for s in range(2)]
        unit_tile = [small_tiles[16 * i + 8 : 16 * i + 16, 128 * s : 128 * s + 128] for s in range(2)]
        for s in range(2):
            norm_rows = norm_rows + at_lanes(pair_tile[s], width, (2 * i + s) * (rows // 2))
        units_here = jnp.where(side == 0, unit_tile[0], unit_tile[1])
        unit_rows_in = unit_rows_in + at_lanes(units_here, units, i * (units // grid.slots))
        head_rows = head_rows + at_lanes(pltpu.roll(units_here, 6, 0), heads_wide, i * (heads_wide // grid.slots))
    every_small[0:8, :] = norm_rows
    every_small[8:9, pl.ds(0, heads_wide)] = head_rows[0:1, :]
    every_small[8:9, pl.ds(heads_wide, heads_wide)] = head_rows[1:2, :]
    turned[0:8, :] = unit_rows_in

    q_cols, v_cols, k_cols = (pl.ds(i * heads_wide, heads_wide) for i in range(3))
    side_cols = pl.ds(pl.multiple_of(side * heads_wide, 128), heads_wide)
    row_bias = every_small[8:9, :]
    row_scale = jnp.where(lax.broadcasted_iota(jnp.int32, (1, 2 * heads_wide), 1) < heads_wide, 0.125, 1.0)

    @pl.loop(0, slots // 256)
    def _(i):
        r = aligned(i * 256, 256)
        raw = (nn(x[r, :], w_qv[...]) + row_bias).astype(bf16)
        qkv[r, pl.ds(0, 2 * heads_wide)] = (raw.astype(f32) * row_scale).astype(bf16)
        qkv[r, k_cols] = nn(x[r, :], w_ko[:, pl.ds(0, heads_wide)]).astype(bf16)

    pump.run(AFTER_PROJECTION)

    lane = lax.broadcasted_iota(jnp.int32, (slots, 128), 1)
    slot = lax.broadcasted_iota(jnp.int32, (slots, 128), 0)
    key_mask = jnp.where(slot < count, 0.0, -1e30).astype(bf16)
    zero, one = jnp.zeros((), bf16), jnp.ones((), bf16)
    block_lane = lax.broadcasted_iota(jnp.int32, (block, 128), 1)
    pairs = heads_wide // 128
    slopes = [2.0 ** (-8.0 * (h + 1) / (4 * pairs)) for h in range(4 * pairs)]

    def prob_slot(upper):
        return work.at[:, pl.ds(upper * slots, slots)]

    def prob_out(pair, upper):
        return pltpu.make_async_copy(prob_slot(upper), probs_far.at[2 * pair + upper], prob_sem.at[upper])

    def prob_in(pair, upper):
        return pltpu.make_async_copy(probs_far.at[2 * pair + upper], prob_slot(upper), prob_sem.at[upper])

    def pair_cols(pair, start=0):
        return pl.ds(pl.multiple_of(start + pair * 128, 128), 128)

    def attend_pair(pair):
        cols = pair_cols(pair)
        for upper in (0, 1):
            own = (lane >= 64) == (upper == 1)
            spare = 0 if upper else 64
            gap = jnp.abs(
                lax.broadcasted_iota(jnp.int32, (block, span), 0)
                - (lax.broadcasted_iota(jnp.int32, (block, span), 1) - (span - slots))
            )
            slope = sum(
                jnp.where(pair == p, jnp.where(side == 0, slopes[2 * p + upper], slopes[2 * (pairs + p) + upper]), 0.0)
                for p in range(pairs)
            )
            bias[...] = gap.astype(f32) * slope
            key_aug[...] = jnp.where(own, qkv[:, pair_cols(pair, 2 * heads_wide)], jnp.where(lane == spare, key_mask, zero))
            value_aug[...] = jnp.where(own, qkv[:, pair_cols(pair, heads_wide)], one)
            query_aug[...] = jnp.where(own, qkv[:, cols], jnp.where(lane == spare, one, zero))

            @pl.when(pair > 0)
            def _(upper=upper):
                prob_out(pair - 1, upper).wait()

            def attend(i, inner_carry, upper=upper):
                r = aligned(i * block, block)
                scores = nt(query_aug[r, :], key_aug[...]) - bias[:, pl.ds(pl.multiple_of(span - slots - i * block, block), slots)]
                top = jnp.max(scores, axis=1, keepdims=True)
                weights = jnp.exp(scores - top).astype(bf16)
                work[r, pl.ds(upper * slots, slots)] = weights
                product = nn(weights, value_aug[...])
                scale = 1.0 / (product[:, 0:1] if upper else product[:, 64:65])
                result = (product * scale).astype(bf16)
                inverse[r, :] = jnp.where(block_lane == 2 * pair + upper, scale, inverse[r, :])
                mixed[r, cols] = jnp.where(block_lane < 64, mixed[r, cols], result) if upper else result
                return inner_carry

            lax.fori_loop(0, slots // block, attend, 0, unroll=2)
            prob_out(pair, upper).start()
        between_pairs(pair)

    inverse[...] = jnp.zeros_like(inverse)
    between_pairs = at_trips(*(pump.take(GATHER_STEPS) for _ in range(pairs)))
    pl.loop(0, pairs)(attend_pair)

    def project(source, weights, target_rows, sink):
        @pl.loop(0, half // 256)
        def _(i):
            r = aligned(target_rows * half + i * 256, 256)
            sink(i, nt(source[r, :], weights[...]))

    def to_outgoing(i, value):
        outgoing[aligned(i * 256, 256), :] = value.astype(bf16)

    def to_attended(i, value):
        attended[aligned(i * 256, 256), :] = value

    w_out = w_ko.at[:, pl.ds(heads_wide, heads_wide)]
    project(mixed, w_out, other, to_outgoing)
    first_swap = swap(outgoing, incoming.at[0], 1)
    pump.run(AFTER_OUT)
    project(mixed, w_out, side, to_attended)
    first_swap.wait()
    gain_one, gain_two = every_small[0:1, :], every_small[1:2, :]
    step = 64

    @pl.loop(0, half // step)
    def _(i):
        r = aligned(i * step, step)
        own = pl.ds(pl.multiple_of(side * half + i * step, step), step)
        total = x[own, :].astype(f32) + attended[r, :] + incoming[0, r, :].astype(f32) + every_small[2:3, :]
        unit, scale = unit_rows(total)
        result = unit * gain_one + every_small[3:4, :]
        unit_one[r, :] = unit
        scale_one[r, :] = jnp.broadcast_to(scale, (step, 128))
        attended[r, :] = result
        attended_low[own, :] = result.astype(bf16)

    low_swap = swap(attended_low.at[mine], attended_low.at[mine], 2)
    for upper in (0, 1):
        prob_out(pairs - 1, upper).wait()
    pump.run(AFTER_NORM)
    gather.finish(GATE)
    gather.finish(UP)

    def feed(rows_side):
        r = aligned(rows_side * half, half)

        @pl.loop(0, units // 256)
        def _(j):
            c = aligned(j * 256, 256)
            c_up = pl.ds(pl.multiple_of(units + j * 256, 256), 256)
            c_hidden = pl.ds(pl.multiple_of(2 * units + j * 256, 256), 256)
            gate = nn(attended_low[r, :], w_gate[:, c]) + turned[0:1, c]
            up = nn(attended_low[r, :], w_up[:, c]) + turned[1:2, c]
            below = 0.5 * (1.0 + lax.erf(gate * ROOT_HALF))
            density = PHI_SCALE * jnp.exp(-0.5 * gate * gate)
            bent = gate * below
            work[r, c_hidden] = (bent * up).astype(bf16)
            work[r, c] = (up * (below + gate * density)).astype(bf16)
            work[r, c_up] = bent.astype(bf16)

    feed(side)
    pump.run()
    low_swap.wait()
    feed(other)
    pump.run()
    gather.finish(LOW)
    gather.finish(HIGH)

    hidden_low, hidden_high = pl.ds(2 * units, units // 2), pl.ds(2 * units + units // 2, units // 2)

    def down(rows_side, sink):
        @pl.loop(0, half // 256)
        def _(i):
            r = aligned(rows_side * half + i * 256, 256)
            sink(i, nt(work[r, hidden_low], w_low[...]) + nt(work[r, hidden_high], w_high[...]))

    def add_attended(i, value):
        r = aligned(i * 256, 256)
        attended[r, :] = attended[r, :] + value

    down(other, to_outgoing)
    second_swap = swap(outgoing, incoming.at[1], 3)
    down(side, add_attended)
    cot_copy.wait()
    second_swap.wait()
    nothing = jnp.zeros((8, width), f32)

    def second_norm(i, carry):
        sum_gain, sum_shift, sum_branch = carry
        r = aligned(i * step, step)
        own = pl.ds(pl.multiple_of(side * half + i * step, step), step)
        position = side * half + i * step + lax.broadcasted_iota(jnp.int32, (step, 1), 0)
        valid = jnp.where(position < count, 1.0, 0.0)
        unit, scale = unit_rows(attended[r, :] + incoming[1, r, :].astype(f32) + every_small[4:5, :])
        grad = cot[r, :].astype(f32) * valid
        cot[r, :] = ((unit * gain_two + every_small[5:6, :]) * valid).astype(bf16)
        back = unit_back(grad * gain_two, unit, scale)
        attended[r, :] = back
        branch_rows[own, :] = back.astype(bf16)
        return sum_gain + fold(grad * unit), sum_shift + fold(grad), sum_branch + fold(back)

    gain_two_sum, shift_two_sum, down_bias_sum = lax.fori_loop(0, half // step, second_norm, (nothing,) * 3)
    branch_swap = swap(branch_rows.at[mine], branch_rows.at[mine], 4)
    output_copy = pltpu.make_async_copy(cot, output, local_sem.at[2])
    output_copy.start()
    small_grads[...] = jnp.zeros_like(small_grads)
    small_grads[1:2, :] = jnp.sum(gain_two_sum, axis=0, keepdims=True)
    small_grads[5:6, :] = jnp.sum(shift_two_sum, axis=0, keepdims=True)
    small_grads[4:5, :] = jnp.sum(down_bias_sum, axis=0, keepdims=True)
    branch_swap.wait()

    def turn(source):
        @pl.loop(0, slots // 256)
        def _(i):
            r = aligned(i * 256, 256)
            grad_t[:, r] = source[r, :].T

    def weight_grad(sink, source, source_start, tile):
        @pl.loop(0, sink.shape[1] // tile)
        def _(j):
            sink[:, aligned(j * tile, tile)] = nn(
                grad_t[...], source[:, pl.ds(pl.multiple_of(source_start + j * tile, tile), tile)]
            ).astype(bf16)

    turn(branch_rows)
    weight_grad(g_low, work, 2 * units, 256)
    scatter.begin(LOW)
    weight_grad(g_high, work, 2 * units + units // 2, 256)
    scatter.begin(HIGH)

    turned[8:24, :] = jnp.zeros((16, units), f32)
    for index, weights in enumerate((w_low, w_high)):
        @pl.loop(0, units // 2 // 256)
        def _(j, index=index, weights=weights):
            c = pl.ds(pl.multiple_of(index * (units // 2) + j * 256, 256), 256)
            c_up = pl.ds(pl.multiple_of(units + index * (units // 2) + j * 256, 256), 256)
            for part in range(2):
                r = pl.ds(part * half, half)
                grad = nn(branch_rows[r, :], weights[:, aligned(j * 256, 256)])
                gate_grad = (grad * work[r, c].astype(f32)).astype(bf16)
                up_grad = (grad * work[r, c_up].astype(f32)).astype(bf16)
                work[r, c] = gate_grad
                work[r, c_up] = up_grad
                turned[8:16, c] = turned[8:16, c] + fold(gate_grad.astype(f32))
                turned[16:24, c] = turned[16:24, c] + fold(up_grad.astype(f32))

    for index in range(2):
        total = jnp.sum(turned[8 + 8 * index : 16 + 8 * index, :], axis=0, keepdims=True)
        for j in range(units // width):
            small_grads[pl.ds(8 + 4 * index + 2 * side + j, 1), :] = total[:, j * width : (j + 1) * width]

    Pump(scatter.sides(LOW, HIGH)).run()
    turn(attended_low)
    weight_grad(g_gate, work, 0, 512)
    scatter.begin(GATE, 1)
    weight_grad(g_up, work, units, 512)
    scatter.begin(UP, 1)
    scatter.begin(GATE, 0)

    gate_cols, up_cols = pl.ds(0, units), pl.ds(units, units)

    def units_back(rows_side, sink):
        @pl.loop(0, half // 256)
        def _(i):
            r = aligned(rows_side * half + i * 256, 256)
            sink(i, nt(work[r, gate_cols], w_gate[...]) + nt(work[r, up_cols], w_up[...]))

    units_back(other, to_outgoing)
    third_swap = swap(outgoing, incoming.at[0], 5)
    units_back(side, add_attended)
    Pump(scatter.lines(LOW, HIGH)).run()
    third_swap.wait()

    def first_norm_back(i, carry):
        sum_gain, sum_shift, sum_branch = carry
        r = aligned(i * step, step)
        own = pl.ds(pl.multiple_of(side * half + i * step, step), step)
        grad = attended[r, :] + incoming[0, r, :].astype(f32)
        unit = unit_one[r, :]
        back = unit_back(grad * gain_one, unit, scale_one[r, 0:1])
        attended[r, :] = back
        branch_rows[own, :] = back.astype(bf16)
        return sum_gain + fold(grad * unit), sum_shift + fold(grad), sum_branch + fold(back)

    prob_in(0, 0).start()
    prob_in(0, 1).start()
    gain_one_sum, shift_one_sum, out_bias_sum = lax.fori_loop(0, half // step, first_norm_back, (nothing,) * 3)
    attn_swap = swap(branch_rows.at[mine], branch_rows.at[mine], 6)
    small_grads[0:1, :] = jnp.sum(gain_one_sum, axis=0, keepdims=True)
    small_grads[3:4, :] = jnp.sum(shift_one_sum, axis=0, keepdims=True)
    small_grads[2:3, :] = jnp.sum(out_bias_sum, axis=0, keepdims=True)
    attn_swap.wait()

    grad_mixed = attended_low.at[:, pl.ds(0, heads_wide)]
    turn(branch_rows)
    g_ko[:, pl.ds(heads_wide, heads_wide)] = nn(grad_t[...], mixed[...]).astype(bf16)
    sides_gate = Pump(scatter.sides(GATE))
    sides_gate.run(2)

    @pl.loop(0, slots // 256)
    def _(i):
        r = aligned(i * 256, 256)
        grad_mixed[r, :] = nn(branch_rows[r, :], w_out[...]).astype(bf16)

    sides_gate.run()
    scatter.begin(UP, 0)

    mixed_t, query_t = pair_b.at[0], pair_b.at[1]

    def pair_back(pair):
        cols, key_cols, value_cols = pair_cols(pair), pair_cols(pair, 2 * heads_wide), pair_cols(pair, heads_wide)
        scales = inverse[...]
        shrink = jnp.where(
            lane < 64,
            jnp.sum(jnp.where(lane == 2 * pair, scales, 0.0), axis=1, keepdims=True),
            jnp.sum(jnp.where(lane == 2 * pair + 1, scales, 0.0), axis=1, keepdims=True),
        )
        scaled = (grad_mixed[:, cols].astype(f32) * shrink).astype(bf16)
        mixed_t[...] = scaled.T
        query_t[...] = qkv[:, cols].T
        outgoing_pair[...] = scaled
        for upper in (0, 1):
            own = (lane >= 64) == (upper == 1)
            spare = 0 if upper else 64
            scaled = outgoing_pair[...]
            dots = jnp.sum(jnp.where(own, scaled.astype(f32) * mixed[:, cols].astype(f32), 0.0), axis=1, keepdims=True)
            dots_high = dots.astype(bf16)
            dots_low = (dots - dots_high.astype(f32)).astype(bf16)
            ones = (lane == spare) | (lane == spare + 1)
            value_aug[...] = jnp.where(own, qkv[:, value_cols], jnp.where(ones, one, zero))
            query_aug[...] = jnp.where(
                own, scaled, jnp.where(lane == spare, -dots_high, jnp.where(lane == spare + 1, -dots_low, zero))
            )
            part = pl.ds(64 * upper, 64)
            base = upper * slots
            prob_in(pair, upper).wait()
            for j in range(slots // 512):
                c = pl.ds(j * 512, 512)
                grad_value_t[part, c] = nn(mixed_t[part, :], work[:, pl.ds(base + j * 512, 512)]).astype(bf16)

            def attend_back(i, inner_carry, upper=upper, base=base):
                r = aligned(i * block, block)
                inner = nt(query_aug[r, :], value_aug[...])
                grads = (work[r, pl.ds(base, slots)].astype(f32) * inner).astype(bf16)
                work[r, pl.ds(base, slots)] = grads
                result = (nn(grads, qkv[:, key_cols]) * 0.125).astype(bf16)
                qkv[r, cols] = jnp.where(block_lane < 64, qkv[r, cols], result) if upper else result
                return inner_carry

            lax.fori_loop(0, slots // block, attend_back, 0, unroll=2)
            for j in range(slots // 512):
                c = pl.ds(j * 512, 512)
                grad_key_t[part, c] = nn(query_t[part, :], work[:, pl.ds(base + j * 512, 512)]).astype(bf16)

            @pl.when(pair + 1 < pairs)
            def _(upper=upper):
                prob_in(pair + 1, upper).start()

        qkv[:, value_cols] = grad_value_t[...].T
        qkv[:, key_cols] = grad_key_t[...].T
        between_pairs(pair)

    outgoing_pair = key_aug
    between_pairs = at_trips(scatter.sides(UP), scatter.lasts(LOW, HIGH), scatter.lines(GATE))
    pl.loop(0, pairs)(pair_back)

    turn(x)
    g_qv[...] = nn(grad_t[...], qkv[:, pl.ds(0, 2 * heads_wide)]).astype(bf16)
    scatter.begin(QV)
    g_ko[:, pl.ds(0, heads_wide)] = nn(grad_t[...], qkv[:, k_cols]).astype(bf16)
    scatter.begin(KO)
    def column_sum(cols):
        def add(i, carry):
            return carry + fold(qkv[aligned(i * 128, 128), cols].astype(f32))

        return jnp.sum(lax.fori_loop(0, slots // 128, add, jnp.zeros((8, heads_wide), f32)), axis=0, keepdims=True)

    small_grads[6:7, side_cols] = column_sum(q_cols)
    small_grads[7:8, side_cols] = column_sum(v_cols)
    sums = SmallSum(grid, small_grads, small_grads, small_box, small_send, small_recv)
    sums.stage(0)

    def inputs_back(rows_side, sink):
        @pl.loop(0, half // 256)
        def _(i):
            r = aligned(rows_side * half + i * 256, 256)
            sink(
                i,
                nt(qkv[r, pl.ds(0, 2 * heads_wide)], w_qv[...]) + nt(qkv[r, k_cols], w_ko[:, pl.ds(0, heads_wide)]),
            )

    inputs_back(other, to_outgoing)
    fourth_swap = swap(outgoing, incoming.at[1], 7)
    sums.stage(1)
    inputs_back(side, add_attended)
    fourth_swap.wait()

    @pl.loop(0, half // step)
    def _(i):
        r = aligned(i * step, step)
        attended[r, :] = attended[r, :] + incoming[1, r, :].astype(f32)

    tokens_copy = pltpu.make_async_copy(attended, grad_tokens, local_sem.at[3])
    tokens_copy.start()
    sums.stage(2)
    Pump(scatter.lines(UP) + scatter.sides(QV, KO)).run()
    sums.stage(3)
    Pump(scatter.lasts(GATE, UP) + scatter.lines(QV, KO) + scatter.lasts(QV, KO)).run()
    sums.stage(4)
    def turn_to(rows_block, start):
        return pltpu.roll(rows_block, (width - start) % width, 1)

    dp = lax.axis_index("dp")
    piece = to_gains.shape[1]
    low_rows, high_rows = small_grads[0:8, :], small_grads[8:16, :]
    norm_part = turn_to(low_rows, (2 * dp + side) * piece)
    to_gains[...] = norm_part[0:2, :piece]
    to_offsets[...] = norm_part[2:6, :piece]
    to_qv_bias[...] = turn_to(low_rows, side * heads_wide + dp * to_qv_bias.shape[1])[6:8, : to_qv_bias.shape[1]]
    unit_piece = to_in_bias.shape[1]
    first_lane = dp * unit_piece
    unit_part = turn_to(high_rows, first_lane % width)
    per_half = units // width
    row = side * per_half + first_lane // width
    for index in range(2):
        chosen = sum(
            jnp.where(row == r, unit_part[2 * per_half * index + r : 2 * per_half * index + r + 1, :], 0.0)
            for r in range(2 * per_half)
        )
        to_in_bias[index : index + 1, :] = chosen[:, :unit_piece]
    output_copy.wait()
    tokens_copy.wait()
    gather.drain()
    scatter.drain()


def layer_call(grid, tokens, cotangent, lengths, qv_part, ko_part, in_part, low_part, high_part, smalls_in):
    rows, wide = qv_part.shape
    width = rows * grid.nz * 4
    half = tokens.shape[0]
    slots = 2 * half
    heads_wide = wide // 2
    units = in_part.shape[2]
    heads = heads_wide // HEAD
    shapes = [
        jax.ShapeDtypeStruct((half, width), bf16),
        jax.ShapeDtypeStruct((half, width), f32),
        jax.ShapeDtypeStruct((3, rows, heads_wide), f32),
        jax.ShapeDtypeStruct((heads_wide, rows), f32),
        jax.ShapeDtypeStruct(in_part.shape, f32),
        jax.ShapeDtypeStruct((units, rows), f32),
        *(jax.ShapeDtypeStruct(part.shape, f32) for part in smalls_in),
        jax.ShapeDtypeStruct((heads, slots, slots), bf16),
    ]
    vmem = pl.BlockSpec(memory_space=pltpu.VMEM)
    smem = pl.BlockSpec(memory_space=pltpu.SMEM)
    anywhere = pl.BlockSpec(memory_space=pl.ANY)
    smalls = small_slots(grid)
    dma = pltpu.SemaphoreType.DMA
    wides = (wide, wide, units, units, units // 2, units // 2)
    scratch = (
        [pltpu.VMEM((width, w), bf16) for w in wides]
        + [
            pltpu.VMEM((16, 128), f32),
            pltpu.VMEM((16, 256), f32),
            pltpu.VMEM((16 * grid.slots, 256), f32),
            pltpu.VMEM((16, width), f32),
            pltpu.VMEM((smalls, 16, width), f32),
            pltpu.VMEM((16, width), f32),
            pltpu.VMEM((slots, width), bf16),
            pltpu.VMEM((slots, 3 * heads_wide), bf16),
            pltpu.VMEM((slots, 128), f32),
            pltpu.VMEM((slots, heads_wide), bf16),
            pltpu.VMEM((slots, 3 * units), bf16),
            pltpu.VMEM((slots, 128), bf16),
            pltpu.VMEM((slots, 128), bf16),
            pltpu.VMEM((slots, 128), bf16),
            pltpu.VMEM((half, max(2 * slots - 256, 2 * width + 128)), f32),
            pltpu.VMEM((slots, width), bf16),
            pltpu.VMEM((slots, width), bf16),
            pltpu.VMEM((half, width), bf16),
            pltpu.VMEM((2, half, width), bf16),
            pltpu.VMEM((half, width), bf16),
            pltpu.VMEM((24, units), f32),
            pltpu.VMEM((width, slots), bf16),
            pltpu.VMEM((2, 128, slots), bf16),
            pltpu.VMEM((128, slots), bf16),
            pltpu.VMEM((128, slots), bf16),
        ]
        + [pltpu.VMEM((width, w), bf16) for w in wides]
        + [pltpu.VMEM((scatter_slots(grid), rows, w), bf16) for w in wides]
        + [
            dma((7, grid.slots)),
            dma((7, grid.slots)),
            dma((6, scatter_slots(grid))),
            dma((6, scatter_slots(grid))),
            dma((smalls,)),
            dma((smalls,)),
            dma((6,)),
            dma((9,)),
            dma((9,)),
            dma((5,)),
            dma((2,)),
        ]
    )
    results = pl.pallas_call(
        functools.partial(layer_body, grid, rows),
        out_shape=shapes,
        in_specs=[anywhere, anywhere, smem] + [anywhere] * 5 + [vmem] * 4,
        out_specs=[anywhere] * 2 + [vmem] * 8 + [anywhere],
        scratch_shapes=scratch,
        compiler_params=pltpu.CompilerParams(collective_id=0, has_side_effects=True, vmem_limit_bytes=VMEM_LIMIT),
        name="layer",
    )(tokens, cotangent, lengths, qv_part, ko_part, in_part, low_part, high_part, *smalls_in)
    return results[:10]


norm_epsilon = 1e-06


def norm_forward(values, gain_row, shift_row):
    centred = values - jnp.mean(values, axis=-1, keepdims=True)
    variance = jnp.mean(centred * centred, axis=-1, keepdims=True)
    inv_scale = lax.rsqrt(variance + norm_epsilon)
    unit_vals = centred * inv_scale
    return (unit_vals * gain_row + shift_row, unit_vals, inv_scale)


def norm_backward(grad_out, unit_vals, inv_scale, gain_row):
    grad_unit = grad_out * gain_row
    inner_term = (
        grad_unit
        - jnp.mean(grad_unit, axis=-1, keepdims=True)
        - unit_vals * jnp.mean(grad_unit * unit_vals, axis=-1, keepdims=True)
    )
    return (
        inner_term * inv_scale,
        jnp.sum(grad_out * unit_vals, axis=0),
        jnp.sum(grad_out, axis=0),
    )


def score_block(query_block, first_row, key_heads, slopes, key_valid):
    block_size = query_block.shape[0]
    heads_here = slopes.shape[0]
    query_heads = query_block.reshape(block_size, heads_here, HEAD)
    raw_scores = jnp.einsum(
        "qhc,khc->hqk", query_heads, key_heads, preferred_element_type=jnp.float32
    )
    query_pos = first_row + lax.iota(jnp.int32, block_size)
    key_pos = lax.iota(jnp.int32, key_heads.shape[0])
    distance = jnp.abs(query_pos[:, None] - key_pos[None, :]).astype(jnp.float32)
    scores = 0.125 * raw_scores - slopes[:, None, None] * distance[None, :, :]
    return (jnp.where(key_valid[None, None, :], scores, -1e30), query_heads)


def attend(queries, key_rows, value_rows, slopes, key_valid):
    slot_count, width_here = queries.shape
    heads_here = width_here // HEAD
    block_size = min(512, slot_count)
    key_heads = key_rows.reshape(slot_count, heads_here, HEAD)
    value_heads = value_rows.reshape(slot_count, heads_here, HEAD)

    def one_block(first_row):
        query_block = lax.dynamic_slice_in_dim(queries, first_row, block_size, 0)
        scores, query_heads = score_block(query_block, first_row, key_heads, slopes, key_valid)
        row_max = jnp.max(scores, axis=-1, keepdims=True)
        exp_scores = jnp.exp(scores - row_max)
        row_total = jnp.sum(exp_scores, axis=-1, keepdims=True)
        weights = (exp_scores / row_total).astype(jnp.bfloat16)
        mixed_block = jnp.einsum(
            "hqk,khc->qhc", weights, value_heads, preferred_element_type=jnp.float32
        )
        return (
            mixed_block.reshape(block_size, width_here).astype(jnp.bfloat16),
            (row_max + jnp.log(row_total))[..., 0],
        )

    first_rows = lax.iota(jnp.int32, slot_count // block_size) * block_size
    mixed_heads, logsum = lax.map(one_block, first_rows)
    return (mixed_heads.reshape(slot_count, width_here), logsum)


def attend_back(queries, key_rows, value_rows, grad_mixed, logsum, slopes, key_valid):
    slot_count, width_here = queries.shape
    heads_here = width_here // HEAD
    block_size = min(512, slot_count)
    key_heads = key_rows.reshape(slot_count, heads_here, HEAD)
    value_heads = value_rows.reshape(slot_count, heads_here, HEAD)

    def one_block(running, block_item):
        grad_keys, grad_values = running
        first_row, block_lse = block_item
        query_block = lax.dynamic_slice_in_dim(queries, first_row, block_size, 0)
        grad_block = lax.dynamic_slice_in_dim(grad_mixed, first_row, block_size, 0)
        scores, query_heads = score_block(query_block, first_row, key_heads, slopes, key_valid)
        probs = jnp.exp(scores - block_lse[..., None])
        grad_heads = grad_block.reshape(block_size, heads_here, HEAD)
        grad_probs = jnp.einsum(
            "qhc,khc->hqk", grad_heads, value_heads, preferred_element_type=jnp.float32
        )
        row_dot = jnp.sum(probs * grad_probs, axis=-1, keepdims=True)
        grad_scores = (probs * (grad_probs - row_dot)).astype(jnp.bfloat16)
        grad_query = 0.125 * jnp.einsum(
            "hqk,khc->qhc", grad_scores, key_heads, preferred_element_type=jnp.float32
        )
        grad_keys = grad_keys + 0.125 * jnp.einsum(
            "hqk,qhc->khc", grad_scores, query_heads, preferred_element_type=jnp.float32
        )
        grad_values = grad_values + jnp.einsum(
            "hqk,qhc->khc",
            probs.astype(jnp.bfloat16),
            grad_heads,
            preferred_element_type=jnp.float32,
        )
        return ((grad_keys, grad_values), grad_query.reshape(block_size, width_here))

    first_rows = lax.iota(jnp.int32, slot_count // block_size) * block_size
    zero_grads = jnp.zeros((slot_count, heads_here, HEAD), jnp.float32)
    (grad_keys, grad_values), grad_queries = lax.scan(
        one_block, (zero_grads, zero_grads), (first_rows, logsum)
    )
    return (
        grad_queries.reshape(slot_count, width_here),
        grad_keys.reshape(slot_count, width_here),
        grad_values.reshape(slot_count, width_here),
    )


def spread(part, index, count):
    wide = jnp.tile(part, (1, count))
    owner = lax.broadcasted_iota(jnp.int32, wide.shape, 1) // part.shape[1]
    return jnp.where(owner == index, wide.astype(jnp.float32), 0.0)


def pick(whole, index, count):
    size = whole.shape[1] // count
    return lax.dynamic_slice_in_dim(whole, index * size, size, 1)


def pack_small(biases_qv, biases_in, rows_all, piece, pieces):
    width = rows_all.shape[1]
    halves = [b if pieces == 1 else spread(b, piece, pieces) for b in (biases_qv, biases_in)]
    rows = [rows_all] + [h.reshape(-1, width) for h in halves]
    packed = jnp.concatenate(rows, axis=0)
    return jnp.pad(packed, ((0, -packed.shape[0] % 8), (0, 0)))


def unpack_small(packed, width_qv, width_in, piece, pieces):
    width = packed.shape[1]
    count_qv = 2 * width_qv * pieces // width
    count_in = 2 * width_in * pieces // width
    whole_qv = packed[6 : 6 + count_qv].reshape(2, -1)
    whole_in = packed[6 + count_qv : 6 + count_qv + count_in].reshape(2, -1)
    return packed[:6], pick(whole_qv, piece, pieces), pick(whole_in, piece, pieces)


def per_device(
    direct,
    tokens,
    lengths,
    qkv_weight,
    qv_bias,
    out_weight,
    in_weight,
    in_bias,
    down_weight,
    norm_gains,
    offsets,
    cotangent,
):
    row_count = tokens.shape[0]
    dp = lax.axis_size("dp")
    pieces = lax.axis_size("tensor")
    piece_index = lax.axis_index("tensor")
    dp_index = lax.axis_index("dp")
    flat_index = dp_index * pieces + piece_index
    grid = Grid3(dp)
    if direct:
        middle = down_weight.shape[0] // 2
        output, grad_tokens, to_qkv, to_out, to_in, to_down, to_gains, to_offsets, to_qv_bias, to_in_bias = layer_call(
            grid,
            tokens,
            cotangent,
            lengths,
            jnp.concatenate([qkv_weight[0], qkv_weight[2]], axis=1),
            jnp.concatenate([qkv_weight[1], out_weight.T], axis=1),
            in_weight,
            down_weight[:middle].T,
            down_weight[middle:].T,
            (norm_gains, offsets, qv_bias, in_bias),
        )
        return output, grad_tokens, to_qkv, to_qv_bias, to_out, to_in, to_in_bias, to_down, to_gains, to_offsets
    slot_count = row_count * pieces
    length = lengths[0]
    heads_here = qkv_weight.shape[2] // HEAD
    head_ids = (piece_index * heads_here + lax.iota(jnp.int32, heads_here)).astype(jnp.float32)
    slopes = jnp.exp2(-8.0 * (head_ids + 1.0) / (heads_here * pieces))
    key_valid = lax.iota(jnp.int32, slot_count) < length
    row_valid = (piece_index * row_count + lax.iota(jnp.int32, row_count) < length).astype(
        jnp.float32
    )[:, None]

    width_qv, width_in = qkv_weight.shape[2], in_weight.shape[2]
    parts = (qkv_weight, out_weight.T, in_weight, down_weight.T)
    small = pack_small(
        spread(qv_bias, dp_index, dp),
        spread(in_bias, dp_index, dp),
        jnp.concatenate([spread(norm_gains, flat_index, dp * pieces), spread(offsets, flat_index, dp * pieces)]),
        piece_index,
        pieces,
    )
    whole_qkv, whole_out_t, whole_in, whole_down_t = (
        lax.all_gather(p, "dp", axis=p.ndim - 2, tiled=True) for p in parts
    )
    small = lax.psum(small, ("dp", "tensor"))
    rows_all, whole_bqv, whole_bin = unpack_small(small, width_qv, width_in, piece_index, pieces)
    gains, shift_rows = rows_all[:2], rows_all[2:6]

    gathered = lax.all_gather(tokens, "tensor", axis=0, tiled=True)
    projected = jnp.einsum("sd,kdc->ksc", gathered, whole_qkv, preferred_element_type=jnp.float32)
    queries = (projected[0] + whole_bqv[0]).astype(jnp.bfloat16)
    key_rows = projected[1].astype(jnp.bfloat16)
    value_rows = (projected[2] + whole_bqv[1]).astype(jnp.bfloat16)
    mixed_heads, logsum = attend(queries, key_rows, value_rows, slopes, key_valid)
    attn_part = jnp.einsum("sc,dc->sd", mixed_heads, whole_out_t, preferred_element_type=jnp.float32)
    attn_total = lax.psum_scatter(
        attn_part.astype(jnp.bfloat16), "tensor", scatter_dimension=0, tiled=True
    ).astype(jnp.float32)
    first_in = tokens.astype(jnp.float32) + attn_total + shift_rows[0]
    attended, unit_one, scale_one = norm_forward(first_in, gains[0], shift_rows[1])
    attended_low = attended.astype(jnp.bfloat16)
    gathered_ff = lax.all_gather(attended_low, "tensor", axis=0, tiled=True)
    pre_acts = jnp.einsum("sd,kdc->ksc", gathered_ff, whole_in, preferred_element_type=jnp.float32)
    pre_acts = pre_acts + whole_bin[:, None, :]
    hidden = (jax.nn.gelu(pre_acts[0], approximate=False) * pre_acts[1]).astype(jnp.bfloat16)
    ff_part = jnp.einsum("sf,df->sd", hidden, whole_down_t, preferred_element_type=jnp.float32)
    ff_total = lax.psum_scatter(
        ff_part.astype(jnp.bfloat16), "tensor", scatter_dimension=0, tiled=True
    ).astype(jnp.float32)
    second_in = attended + ff_total + shift_rows[2]
    final_norm, unit_two, scale_two = norm_forward(second_in, gains[1], shift_rows[3])
    output = (final_norm * row_valid).astype(jnp.bfloat16)
    grad_final = cotangent.astype(jnp.float32) * row_valid
    grad_second, grad_gain_two, grad_shift_two = norm_backward(
        grad_final, unit_two, scale_two, gains[1]
    )
    grad_bdown = jnp.sum(grad_second, axis=0)
    grad_ff_rows = lax.all_gather(grad_second.astype(jnp.bfloat16), "tensor", axis=0, tiled=True)
    grad_down_t = jnp.einsum("sd,sf->df", grad_ff_rows, hidden, preferred_element_type=jnp.float32)
    grad_hidden = jnp.einsum("sd,df->sf", grad_ff_rows, whole_down_t, preferred_element_type=jnp.float32)
    pullback = jax.vjp(
        lambda gate_pre, up_pre: jax.nn.gelu(gate_pre, approximate=False) * up_pre,
        pre_acts[0],
        pre_acts[1],
    )[1]
    grad_gate, grad_up = pullback(grad_hidden)
    grad_pre = jnp.stack([grad_gate, grad_up]).astype(jnp.bfloat16)
    grad_bin = jnp.sum(grad_pre, axis=1, dtype=jnp.float32)
    grad_in = jnp.einsum("sd,ksc->kdc", gathered_ff, grad_pre, preferred_element_type=jnp.float32)
    ff_back = jnp.einsum("ksc,kdc->sd", grad_pre, whole_in, preferred_element_type=jnp.float32)
    grad_attended = grad_second + lax.psum_scatter(
        ff_back.astype(jnp.bfloat16), "tensor", scatter_dimension=0, tiled=True
    ).astype(jnp.float32)
    grad_first, grad_gain_one, grad_shift_one = norm_backward(
        grad_attended, unit_one, scale_one, gains[0]
    )
    grad_bout = jnp.sum(grad_first, axis=0)
    grad_attn_rows = lax.all_gather(grad_first.astype(jnp.bfloat16), "tensor", axis=0, tiled=True)
    grad_out_t = jnp.einsum("sd,sc->dc", grad_attn_rows, mixed_heads, preferred_element_type=jnp.float32)
    grad_mixed = jnp.einsum(
        "sd,dc->sc", grad_attn_rows, whole_out_t, preferred_element_type=jnp.float32
    ).astype(jnp.bfloat16)
    grad_queries, grad_keys, grad_values = attend_back(
        queries, key_rows, value_rows, grad_mixed, logsum, slopes, key_valid
    )
    grad_qkv = jnp.stack([grad_queries, grad_keys, grad_values]).astype(jnp.bfloat16)
    grad_wqkv = jnp.einsum("sd,ksc->kdc", gathered, grad_qkv, preferred_element_type=jnp.float32)
    grad_bqv = jnp.stack(
        [
            jnp.sum(grad_qkv[0], axis=0, dtype=jnp.float32),
            jnp.sum(grad_qkv[2], axis=0, dtype=jnp.float32),
        ]
    )
    input_back = jnp.einsum("ksc,kdc->sd", grad_qkv, whole_qkv, preferred_element_type=jnp.float32)
    grad_tokens = grad_first + lax.psum_scatter(
        input_back.astype(jnp.bfloat16), "tensor", scatter_dimension=0, tiled=True
    ).astype(jnp.float32)

    small_grads = pack_small(
        grad_bqv,
        grad_bin,
        jnp.stack([grad_gain_one, grad_gain_two, grad_bout, grad_shift_one, grad_bdown, grad_shift_two]),
        piece_index,
        pieces,
    )
    grads = tuple(g.astype(jnp.bfloat16) for g in (grad_wqkv, grad_out_t, grad_in, grad_down_t))
    shard_wqkv, shard_out_t, shard_in, shard_down_t = (
        lax.psum_scatter(g.astype(jnp.float32), "dp", scatter_dimension=g.ndim - 2, tiled=True) for g in grads
    )
    small_grads = lax.psum(small_grads, ("dp", "tensor"))
    row_grads, bqv_grads, bin_grads = unpack_small(small_grads, width_qv, width_in, piece_index, pieces)
    own_rows = pick(row_grads, flat_index, dp * pieces)
    return (
        output,
        grad_tokens,
        shard_wqkv,
        pick(bqv_grads, dp_index, dp),
        shard_out_t.T,
        shard_in,
        pick(bin_grads, dp_index, dp),
        shard_down_t.T,
        own_rows[:2],
        own_rows[2:],
    )


def solution(mesh):
    placed = (
        P(("dp", "tensor"), None),
        P("dp"),
        P(None, "dp", "tensor"),
        P(None, ("tensor", "dp")),
        P("tensor", "dp"),
        P(None, "dp", "tensor"),
        P(None, ("tensor", "dp")),
        P("tensor", "dp"),
        P(None, ("dp", "tensor")),
        P(None, ("dp", "tensor")),
        P(("dp", "tensor"), None),
    )

    def run(*args):
        dp = mesh.shape["dp"]
        direct = dp % 4 == 0 and (args[2].shape[1] // dp) % 16 == 0 and mesh.shape["tensor"] == 2
        return jax.shard_map(
            functools.partial(per_device, direct),
            mesh=mesh,
            in_specs=placed,
            out_specs=(
                P(("dp", "tensor"), None),
                P(("dp", "tensor"), None),
                P(None, "dp", "tensor"),
                P(None, ("tensor", "dp")),
                P("tensor", "dp"),
                P(None, "dp", "tensor"),
                P(None, ("tensor", "dp")),
                P("tensor", "dp"),
                P(None, ("dp", "tensor")),
                P(None, ("dp", "tensor")),
            ),
            check_vma=False,
        )(*args)

    return run
```

```python
import functools
import itertools

import jax
import jax.numpy as jnp
from jax import lax
from jax.experimental import pallas as pl
from jax.experimental.pallas import tpu as pltpu
from jax.sharding import PartitionSpec as P

HEAD = 64
MESH = pl.DeviceIdType.MESH
VMEM_LIMIT = 64 * 1024 * 1024 - 65536


class Grid3:
    def __init__(self, dp):
        self.nz = dp // 4
        self.slots = dp

    def here(self):
        me = lax.axis_index("dp")
        self.z, self.y, self.x = me // 4, (me // 2) % 2, me % 2
        z, nz = self.z, self.nz
        self.low, self.high = z > 0, z < nz - 1
        near = [sorted(range(1, nz), key=lambda k: (abs((p + k) % nz - p), k)) for p in range(nz)]
        self.by_distance = [(sum(jnp.where(z == p, near[p][j], 0) for p in range(nz)), 0, 0) for j in range(nz - 1)]
        self.line = []
        for d in self.by_distance:
            above = (z + d[0]) % nz > z
            self.line.append((above, jnp.where(above, z, nz - 1 - z) > 0))

    def at(self, dz, dy, dx):
        y = 1 - self.y if dy else self.y
        x = 1 - self.x if dx else self.x
        return (((self.z + dz) % self.nz) * 2 + y) * 2 + x

    def slot(self, d):
        return (d[0] % self.nz) * 4 + d[1] * 2 + d[2]

    def steps(self, axis):
        if axis == "z":
            return [(k, 0, 0) for k in range(1, self.nz)]
        return [(0, 1, 0)] if axis == "y" else [(0, 0, 1)]

    def seen_from(self, d, move):
        return ((d[0] - move[0] + self.nz) % self.nz, d[1] ^ move[1], d[2] ^ move[2])

    def span(self, axis):
        if axis == "z":
            return [(k, 0, 0) for k in range(self.nz)]
        return [(0, 0, 0), (0, 1, 0)] if axis == "y" else [(0, 0, 0), (0, 0, 1)]


def joined(*ds):
    return tuple(sum(part) for part in zip(*ds))


def remote(src, dst, send_sem, recv_sem, **device):
    return pltpu.make_async_remote_copy(
        src_ref=src, dst_ref=dst, send_sem=send_sem, recv_sem=recv_sem, device_id=device, device_id_type=MESH
    )


def greet(grid, partner):
    barrier = pltpu.get_barrier_semaphore()
    moves = [m for axis in "zyx" for m in grid.steps(axis)]
    for move in moves:
        pl.semaphore_signal(barrier, inc=1, device_id={"dp": grid.at(*move)}, device_id_type=MESH)
    pl.semaphore_signal(barrier, inc=1, device_id={"tensor": partner}, device_id_type=MESH)
    pl.semaphore_wait(barrier, len(moves) + 1)


class SmallSum:
    def __init__(self, grid, value, out, box, send, recv):
        self.grid = grid
        self.value, self.out, self.box, self.send, self.recv = value, out, box, send, recv
        self.copies = []

    def _post(self, slot, **device):
        copy = remote(self.out, self.box.at[slot], self.send.at[slot], self.recv.at[slot], **device)
        copy.start()
        self.copies.append(copy)

    def stage(self, number):
        grid = self.grid
        if number == 0:
            self.out[...] = self.value[...]
            self._post(0, tensor=1 - lax.axis_index("tensor"))
            return
        for copy in self.copies:
            copy.wait()
        self.copies = []
        if number == 1:
            self.out[...] = self.out[...] + self.box[0]
            self._post(1, dp=grid.at(0, 0, 1))
        elif number == 2:
            self.out[...] = self.out[...] + self.box[1]
            self._post(2, dp=grid.at(0, 1, 0))
        elif number == 3:
            self.out[...] = self.out[...] + self.box[2]
            for k in range(1, grid.nz):
                self._post(2 + k, dp=grid.at(k, 0, 0))
        else:
            total = self.out[...]
            for k in range(1, grid.nz):
                total = total + self.box[2 + k]
            self.out[...] = total


def small_slots(grid):
    return 2 + grid.nz


class Gather:
    def __init__(self, grid, chunks, send, recv):
        self.grid, self.chunks = grid, chunks
        self.send_sem, self.recv_sem = send, recv
        self.sent = []

    def _dst(self, number, d):
        rows = self.chunks[number][0].shape[0]
        return self.chunks[number][1].at[pl.ds(pl.multiple_of(self.grid.at(*d) * rows, rows), rows)]

    def _copy(self, number, d, move):
        dst = self._dst(number, d)
        if isinstance(move, int):
            move = (jnp.where(self.grid.line[move][0], -1, 1), 0, 0)
        source = self.chunks[number][0] if isinstance(d[0], int) and d == (0, 0, 0) else dst
        slot = self.grid.slot(self.grid.seen_from(d, move))
        return remote(source, dst, self.send_sem.at[number, slot], self.recv_sem.at[number, slot], dp=self.grid.at(*move))

    def _start(self, allowed, *args):
        if allowed is None:
            self._copy(*args).start()
        else:
            pl.when(allowed)(lambda: self._copy(*args).start())
        self.sent.append((allowed, args))

    def send(self, number, d, axis):
        if axis == "z":
            self._start(self.grid.low, number, d, (-1, 0, 0))
            self._start(self.grid.high, number, d, (1, 0, 0))
        else:
            self._start(None, number, d, self.grid.steps(axis)[0])

    def relay(self, number, d, j):
        self._start(self.grid.line[j][1], number, d, j)

    def arrive(self, number, d):
        dst, slot = self._dst(number, d), self.grid.slot(d)
        remote(dst, dst, self.send_sem.at[number, slot], self.recv_sem.at[number, slot], dp=self.grid.at(*d)).wait_recv()

    def moved(self, axis):
        return self.grid.by_distance if axis == "z" else self.grid.steps(axis)

    def first(self, number):
        return [(self.pass_first, number, d, j) for j, d in enumerate(self.moved(self.chunks[number][2][0]))]

    def second(self, number):
        one, two = self.chunks[number][2][:2]
        return [
            (self.pass_second, number, joined(a, b), j) for j, b in enumerate(self.moved(two)) for a in self.grid.span(one)
        ]

    def third(self, number):
        one, two, three = self.chunks[number][2]
        return [joined(a, b, c) for a in self.grid.span(one) for b in self.grid.span(two) for c in self.grid.steps(three)]

    def pass_first(self, number, d, j):
        order = self.chunks[number][2]
        self.arrive(number, d)
        if order[0] == "z":
            self.relay(number, d, j)
        for axis in order[1:]:
            self.send(number, d, axis)

    def pass_second(self, number, d, j):
        order = self.chunks[number][2]
        self.arrive(number, d)
        if order[1] == "z":
            self.relay(number, d, j)
        self.send(number, d, order[2])

    def finish(self, number):
        for d in self.third(number):
            self.arrive(number, d)

    def drain(self):
        for allowed, args in self.sent:
            if allowed is None:
                self._copy(*args).wait_send()
            else:
                pl.when(allowed)(lambda args=args: self._copy(*args).wait_send())
        self.sent = []


class Scatter:
    def __init__(self, grid, rows, chunks, send, recv):
        self.grid, self.rows, self.chunks = grid, rows, chunks
        self.send_sem, self.recv_sem = send, recv
        self.sent = []
        self.far_first = [2, 1, 3] if grid.nz == 4 else list(range(1, grid.nz))
        self.second, self.line, self.crossing = 2 * grid.nz, 3 * grid.nz - 1, 4 * grid.nz - 2

    def part(self, number, d):
        return self.chunks[number][0].at[pl.ds(pl.multiple_of(self.grid.at(*d) * self.rows, self.rows), self.rows)]

    def box(self, number, slot):
        return self.chunks[number][3].at[slot]

    def other(self, number):
        return "y" if self.chunks[number][2][0] == "x" else "x"

    def place(self, number, dz, e):
        return (dz, e, 0) if self.other(number) == "y" else (dz, 0, e)

    def _copy(self, number, kind, dz, e=0):
        grid = self.grid
        if kind == "own":
            move = grid.steps(self.chunks[number][2][0])[0]
            source, slot = self.part(number, joined(self.place(number, dz, e), move)), dz * 2 + e
        elif kind == "side":
            move = grid.steps(self.other(number))[0]
            source, slot = self.box(number, dz * 2 + 1), self.second + dz
        elif kind == "cross":
            move = grid.steps(self.other(number))[0]
            source, slot = self.box(number, 1), self.crossing
        elif kind == "middle":
            move = (dz, 0, 0)
            source, slot = self.box(number, dz * 2 + e), self.middle_slot(dz, e)
        else:
            move = (dz, 0, 0)
            source, slot = self.box(number, dz * 2), self.line + dz
        return remote(
            source, self.box(number, slot), self.send_sem.at[number, slot], self.recv_sem.at[number, slot], dp=grid.at(*move)
        )

    def _send(self, *args):
        self._copy(*args).start()
        self.sent.append(args)

    def _arrive(self, number, slot):
        box = self.box(number, slot)
        remote(box, box, self.send_sem.at[number, slot], self.recv_sem.at[number, slot], dp=0).wait_recv()

    def begin(self, number, *halves):
        for e in halves or (1, 0):
            for dz in self.far_first + [0]:
                self._send(number, "own", dz, e)

    def held(self, number, dz, e):
        slot = dz * 2 + e
        self._arrive(number, slot)
        return self.part(number, self.place(number, dz, e))[...].astype(jnp.float32) + self.box(number, slot)[...].astype(jnp.float32)

    def side(self, number, dz):
        self.box(number, dz * 2 + 1)[...] = self.held(number, dz, 1).astype(jnp.bfloat16)
        self._send(number, "side", dz)

    def both(self, number, dz):
        value = self.held(number, dz, 0)
        self._arrive(number, self.second + dz)
        return value + self.box(number, self.second + dz)[...].astype(jnp.float32)

    def along(self, number, dz):
        self.box(number, dz * 2)[...] = self.both(number, dz).astype(jnp.bfloat16)
        self._send(number, "line", dz)

    def middle_slot(self, dz, e):
        return self.second + e * (self.grid.nz - 1) + dz - 1

    def middle(self, number, dz, e):
        self.box(number, dz * 2 + e)[...] = self.held(number, dz, e).astype(jnp.bfloat16)
        self._send(number, "middle", dz, e)

    def line_total(self, number, e):
        total = self.held(number, 0, e)
        for dz in self.far_first:
            slot = self.middle_slot(dz, e)
            self._arrive(number, slot)
            total = total + self.box(number, slot)[...].astype(jnp.float32)
        return total

    def cross(self, number):
        self.box(number, 1)[...] = self.line_total(number, 1).astype(jnp.bfloat16)
        self._send(number, "cross", 0)

    def z_second(self, number):
        return self.chunks[number][2][1] == "z"

    def sides(self, *numbers):
        if self.z_second(numbers[0]):
            return [(self.middle, n, dz, e) for e in (1, 0) for dz in self.far_first for n in numbers]
        return [(self.side, n, dz) for dz in self.far_first + [0] for n in numbers]

    def lines(self, *numbers):
        if self.z_second(numbers[0]):
            return [(self.cross, n) for n in numbers]
        return [(self.along, n, dz) for dz in self.far_first for n in numbers]

    def lasts(self, *numbers):
        return [(self.last, n) for n in numbers]

    def last(self, number):
        if self.z_second(number):
            total = self.line_total(number, 0)
            self._arrive(number, self.crossing)
            total = total + self.box(number, self.crossing)[...].astype(jnp.float32)
        else:
            total = self.both(number, 0)
            for dz in self.far_first:
                self._arrive(number, self.line + dz)
                total = total + self.box(number, self.line + dz)[...].astype(jnp.float32)
        self.chunks[number][1](total)

    def drain(self):
        for args in self.sent:
            self._copy(*args).wait_send()
        self.sent = []


def scatter_slots(grid):
    return 4 * grid.nz - 1
bf16, f32 = jnp.bfloat16, jnp.float32
NORM_EPSILON = 1e-06
EARLY = 12
AFTER_PROJECTION = 4
GATHER_STEPS = 4
AFTER_OUT = 4
AFTER_NORM = 4
ROOT_HALF = 0.7071067811865476
PHI_SCALE = 0.3989422804014327


def nn(a, b):
    return jnp.dot(a, b, preferred_element_type=f32)


def nt(a, b):
    return lax.dot_general(a, b, (((1,), (1,)), ((), ())), preferred_element_type=f32)


def aligned(start, size):
    return pl.ds(pl.multiple_of(start, size), size)


def unit_rows(values):
    centred = values - jnp.mean(values, axis=-1, keepdims=True)
    variance = jnp.mean(centred * centred, axis=-1, keepdims=True)
    scale = lax.rsqrt(variance + NORM_EPSILON)
    return centred * scale, scale


def unit_back(grad_unit, unit, scale):
    inner = (
        grad_unit
        - jnp.mean(grad_unit, axis=-1, keepdims=True)
        - unit * jnp.mean(grad_unit * unit, axis=-1, keepdims=True)
    )
    return inner * scale


def fold(rows):
    return jnp.sum(rows.reshape(rows.shape[0] // 8, 8, rows.shape[1]), axis=0)


def merged(*lists):
    return [entry for row in itertools.zip_longest(*lists) for entry in row if entry is not None]


class Pump:
    def __init__(self, steps=()):
        self.steps = list(steps)

    def take(self, count=None):
        count = len(self.steps) if count is None else min(count, len(self.steps))
        taken, self.steps = self.steps[:count], self.steps[count:]
        return taken

    def run(self, count=None):
        for function, *args in self.take(count):
            function(*args)


def at_trips(*shares):
    def run(index):
        for trip, share in enumerate(shares):

            @pl.when(index == trip)
            def _(share=share):
                Pump(share).run()

    return run


def layer_body(
    grid, rows,
    tokens, cotangent, length, qkv_part, out_part, in_part, down_part, gains_part, offsets_part, qv_bias, in_bias,
    output, grad_tokens, to_qkv, to_out, to_in, to_down, to_gains, to_offsets, to_qv_bias, to_in_bias, probs_far,
    w_qv, w_ko, w_gate, w_up, w_low, w_high, small_mine, small_pair, small_tiles, every_small, small_box, small_grads,
    x, qkv, inverse, mixed, work, key_aug, value_aug, query_aug,
    rows_f32, attended_low, branch_rows, outgoing, incoming, cot, turned,
    grad_t, pair_b, grad_value_t, grad_key_t,
    g_qv, g_ko, g_gate, g_up, g_low, g_high, box_qv, box_ko, box_gate, box_up, box_low, box_high,
    gather_send, gather_recv, scatter_send, scatter_recv, small_send, small_recv, own_sem, swap_send, swap_recv, local_sem, prob_sem,
):
    grid.here()
    side = lax.axis_index("tensor")
    other = 1 - side
    half = tokens.shape[0]
    slots = 2 * half
    width = tokens.shape[1]
    heads_wide = mixed.shape[1]
    units = w_gate.shape[1]
    mine = aligned(side * half, half)
    count = length[0]
    attended, unit_one = rows_f32.at[:, pl.ds(0, width)], rows_f32.at[:, pl.ds(width, width)]
    scale_one = rows_f32.at[:, pl.ds(2 * width, 128)]
    block = 256
    span = 2 * slots - block
    bias = rows_f32.at[pl.ds(0, block), pl.ds(0, span)]

    own_rows = aligned(grid.at(0, 0, 0) * rows, rows)
    low, high = pl.ds(0, units // 2), pl.ds(units // 2, units // 2)
    one_head, two_head = pl.ds(0, heads_wide), pl.ds(heads_wide, heads_wide)
    own_copies = [
        pltpu.make_async_copy(source, target, own_sem.at[n])
        for n, (source, target) in enumerate(
            [
                (qkv_part.at[0], w_qv.at[own_rows, one_head]),
                (qkv_part.at[2], w_qv.at[own_rows, two_head]),
                (qkv_part.at[1], w_ko.at[own_rows, one_head]),
                (out_part, w_ko.at[own_rows, two_head]),
                (in_part.at[0], w_gate.at[own_rows]),
                (in_part.at[1], w_up.at[own_rows]),
                (down_part.at[:, low], w_low.at[own_rows]),
                (down_part.at[:, high], w_high.at[own_rows]),
            ]
        )
    ]
    for copy in own_copies:
        copy.start()
    greet(grid, other)

    gather = Gather(grid, [
        (w_qv.at[own_rows], w_qv, "zyx"),
        (w_ko.at[own_rows], w_ko, "zxy"),
        (w_gate.at[own_rows], w_gate, "yzx"),
        (w_up.at[own_rows], w_up, "xzy"),
        (w_low.at[own_rows], w_low, "zyx"),
        (w_high.at[own_rows], w_high, "zxy"),
        (small_pair, small_tiles, "zyx"),
    ], gather_send, gather_recv)
    def sink_qv(total):
        to_qkv[0], to_qkv[2] = total[:, :heads_wide], total[:, heads_wide:]

    def sink_ko(total):
        to_qkv[1] = total[:, :heads_wide]
        to_out[...] = total[:, heads_wide:]

    def sink_gate(total):
        to_in[0] = total

    def sink_up(total):
        to_in[1] = total

    def sink_low(total):
        to_down[:, : units // 2] = total

    def sink_high(total):
        to_down[:, units // 2 :] = total

    scatter = Scatter(grid, rows, [
        (g_qv, sink_qv, "xyz", box_qv),
        (g_ko, sink_ko, "yxz", box_ko),
        (g_gate, sink_gate, "xyz", box_gate),
        (g_up, sink_up, "yxz", box_up),
        (g_low, sink_low, "xzy", box_low),
        (g_high, sink_high, "yzx", box_high),
    ], scatter_send, scatter_recv)
    QV, KO, GATE, UP, LOW, HIGH, SMALL = range(7)

    def swap(source, target, slot):
        copy = remote(source, target, swap_send.at[slot], swap_recv.at[slot], tensor=other)
        copy.start()
        return copy

    token_swap = swap(tokens, x.at[mine], 0)
    token_copy = pltpu.make_async_copy(tokens, x.at[mine], local_sem.at[0])
    token_copy.start()
    cot_copy = pltpu.make_async_copy(cotangent, cot, local_sem.at[1])
    cot_copy.start()
    my_lanes = pl.ds(pl.multiple_of(side * 128, 128), 128)
    small_mine[...] = jnp.zeros_like(small_mine)
    small_mine[0:2, 0 : gains_part.shape[1]] = gains_part[...]
    small_mine[2:6, 0 : offsets_part.shape[1]] = offsets_part[...]
    small_mine[8:10, 0 : in_bias.shape[1]] = in_bias[...].astype(f32)
    small_mine[10:12, 0 : qv_bias.shape[1]] = qv_bias[...].astype(f32)
    small_pair[:, my_lanes] = small_mine[...]
    small_swap = swap(small_mine, small_pair.at[:, my_lanes], 8)
    pieces = {QV: (0, 1), KO: (2, 3), GATE: (4,), UP: (5,), LOW: (6,), HIGH: (7,)}
    for n in pieces:
        for piece in pieces[n]:
            own_copies[piece].wait()
        for axis in gather.chunks[n][2]:
            gather.send(n, (0, 0, 0), axis)
        if n == KO:
            small_swap.wait()
            for axis in gather.chunks[SMALL][2]:
                gather.send(SMALL, (0, 0, 0), axis)
            small_tiles[aligned(grid.at(0, 0, 0) * 16, 16), :] = small_pair[...]
    near_units = merged(gather.second(GATE), gather.second(UP))
    ends_first = merged(gather.first(LOW), gather.first(HIGH))
    ends_second = merged(gather.second(LOW), gather.second(HIGH))
    early = (
        merged(gather.first(QV), gather.first(SMALL), gather.first(KO))
        + merged(gather.first(GATE), gather.first(UP))
        + merged(merged(gather.second(QV), gather.second(SMALL), gather.second(KO)), near_units[:EARLY])
    )
    pump = Pump(early)
    pump.run()
    pump = Pump(merged(near_units[EARLY:], ends_first) + ends_second)
    token_copy.wait()
    token_swap.wait()
    for number in (SMALL, QV, KO):
        gather.finish(number)

    norm_rows = jnp.zeros((8, width), f32)
    head_rows = jnp.zeros((8, heads_wide), f32)
    unit_rows_in = jnp.zeros((8, units), f32)

    def at_lanes(tile, lanes, start):
        wide = jnp.concatenate([tile, jnp.zeros((8, lanes - 128), f32)], axis=1)
        return pltpu.roll(wide, start, 1) if start else wide

    for i in range(grid.slots):
        pair_tile = [small_tiles[16 * i : 16 * i + 8, 128 * s : 128 * s + 128] for s in range(2)]
        unit_tile = [small_tiles[16 * i + 8 : 16 * i + 16, 128 * s : 128 * s + 128] for s in range(2)]
        for s in range(2):
            norm_rows = norm_rows + at_lanes(pair_tile[s], width, (2 * i + s) * (rows // 2))
        units_here = jnp.where(side == 0, unit_tile[0], unit_tile[1])
        unit_rows_in = unit_rows_in + at_lanes(units_here, units, i * (units // grid.slots))
        head_rows = head_rows + at_lanes(pltpu.roll(units_here, 6, 0), heads_wide, i * (heads_wide // grid.slots))
    every_small[0:8, :] = norm_rows
    every_small[8:9, pl.ds(0, heads_wide)] = head_rows[0:1, :]
    every_small[8:9, pl.ds(heads_wide, heads_wide)] = head_rows[1:2, :]
    turned[0:8, :] = unit_rows_in

    q_cols, v_cols, k_cols = (pl.ds(i * heads_wide, heads_wide) for i in range(3))
    side_cols = pl.ds(pl.multiple_of(side * heads_wide, 128), heads_wide)
    row_bias = every_small[8:9, :]
    row_scale = jnp.where(lax.broadcasted_iota(jnp.int32, (1, 2 * heads_wide), 1) < heads_wide, 0.125, 1.0)

    @pl.loop(0, slots // 256)
    def _(i):
        r = aligned(i * 256, 256)
        raw = (nn(x[r, :], w_qv[...]) + row_bias).astype(bf16)
        qkv[r, pl.ds(0, 2 * heads_wide)] = (raw.astype(f32) * row_scale).astype(bf16)
        qkv[r, k_cols] = nn(x[r, :], w_ko[:, pl.ds(0, heads_wide)]).astype(bf16)

    pump.run(AFTER_PROJECTION)

    lane = lax.broadcasted_iota(jnp.int32, (slots, 128), 1)
    slot = lax.broadcasted_iota(jnp.int32, (slots, 128), 0)
    key_mask = jnp.where(slot < count, 0.0, -1e30).astype(bf16)
    zero, one = jnp.zeros((), bf16), jnp.ones((), bf16)
    block_lane = lax.broadcasted_iota(jnp.int32, (block, 128), 1)
    pairs = heads_wide // 128
    slopes = [2.0 ** (-8.0 * (h + 1) / (4 * pairs)) for h in range(4 * pairs)]

    def prob_slot(upper):
        return work.at[:, pl.ds(upper * slots, slots)]

    def prob_out(pair, upper):
        return pltpu.make_async_copy(prob_slot(upper), probs_far.at[2 * pair + upper], prob_sem.at[upper])

    def prob_in(pair, upper):
        return pltpu.make_async_copy(probs_far.at[2 * pair + upper], prob_slot(upper), prob_sem.at[upper])

    def pair_cols(pair, start=0):
        return pl.ds(pl.multiple_of(start + pair * 128, 128), 128)

    def attend_pair(pair):
        cols = pair_cols(pair)
        for upper in (0, 1):
            own = (lane >= 64) == (upper == 1)
            spare = 0 if upper else 64
            gap = jnp.abs(
                lax.broadcasted_iota(jnp.int32, (block, span), 0)
                - (lax.broadcasted_iota(jnp.int32, (block, span), 1) - (span - slots))
            )
            slope = sum(
                jnp.where(pair == p, jnp.where(side == 0, slopes[2 * p + upper], slopes[2 * (pairs + p) + upper]), 0.0)
                for p in range(pairs)
            )
            bias[...] = gap.astype(f32) * slope
            key_aug[...] = jnp.where(own, qkv[:, pair_cols(pair, 2 * heads_wide)], jnp.where(lane == spare, key_mask, zero))
            value_aug[...] = jnp.where(own, qkv[:, pair_cols(pair, heads_wide)], one)
            query_aug[...] = jnp.where(own, qkv[:, cols], jnp.where(lane == spare, one, zero))

            @pl.when(pair > 0)
            def _(upper=upper):
                prob_out(pair - 1, upper).wait()

            def attend(i, inner_carry, upper=upper):
                r = aligned(i * block, block)
                scores = nt(query_aug[r, :], key_aug[...]) - bias[:, pl.ds(pl.multiple_of(span - slots - i * block, block), slots)]
                top = jnp.max(scores, axis=1, keepdims=True)
                weights = jnp.exp(scores - top).astype(bf16)
                work[r, pl.ds(upper * slots, slots)] = weights
                product = nn(weights, value_aug[...])
                scale = 1.0 / (product[:, 0:1] if upper else product[:, 64:65])
                result = (product * scale).astype(bf16)
                inverse[r, :] = jnp.where(block_lane == 2 * pair + upper, scale, inverse[r, :])
                mixed[r, cols] = jnp.where(block_lane < 64, mixed[r, cols], result) if upper else result
                return inner_carry

            lax.fori_loop(0, slots // block, attend, 0, unroll=2)
            prob_out(pair, upper).start()
        between_pairs(pair)

    inverse[...] = jnp.zeros_like(inverse)
    between_pairs = at_trips(*(pump.take(GATHER_STEPS) for _ in range(pairs)))
    pl.loop(0, pairs)(attend_pair)

    def project(source, weights, target_rows, sink):
        @pl.loop(0, half // 256)
        def _(i):
            r = aligned(target_rows * half + i * 256, 256)
            sink(i, nt(source[r, :], weights[...]))

    def to_outgoing(i, value):
        outgoing[aligned(i * 256, 256), :] = value.astype(bf16)

    def to_attended(i, value):
        attended[aligned(i * 256, 256), :] = value

    w_out = w_ko.at[:, pl.ds(heads_wide, heads_wide)]
    project(mixed, w_out, other, to_outgoing)
    first_swap = swap(outgoing, incoming.at[0], 1)
    pump.run(AFTER_OUT)
    project(mixed, w_out, side, to_attended)
    first_swap.wait()
    gain_one, gain_two = every_small[0:1, :], every_small[1:2, :]
    step = 64

    @pl.loop(0, half // step)
    def _(i):
        r = aligned(i * step, step)
        own = pl.ds(pl.multiple_of(side * half + i * step, step), step)
        total = x[own, :].astype(f32) + attended[r, :] + incoming[0, r, :].astype(f32) + every_small[2:3, :]
        unit, scale = unit_rows(total)
        result = unit * gain_one + every_small[3:4, :]
        unit_one[r, :] = unit
        scale_one[r, :] = jnp.broadcast_to(scale, (step, 128))
        attended[r, :] = result
        attended_low[own, :] = result.astype(bf16)

    low_swap = swap(attended_low.at[mine], attended_low.at[mine], 2)
    for upper in (0, 1):
        prob_out(pairs - 1, upper).wait()
    pump.run(AFTER_NORM)
    gather.finish(GATE)
    gather.finish(UP)

    def feed(rows_side):
        r = aligned(rows_side * half, half)

        @pl.loop(0, units // 256)
        def _(j):
            c = aligned(j * 256, 256)
            c_up = pl.ds(pl.multiple_of(units + j * 256, 256), 256)
            c_hidden = pl.ds(pl.multiple_of(2 * units + j * 256, 256), 256)
            gate = nn(attended_low[r, :], w_gate[:, c]) + turned[0:1, c]
            up = nn(attended_low[r, :], w_up[:, c]) + turned[1:2, c]
            below = 0.5 * (1.0 + lax.erf(gate * ROOT_HALF))
            density = PHI_SCALE * jnp.exp(-0.5 * gate * gate)
            bent = gate * below
            work[r, c_hidden] = (bent * up).astype(bf16)
            work[r, c] = (up * (below + gate * density)).astype(bf16)
            work[r, c_up] = bent.astype(bf16)

    feed(side)
    pump.run()
    low_swap.wait()
    feed(other)
    pump.run()
    gather.finish(LOW)
    gather.finish(HIGH)

    hidden_low, hidden_high = pl.ds(2 * units, units // 2), pl.ds(2 * units + units // 2, units // 2)

    def down(rows_side, sink):
        @pl.loop(0, half // 256)
        def _(i):
            r = aligned(rows_side * half + i * 256, 256)
            sink(i, nt(work[r, hidden_low], w_low[...]) + nt(work[r, hidden_high], w_high[...]))

    def add_attended(i, value):
        r = aligned(i * 256, 256)
        attended[r, :] = attended[r, :] + value

    down(other, to_outgoing)
    second_swap = swap(outgoing, incoming.at[1], 3)
    down(side, add_attended)
    cot_copy.wait()
    second_swap.wait()
    nothing = jnp.zeros((8, width), f32)

    def second_norm(i, carry):
        sum_gain, sum_shift, sum_branch = carry
        r = aligned(i * step, step)
        own = pl.ds(pl.multiple_of(side * half + i * step, step), step)
        position = side * half + i * step + lax.broadcasted_iota(jnp.int32, (step, 1), 0)
        valid = jnp.where(position < count, 1.0, 0.0)
        unit, scale = unit_rows(attended[r, :] + incoming[1, r, :].astype(f32) + every_small[4:5, :])
        grad = cot[r, :].astype(f32) * valid
        cot[r, :] = ((unit * gain_two + every_small[5:6, :]) * valid).astype(bf16)
        back = unit_back(grad * gain_two, unit, scale)
        attended[r, :] = back
        branch_rows[own, :] = back.astype(bf16)
        return sum_gain + fold(grad * unit), sum_shift + fold(grad), sum_branch + fold(back)

    gain_two_sum, shift_two_sum, down_bias_sum = lax.fori_loop(0, half // step, second_norm, (nothing,) * 3)
    branch_swap = swap(branch_rows.at[mine], branch_rows.at[mine], 4)
    output_copy = pltpu.make_async_copy(cot, output, local_sem.at[2])
    output_copy.start()
    small_grads[...] = jnp.zeros_like(small_grads)
    small_grads[1:2, :] = jnp.sum(gain_two_sum, axis=0, keepdims=True)
    small_grads[5:6, :] = jnp.sum(shift_two_sum, axis=0, keepdims=True)
    small_grads[4:5, :] = jnp.sum(down_bias_sum, axis=0, keepdims=True)
    branch_swap.wait()

    def turn(source):
        @pl.loop(0, slots // 256)
        def _(i):
            r = aligned(i * 256, 256)
            grad_t[:, r] = source[r, :].T

    def weight_grad(sink, source, source_start, tile):
        @pl.loop(0, sink.shape[1] // tile)
        def _(j):
            sink[:, aligned(j * tile, tile)] = nn(
                grad_t[...], source[:, pl.ds(pl.multiple_of(source_start + j * tile, tile), tile)]
            ).astype(bf16)

    turn(branch_rows)
    weight_grad(g_low, work, 2 * units, 256)
    scatter.begin(LOW)
    weight_grad(g_high, work, 2 * units + units // 2, 256)
    scatter.begin(HIGH)

    turned[8:24, :] = jnp.zeros((16, units), f32)
    for index, weights in enumerate((w_low, w_high)):
        @pl.loop(0, units // 2 // 256)
        def _(j, index=index, weights=weights):
            c = pl.ds(pl.multiple_of(index * (units // 2) + j * 256, 256), 256)
            c_up = pl.ds(pl.multiple_of(units + index * (units // 2) + j * 256, 256), 256)
            for part in range(2):
                r = pl.ds(part * half, half)
                grad = nn(branch_rows[r, :], weights[:, aligned(j * 256, 256)])
                gate_grad = (grad * work[r, c].astype(f32)).astype(bf16)
                up_grad = (grad * work[r, c_up].astype(f32)).astype(bf16)
                work[r, c] = gate_grad
                work[r, c_up] = up_grad
                turned[8:16, c] = turned[8:16, c] + fold(gate_grad.astype(f32))
                turned[16:24, c] = turned[16:24, c] + fold(up_grad.astype(f32))

    for index in range(2):
        total = jnp.sum(turned[8 + 8 * index : 16 + 8 * index, :], axis=0, keepdims=True)
        for j in range(units // width):
            small_grads[pl.ds(8 + 4 * index + 2 * side + j, 1), :] = total[:, j * width : (j + 1) * width]

    sides_ends = Pump(scatter.sides(LOW, HIGH))
    sides_ends.run(6)
    turn(attended_low)
    weight_grad(g_gate, work, 0, 512)
    scatter.begin(GATE, 1)
    weight_grad(g_up, work, units, 512)
    scatter.begin(UP, 1)
    scatter.begin(GATE, 0)
    sides_ends.run()

    gate_cols, up_cols = pl.ds(0, units), pl.ds(units, units)

    def units_back(rows_side, sink):
        @pl.loop(0, half // 256)
        def _(i):
            r = aligned(rows_side * half + i * 256, 256)
            sink(i, nt(work[r, gate_cols], w_gate[...]) + nt(work[r, up_cols], w_up[...]))

    units_back(other, to_outgoing)
    third_swap = swap(outgoing, incoming.at[0], 5)
    units_back(side, add_attended)
    Pump(scatter.lines(LOW, HIGH)).run()
    third_swap.wait()

    def first_norm_back(i, carry):
        sum_gain, sum_shift, sum_branch = carry
        r = aligned(i * step, step)
        own = pl.ds(pl.multiple_of(side * half + i * step, step), step)
        grad = attended[r, :] + incoming[0, r, :].astype(f32)
        unit = unit_one[r, :]
        back = unit_back(grad * gain_one, unit, scale_one[r, 0:1])
        attended[r, :] = back
        branch_rows[own, :] = back.astype(bf16)
        return sum_gain + fold(grad * unit), sum_shift + fold(grad), sum_branch + fold(back)

    prob_in(0, 0).start()
    prob_in(0, 1).start()
    gain_one_sum, shift_one_sum, out_bias_sum = lax.fori_loop(0, half // step, first_norm_back, (nothing,) * 3)
    attn_swap = swap(branch_rows.at[mine], branch_rows.at[mine], 6)
    small_grads[0:1, :] = jnp.sum(gain_one_sum, axis=0, keepdims=True)
    small_grads[3:4, :] = jnp.sum(shift_one_sum, axis=0, keepdims=True)
    small_grads[2:3, :] = jnp.sum(out_bias_sum, axis=0, keepdims=True)
    attn_swap.wait()

    grad_mixed = attended_low.at[:, pl.ds(0, heads_wide)]
    turn(branch_rows)
    g_ko[:, pl.ds(heads_wide, heads_wide)] = nn(grad_t[...], mixed[...]).astype(bf16)
    sides_gate = Pump(scatter.sides(GATE))
    sides_gate.run(2)

    @pl.loop(0, slots // 256)
    def _(i):
        r = aligned(i * 256, 256)
        grad_mixed[r, :] = nn(branch_rows[r, :], w_out[...]).astype(bf16)

    sides_gate.run()
    scatter.begin(UP, 0)

    mixed_t, query_t = pair_b.at[0], pair_b.at[1]

    def pair_back(pair):
        cols, key_cols, value_cols = pair_cols(pair), pair_cols(pair, 2 * heads_wide), pair_cols(pair, heads_wide)
        scales = inverse[...]
        shrink = jnp.where(
            lane < 64,
            jnp.sum(jnp.where(lane == 2 * pair, scales, 0.0), axis=1, keepdims=True),
            jnp.sum(jnp.where(lane == 2 * pair + 1, scales, 0.0), axis=1, keepdims=True),
        )
        scaled = (grad_mixed[:, cols].astype(f32) * shrink).astype(bf16)
        mixed_t[...] = scaled.T
        query_t[...] = qkv[:, cols].T
        outgoing_pair[...] = scaled
        for upper in (0, 1):
            own = (lane >= 64) == (upper == 1)
            spare = 0 if upper else 64
            scaled = outgoing_pair[...]
            dots = jnp.sum(jnp.where(own, scaled.astype(f32) * mixed[:, cols].astype(f32), 0.0), axis=1, keepdims=True)
            dots_high = dots.astype(bf16)
            dots_low = (dots - dots_high.astype(f32)).astype(bf16)
            ones = (lane == spare) | (lane == spare + 1)
            value_aug[...] = jnp.where(own, qkv[:, value_cols], jnp.where(ones, one, zero))
            query_aug[...] = jnp.where(
                own, scaled, jnp.where(lane == spare, -dots_high, jnp.where(lane == spare + 1, -dots_low, zero))
            )
            part = pl.ds(64 * upper, 64)
            base = upper * slots
            prob_in(pair, upper).wait()
            for j in range(slots // 512):
                c = pl.ds(j * 512, 512)
                grad_value_t[part, c] = nn(mixed_t[part, :], work[:, pl.ds(base + j * 512, 512)]).astype(bf16)

            def attend_back(i, inner_carry, upper=upper, base=base):
                r = aligned(i * block, block)
                inner = nt(query_aug[r, :], value_aug[...])
                grads = (work[r, pl.ds(base, slots)].astype(f32) * inner).astype(bf16)
                work[r, pl.ds(base, slots)] = grads
                result = (nn(grads, qkv[:, key_cols]) * 0.125).astype(bf16)
                qkv[r, cols] = jnp.where(block_lane < 64, qkv[r, cols], result) if upper else result
                return inner_carry

            lax.fori_loop(0, slots // block, attend_back, 0, unroll=2)
            for j in range(slots // 512):
                c = pl.ds(j * 512, 512)
                grad_key_t[part, c] = nn(query_t[part, :], work[:, pl.ds(base + j * 512, 512)]).astype(bf16)

            @pl.when(pair + 1 < pairs)
            def _(upper=upper):
                prob_in(pair + 1, upper).start()

        qkv[:, value_cols] = grad_value_t[...].T
        qkv[:, key_cols] = grad_key_t[...].T
        between_pairs(pair)

    outgoing_pair = key_aug
    between_pairs = at_trips(scatter.sides(UP), scatter.lasts(LOW, HIGH), scatter.lines(GATE))
    pl.loop(0, pairs)(pair_back)

    turn(x)
    g_qv[...] = nn(grad_t[...], qkv[:, pl.ds(0, 2 * heads_wide)]).astype(bf16)
    scatter.begin(QV)
    g_ko[:, pl.ds(0, heads_wide)] = nn(grad_t[...], qkv[:, k_cols]).astype(bf16)
    scatter.begin(KO)
    def column_sum(cols):
        def add(i, carry):
            return carry + fold(qkv[aligned(i * 128, 128), cols].astype(f32))

        return jnp.sum(lax.fori_loop(0, slots // 128, add, jnp.zeros((8, heads_wide), f32)), axis=0, keepdims=True)

    small_grads[6:7, side_cols] = column_sum(q_cols)
    small_grads[7:8, side_cols] = column_sum(v_cols)
    sums = SmallSum(grid, small_grads, small_grads, small_box, small_send, small_recv)
    sums.stage(0)

    def inputs_back(rows_side, sink):
        @pl.loop(0, half // 256)
        def _(i):
            r = aligned(rows_side * half + i * 256, 256)
            sink(
                i,
                nt(qkv[r, pl.ds(0, 2 * heads_wide)], w_qv[...]) + nt(qkv[r, k_cols], w_ko[:, pl.ds(0, heads_wide)]),
            )

    inputs_back(other, to_outgoing)
    fourth_swap = swap(outgoing, incoming.at[1], 7)
    sums.stage(1)
    inputs_back(side, add_attended)
    fourth_swap.wait()

    @pl.loop(0, half // step)
    def _(i):
        r = aligned(i * step, step)
        attended[r, :] = attended[r, :] + incoming[1, r, :].astype(f32)

    tokens_copy = pltpu.make_async_copy(attended, grad_tokens, local_sem.at[3])
    tokens_copy.start()
    sums.stage(2)
    Pump(scatter.lines(UP) + scatter.sides(QV, KO)).run()
    sums.stage(3)
    Pump(scatter.lasts(GATE, UP) + scatter.lines(QV, KO) + scatter.lasts(QV, KO)).run()
    sums.stage(4)
    def turn_to(rows_block, start):
        return pltpu.roll(rows_block, (width - start) % width, 1)

    dp = lax.axis_index("dp")
    piece = to_gains.shape[1]
    low_rows, high_rows = small_grads[0:8, :], small_grads[8:16, :]
    norm_part = turn_to(low_rows, (2 * dp + side) * piece)
    to_gains[...] = norm_part[0:2, :piece]
    to_offsets[...] = norm_part[2:6, :piece]
    to_qv_bias[...] = turn_to(low_rows, side * heads_wide + dp * to_qv_bias.shape[1])[6:8, : to_qv_bias.shape[1]]
    unit_piece = to_in_bias.shape[1]
    first_lane = dp * unit_piece
    unit_part = turn_to(high_rows, first_lane % width)
    per_half = units // width
    row = side * per_half + first_lane // width
    for index in range(2):
        chosen = sum(
            jnp.where(row == r, unit_part[2 * per_half * index + r : 2 * per_half * index + r + 1, :], 0.0)
            for r in range(2 * per_half)
        )
        to_in_bias[index : index + 1, :] = chosen[:, :unit_piece]
    output_copy.wait()
    tokens_copy.wait()
    gather.drain()
    scatter.drain()


def layer_call(grid, tokens, cotangent, lengths, qkv_part, out_part, in_part, down_part, smalls_in):
    rows, heads_wide = out_part.shape
    wide = 2 * heads_wide
    width = rows * grid.nz * 4
    half = tokens.shape[0]
    slots = 2 * half
    units = in_part.shape[2]
    heads = heads_wide // HEAD
    shapes = [
        jax.ShapeDtypeStruct((half, width), bf16),
        jax.ShapeDtypeStruct((half, width), f32),
        jax.ShapeDtypeStruct((3, rows, heads_wide), f32),
        jax.ShapeDtypeStruct((rows, heads_wide), f32),
        jax.ShapeDtypeStruct(in_part.shape, f32),
        jax.ShapeDtypeStruct((rows, units), f32),
        *(jax.ShapeDtypeStruct(part.shape, f32) for part in smalls_in),
        jax.ShapeDtypeStruct((heads, slots, slots), bf16),
    ]
    vmem = pl.BlockSpec(memory_space=pltpu.VMEM)
    smem = pl.BlockSpec(memory_space=pltpu.SMEM)
    anywhere = pl.BlockSpec(memory_space=pl.ANY)
    smalls = small_slots(grid)
    dma = pltpu.SemaphoreType.DMA
    wides = (wide, wide, units, units, units // 2, units // 2)
    scratch = (
        [pltpu.VMEM((width, w), bf16) for w in wides]
        + [
            pltpu.VMEM((16, 128), f32),
            pltpu.VMEM((16, 256), f32),
            pltpu.VMEM((16 * grid.slots, 256), f32),
            pltpu.VMEM((16, width), f32),
            pltpu.VMEM((smalls, 16, width), f32),
            pltpu.VMEM((16, width), f32),
            pltpu.VMEM((slots, width), bf16),
            pltpu.VMEM((slots, 3 * heads_wide), bf16),
            pltpu.VMEM((slots, 128), f32),
            pltpu.VMEM((slots, heads_wide), bf16),
            pltpu.VMEM((slots, 3 * units), bf16),
            pltpu.VMEM((slots, 128), bf16),
            pltpu.VMEM((slots, 128), bf16),
            pltpu.VMEM((slots, 128), bf16),
            pltpu.VMEM((half, max(2 * slots - 256, 2 * width + 128)), f32),
            pltpu.VMEM((slots, width), bf16),
            pltpu.VMEM((slots, width), bf16),
            pltpu.VMEM((half, width), bf16),
            pltpu.VMEM((2, half, width), bf16),
            pltpu.VMEM((half, width), bf16),
            pltpu.VMEM((24, units), f32),
            pltpu.VMEM((width, slots), bf16),
            pltpu.VMEM((2, 128, slots), bf16),
            pltpu.VMEM((128, slots), bf16),
            pltpu.VMEM((128, slots), bf16),
        ]
        + [pltpu.VMEM((width, w), bf16) for w in wides]
        + [pltpu.VMEM((scatter_slots(grid), rows, w), bf16) for w in wides]
        + [
            dma((7, grid.slots)),
            dma((7, grid.slots)),
            dma((6, scatter_slots(grid))),
            dma((6, scatter_slots(grid))),
            dma((smalls,)),
            dma((smalls,)),
            dma((8,)),
            dma((9,)),
            dma((9,)),
            dma((5,)),
            dma((2,)),
        ]
    )
    results = pl.pallas_call(
        functools.partial(layer_body, grid, rows),
        out_shape=shapes,
        in_specs=[anywhere, anywhere, smem] + [anywhere] * 4 + [vmem] * 4,
        out_specs=[anywhere] * 2 + [vmem] * 8 + [anywhere],
        scratch_shapes=scratch,
        compiler_params=pltpu.CompilerParams(collective_id=0, has_side_effects=True, vmem_limit_bytes=VMEM_LIMIT),
        name="layer",
    )(tokens, cotangent, lengths, qkv_part, out_part, in_part, down_part, *smalls_in)
    return results[:10]


norm_epsilon = 1e-06


def norm_forward(values, gain_row, shift_row):
    centred = values - jnp.mean(values, axis=-1, keepdims=True)
    variance = jnp.mean(centred * centred, axis=-1, keepdims=True)
    inv_scale = lax.rsqrt(variance + norm_epsilon)
    unit_vals = centred * inv_scale
    return (unit_vals * gain_row + shift_row, unit_vals, inv_scale)


def norm_backward(grad_out, unit_vals, inv_scale, gain_row):
    grad_unit = grad_out * gain_row
    inner_term = (
        grad_unit
        - jnp.mean(grad_unit, axis=-1, keepdims=True)
        - unit_vals * jnp.mean(grad_unit * unit_vals, axis=-1, keepdims=True)
    )
    return (
        inner_term * inv_scale,
        jnp.sum(grad_out * unit_vals, axis=0),
        jnp.sum(grad_out, axis=0),
    )


def score_block(query_block, first_row, key_heads, slopes, key_valid):
    block_size = query_block.shape[0]
    heads_here = slopes.shape[0]
    query_heads = query_block.reshape(block_size, heads_here, HEAD)
    raw_scores = jnp.einsum(
        "qhc,khc->hqk", query_heads, key_heads, preferred_element_type=jnp.float32
    )
    query_pos = first_row + lax.iota(jnp.int32, block_size)
    key_pos = lax.iota(jnp.int32, key_heads.shape[0])
    distance = jnp.abs(query_pos[:, None] - key_pos[None, :]).astype(jnp.float32)
    scores = 0.125 * raw_scores - slopes[:, None, None] * distance[None, :, :]
    return (jnp.where(key_valid[None, None, :], scores, -1e30), query_heads)


def attend(queries, key_rows, value_rows, slopes, key_valid):
    slot_count, width_here = queries.shape
    heads_here = width_here // HEAD
    block_size = min(512, slot_count)
    key_heads = key_rows.reshape(slot_count, heads_here, HEAD)
    value_heads = value_rows.reshape(slot_count, heads_here, HEAD)

    def one_block(first_row):
        query_block = lax.dynamic_slice_in_dim(queries, first_row, block_size, 0)
        scores, query_heads = score_block(query_block, first_row, key_heads, slopes, key_valid)
        row_max = jnp.max(scores, axis=-1, keepdims=True)
        exp_scores = jnp.exp(scores - row_max)
        row_total = jnp.sum(exp_scores, axis=-1, keepdims=True)
        weights = (exp_scores / row_total).astype(jnp.bfloat16)
        mixed_block = jnp.einsum(
            "hqk,khc->qhc", weights, value_heads, preferred_element_type=jnp.float32
        )
        return (
            mixed_block.reshape(block_size, width_here).astype(jnp.bfloat16),
            (row_max + jnp.log(row_total))[..., 0],
        )

    first_rows = lax.iota(jnp.int32, slot_count // block_size) * block_size
    mixed_heads, logsum = lax.map(one_block, first_rows)
    return (mixed_heads.reshape(slot_count, width_here), logsum)


def attend_back(queries, key_rows, value_rows, grad_mixed, logsum, slopes, key_valid):
    slot_count, width_here = queries.shape
    heads_here = width_here // HEAD
    block_size = min(512, slot_count)
    key_heads = key_rows.reshape(slot_count, heads_here, HEAD)
    value_heads = value_rows.reshape(slot_count, heads_here, HEAD)

    def one_block(running, block_item):
        grad_keys, grad_values = running
        first_row, block_lse = block_item
        query_block = lax.dynamic_slice_in_dim(queries, first_row, block_size, 0)
        grad_block = lax.dynamic_slice_in_dim(grad_mixed, first_row, block_size, 0)
        scores, query_heads = score_block(query_block, first_row, key_heads, slopes, key_valid)
        probs = jnp.exp(scores - block_lse[..., None])
        grad_heads = grad_block.reshape(block_size, heads_here, HEAD)
        grad_probs = jnp.einsum(
            "qhc,khc->hqk", grad_heads, value_heads, preferred_element_type=jnp.float32
        )
        row_dot = jnp.sum(probs * grad_probs, axis=-1, keepdims=True)
        grad_scores = (probs * (grad_probs - row_dot)).astype(jnp.bfloat16)
        grad_query = 0.125 * jnp.einsum(
            "hqk,khc->qhc", grad_scores, key_heads, preferred_element_type=jnp.float32
        )
        grad_keys = grad_keys + 0.125 * jnp.einsum(
            "hqk,qhc->khc", grad_scores, query_heads, preferred_element_type=jnp.float32
        )
        grad_values = grad_values + jnp.einsum(
            "hqk,qhc->khc",
            probs.astype(jnp.bfloat16),
            grad_heads,
            preferred_element_type=jnp.float32,
        )
        return ((grad_keys, grad_values), grad_query.reshape(block_size, width_here))

    first_rows = lax.iota(jnp.int32, slot_count // block_size) * block_size
    zero_grads = jnp.zeros((slot_count, heads_here, HEAD), jnp.float32)
    (grad_keys, grad_values), grad_queries = lax.scan(
        one_block, (zero_grads, zero_grads), (first_rows, logsum)
    )
    return (
        grad_queries.reshape(slot_count, width_here),
        grad_keys.reshape(slot_count, width_here),
        grad_values.reshape(slot_count, width_here),
    )


def spread(part, index, count):
    wide = jnp.tile(part, (1, count))
    owner = lax.broadcasted_iota(jnp.int32, wide.shape, 1) // part.shape[1]
    return jnp.where(owner == index, wide.astype(jnp.float32), 0.0)


def pick(whole, index, count):
    size = whole.shape[1] // count
    return lax.dynamic_slice_in_dim(whole, index * size, size, 1)


def pack_small(biases_qv, biases_in, rows_all, piece, pieces):
    width = rows_all.shape[1]
    halves = [b if pieces == 1 else spread(b, piece, pieces) for b in (biases_qv, biases_in)]
    rows = [rows_all] + [h.reshape(-1, width) for h in halves]
    packed = jnp.concatenate(rows, axis=0)
    return jnp.pad(packed, ((0, -packed.shape[0] % 8), (0, 0)))


def unpack_small(packed, width_qv, width_in, piece, pieces):
    width = packed.shape[1]
    count_qv = 2 * width_qv * pieces // width
    count_in = 2 * width_in * pieces // width
    whole_qv = packed[6 : 6 + count_qv].reshape(2, -1)
    whole_in = packed[6 + count_qv : 6 + count_qv + count_in].reshape(2, -1)
    return packed[:6], pick(whole_qv, piece, pieces), pick(whole_in, piece, pieces)


def per_device(
    direct,
    tokens,
    lengths,
    qkv_weight,
    qv_bias,
    out_weight,
    in_weight,
    in_bias,
    down_weight,
    norm_gains,
    offsets,
    cotangent,
):
    row_count = tokens.shape[0]
    dp = lax.axis_size("dp")
    pieces = lax.axis_size("tensor")
    piece_index = lax.axis_index("tensor")
    dp_index = lax.axis_index("dp")
    flat_index = dp_index * pieces + piece_index
    grid = Grid3(dp)
    if direct:
        output, grad_tokens, to_qkv, to_out, to_in, to_down, to_gains, to_offsets, to_qv_bias, to_in_bias = layer_call(
            grid,
            tokens,
            cotangent,
            lengths,
            qkv_weight,
            out_weight.T,
            in_weight,
            down_weight.T,
            (norm_gains, offsets, qv_bias, in_bias),
        )
        return output, grad_tokens, to_qkv, to_qv_bias, to_out.T, to_in, to_in_bias, to_down.T, to_gains, to_offsets
    slot_count = row_count * pieces
    length = lengths[0]
    heads_here = qkv_weight.shape[2] // HEAD
    head_ids = (piece_index * heads_here + lax.iota(jnp.int32, heads_here)).astype(jnp.float32)
    slopes = jnp.exp2(-8.0 * (head_ids + 1.0) / (heads_here * pieces))
    key_valid = lax.iota(jnp.int32, slot_count) < length
    row_valid = (piece_index * row_count + lax.iota(jnp.int32, row_count) < length).astype(
        jnp.float32
    )[:, None]

    width_qv, width_in = qkv_weight.shape[2], in_weight.shape[2]
    parts = (qkv_weight, out_weight.T, in_weight, down_weight.T)
    small = pack_small(
        spread(qv_bias, dp_index, dp),
        spread(in_bias, dp_index, dp),
        jnp.concatenate([spread(norm_gains, flat_index, dp * pieces), spread(offsets, flat_index, dp * pieces)]),
        piece_index,
        pieces,
    )
    whole_qkv, whole_out_t, whole_in, whole_down_t = (
        lax.all_gather(p, "dp", axis=p.ndim - 2, tiled=True) for p in parts
    )
    small = lax.psum(small, ("dp", "tensor"))
    rows_all, whole_bqv, whole_bin = unpack_small(small, width_qv, width_in, piece_index, pieces)
    gains, shift_rows = rows_all[:2], rows_all[2:6]

    gathered = lax.all_gather(tokens, "tensor", axis=0, tiled=True)
    projected = jnp.einsum("sd,kdc->ksc", gathered, whole_qkv, preferred_element_type=jnp.float32)
    queries = (projected[0] + whole_bqv[0]).astype(jnp.bfloat16)
    key_rows = projected[1].astype(jnp.bfloat16)
    value_rows = (projected[2] + whole_bqv[1]).astype(jnp.bfloat16)
    mixed_heads, logsum = attend(queries, key_rows, value_rows, slopes, key_valid)
    attn_part = jnp.einsum("sc,dc->sd", mixed_heads, whole_out_t, preferred_element_type=jnp.float32)
    attn_total = lax.psum_scatter(
        attn_part.astype(jnp.bfloat16), "tensor", scatter_dimension=0, tiled=True
    ).astype(jnp.float32)
    first_in = tokens.astype(jnp.float32) + attn_total + shift_rows[0]
    attended, unit_one, scale_one = norm_forward(first_in, gains[0], shift_rows[1])
    attended_low = attended.astype(jnp.bfloat16)
    gathered_ff = lax.all_gather(attended_low, "tensor", axis=0, tiled=True)
    pre_acts = jnp.einsum("sd,kdc->ksc", gathered_ff, whole_in, preferred_element_type=jnp.float32)
    pre_acts = pre_acts + whole_bin[:, None, :]
    hidden = (jax.nn.gelu(pre_acts[0], approximate=False) * pre_acts[1]).astype(jnp.bfloat16)
    ff_part = jnp.einsum("sf,df->sd", hidden, whole_down_t, preferred_element_type=jnp.float32)
    ff_total = lax.psum_scatter(
        ff_part.astype(jnp.bfloat16), "tensor", scatter_dimension=0, tiled=True
    ).astype(jnp.float32)
    second_in = attended + ff_total + shift_rows[2]
    final_norm, unit_two, scale_two = norm_forward(second_in, gains[1], shift_rows[3])
    output = (final_norm * row_valid).astype(jnp.bfloat16)
    grad_final = cotangent.astype(jnp.float32) * row_valid
    grad_second, grad_gain_two, grad_shift_two = norm_backward(
        grad_final, unit_two, scale_two, gains[1]
    )
    grad_bdown = jnp.sum(grad_second, axis=0)
    grad_ff_rows = lax.all_gather(grad_second.astype(jnp.bfloat16), "tensor", axis=0, tiled=True)
    grad_down_t = jnp.einsum("sd,sf->df", grad_ff_rows, hidden, preferred_element_type=jnp.float32)
    grad_hidden = jnp.einsum("sd,df->sf", grad_ff_rows, whole_down_t, preferred_element_type=jnp.float32)
    pullback = jax.vjp(
        lambda gate_pre, up_pre: jax.nn.gelu(gate_pre, approximate=False) * up_pre,
        pre_acts[0],
        pre_acts[1],
    )[1]
    grad_gate, grad_up = pullback(grad_hidden)
    grad_pre = jnp.stack([grad_gate, grad_up]).astype(jnp.bfloat16)
    grad_bin = jnp.sum(grad_pre, axis=1, dtype=jnp.float32)
    grad_in = jnp.einsum("sd,ksc->kdc", gathered_ff, grad_pre, preferred_element_type=jnp.float32)
    ff_back = jnp.einsum("ksc,kdc->sd", grad_pre, whole_in, preferred_element_type=jnp.float32)
    grad_attended = grad_second + lax.psum_scatter(
        ff_back.astype(jnp.bfloat16), "tensor", scatter_dimension=0, tiled=True
    ).astype(jnp.float32)
    grad_first, grad_gain_one, grad_shift_one = norm_backward(
        grad_attended, unit_one, scale_one, gains[0]
    )
    grad_bout = jnp.sum(grad_first, axis=0)
    grad_attn_rows = lax.all_gather(grad_first.astype(jnp.bfloat16), "tensor", axis=0, tiled=True)
    grad_out_t = jnp.einsum("sd,sc->dc", grad_attn_rows, mixed_heads, preferred_element_type=jnp.float32)
    grad_mixed = jnp.einsum(
        "sd,dc->sc", grad_attn_rows, whole_out_t, preferred_element_type=jnp.float32
    ).astype(jnp.bfloat16)
    grad_queries, grad_keys, grad_values = attend_back(
        queries, key_rows, value_rows, grad_mixed, logsum, slopes, key_valid
    )
    grad_qkv = jnp.stack([grad_queries, grad_keys, grad_values]).astype(jnp.bfloat16)
    grad_wqkv = jnp.einsum("sd,ksc->kdc", gathered, grad_qkv, preferred_element_type=jnp.float32)
    grad_bqv = jnp.stack(
        [
            jnp.sum(grad_qkv[0], axis=0, dtype=jnp.float32),
            jnp.sum(grad_qkv[2], axis=0, dtype=jnp.float32),
        ]
    )
    input_back = jnp.einsum("ksc,kdc->sd", grad_qkv, whole_qkv, preferred_element_type=jnp.float32)
    grad_tokens = grad_first + lax.psum_scatter(
        input_back.astype(jnp.bfloat16), "tensor", scatter_dimension=0, tiled=True
    ).astype(jnp.float32)

    small_grads = pack_small(
        grad_bqv,
        grad_bin,
        jnp.stack([grad_gain_one, grad_gain_two, grad_bout, grad_shift_one, grad_bdown, grad_shift_two]),
        piece_index,
        pieces,
    )
    grads = tuple(g.astype(jnp.bfloat16) for g in (grad_wqkv, grad_out_t, grad_in, grad_down_t))
    shard_wqkv, shard_out_t, shard_in, shard_down_t = (
        lax.psum_scatter(g.astype(jnp.float32), "dp", scatter_dimension=g.ndim - 2, tiled=True) for g in grads
    )
    small_grads = lax.psum(small_grads, ("dp", "tensor"))
    row_grads, bqv_grads, bin_grads = unpack_small(small_grads, width_qv, width_in, piece_index, pieces)
    own_rows = pick(row_grads, flat_index, dp * pieces)
    return (
        output,
        grad_tokens,
        shard_wqkv,
        pick(bqv_grads, dp_index, dp),
        shard_out_t.T,
        shard_in,
        pick(bin_grads, dp_index, dp),
        shard_down_t.T,
        own_rows[:2],
        own_rows[2:],
    )


def solution(mesh):
    placed = (
        P(("dp", "tensor"), None),
        P("dp"),
        P(None, "dp", "tensor"),
        P(None, ("tensor", "dp")),
        P("tensor", "dp"),
        P(None, "dp", "tensor"),
        P(None, ("tensor", "dp")),
        P("tensor", "dp"),
        P(None, ("dp", "tensor")),
        P(None, ("dp", "tensor")),
        P(("dp", "tensor"), None),
    )

    def run(*args):
        dp = mesh.shape["dp"]
        direct = dp % 4 == 0 and (args[2].shape[1] // dp) % 16 == 0 and mesh.shape["tensor"] == 2
        return jax.shard_map(
            functools.partial(per_device, direct),
            mesh=mesh,
            in_specs=placed,
            out_specs=(
                P(("dp", "tensor"), None),
                P(("dp", "tensor"), None),
                P(None, "dp", "tensor"),
                P(None, ("tensor", "dp")),
                P("tensor", "dp"),
                P(None, "dp", "tensor"),
                P(None, ("tensor", "dp")),
                P("tensor", "dp"),
                P(None, ("dp", "tensor")),
                P(None, ("dp", "tensor")),
            ),
            check_vma=False,
        )(*args)

    return run
```

```python
import functools
import itertools

import jax
import jax.numpy as jnp
from jax import lax
from jax.experimental import pallas as pl
from jax.experimental.pallas import tpu as pltpu
from jax.sharding import PartitionSpec as P

HEAD = 64
MESH = pl.DeviceIdType.MESH
VMEM_LIMIT = 64 * 1024 * 1024 - 65536


class Grid3:
    def __init__(self, dp):
        self.nz = dp // 4
        self.slots = dp

    def here(self):
        me = lax.axis_index("dp")
        self.z, self.y, self.x = me // 4, (me // 2) % 2, me % 2
        z, nz = self.z, self.nz
        self.low, self.high = z > 0, z < nz - 1
        near = [sorted(range(1, nz), key=lambda k: (abs((p + k) % nz - p), k)) for p in range(nz)]
        self.by_distance = [(sum(jnp.where(z == p, near[p][j], 0) for p in range(nz)), 0, 0) for j in range(nz - 1)]
        self.line = []
        for d in self.by_distance:
            above = (z + d[0]) % nz > z
            self.line.append((above, jnp.where(above, z, nz - 1 - z) > 0))

    def at(self, dz, dy, dx):
        y = 1 - self.y if dy else self.y
        x = 1 - self.x if dx else self.x
        return (((self.z + dz) % self.nz) * 2 + y) * 2 + x

    def slot(self, d):
        return (d[0] % self.nz) * 4 + d[1] * 2 + d[2]

    def steps(self, axis):
        if axis == "z":
            return [(k, 0, 0) for k in range(1, self.nz)]
        return [(0, 1, 0)] if axis == "y" else [(0, 0, 1)]

    def seen_from(self, d, move):
        return ((d[0] - move[0] + self.nz) % self.nz, d[1] ^ move[1], d[2] ^ move[2])

    def span(self, axis):
        if axis == "z":
            return [(k, 0, 0) for k in range(self.nz)]
        return [(0, 0, 0), (0, 1, 0)] if axis == "y" else [(0, 0, 0), (0, 0, 1)]


def joined(*ds):
    return tuple(sum(part) for part in zip(*ds))


def remote(src, dst, send_sem, recv_sem, **device):
    return pltpu.make_async_remote_copy(
        src_ref=src, dst_ref=dst, send_sem=send_sem, recv_sem=recv_sem, device_id=device, device_id_type=MESH
    )


def greet(grid, partner):
    barrier = pltpu.get_barrier_semaphore()
    moves = [m for axis in "zyx" for m in grid.steps(axis)]
    for move in moves:
        pl.semaphore_signal(barrier, inc=1, device_id={"dp": grid.at(*move)}, device_id_type=MESH)
    pl.semaphore_signal(barrier, inc=1, device_id={"tensor": partner}, device_id_type=MESH)
    pl.semaphore_wait(barrier, len(moves) + 1)


class SmallSum:
    def __init__(self, grid, value, out, box, send, recv):
        self.grid = grid
        self.value, self.out, self.box, self.send, self.recv = value, out, box, send, recv
        self.copies = []

    def _post(self, slot, **device):
        copy = remote(self.out, self.box.at[slot], self.send.at[slot], self.recv.at[slot], **device)
        copy.start()
        self.copies.append(copy)

    def stage(self, number):
        grid = self.grid
        if number == 0:
            self.out[...] = self.value[...]
            self._post(0, tensor=1 - lax.axis_index("tensor"))
            return
        for copy in self.copies:
            copy.wait()
        self.copies = []
        if number == 1:
            self.out[...] = self.out[...] + self.box[0]
            for k in range(1, grid.nz):
                self._post(2 + k, dp=grid.at(k, 0, 0))
        elif number == 2:
            total = self.out[...]
            for k in range(1, grid.nz):
                total = total + self.box[2 + k]
            self.out[...] = total
            self._post(1, dp=grid.at(0, 0, 1))
        elif number == 3:
            self.out[...] = self.out[...] + self.box[1]
            self._post(2, dp=grid.at(0, 1, 0))
        else:
            self.out[...] = self.out[...] + self.box[2]


def small_slots(grid):
    return 2 + grid.nz


class Gather:
    def __init__(self, grid, chunks, send, recv):
        self.grid, self.chunks = grid, chunks
        self.send_sem, self.recv_sem = send, recv
        self.sent = []

    def _dst(self, number, d):
        rows = self.chunks[number][0].shape[0]
        return self.chunks[number][1].at[pl.ds(pl.multiple_of(self.grid.at(*d) * rows, rows), rows)]

    def _copy(self, number, d, move):
        dst = self._dst(number, d)
        if isinstance(move, int):
            move = (jnp.where(self.grid.line[move][0], -1, 1), 0, 0)
        source = self.chunks[number][0] if isinstance(d[0], int) and d == (0, 0, 0) else dst
        slot = self.grid.slot(self.grid.seen_from(d, move))
        return remote(source, dst, self.send_sem.at[number, slot], self.recv_sem.at[number, slot], dp=self.grid.at(*move))

    def _start(self, allowed, *args):
        if allowed is None:
            self._copy(*args).start()
        else:
            pl.when(allowed)(lambda: self._copy(*args).start())
        self.sent.append((allowed, args))

    def send(self, number, d, axis):
        if axis == "z":
            self._start(self.grid.low, number, d, (-1, 0, 0))
            self._start(self.grid.high, number, d, (1, 0, 0))
        else:
            self._start(None, number, d, self.grid.steps(axis)[0])

    def relay(self, number, d, j):
        self._start(self.grid.line[j][1], number, d, j)

    def arrive(self, number, d):
        dst, slot = self._dst(number, d), self.grid.slot(d)
        remote(dst, dst, self.send_sem.at[number, slot], self.recv_sem.at[number, slot], dp=self.grid.at(*d)).wait_recv()

    def moved(self, axis):
        return self.grid.by_distance if axis == "z" else self.grid.steps(axis)

    def first(self, number):
        return [(self.pass_first, number, d, j) for j, d in enumerate(self.moved(self.chunks[number][2][0]))]

    def second(self, number):
        one, two = self.chunks[number][2][:2]
        return [
            (self.pass_second, number, joined(a, b), j) for j, b in enumerate(self.moved(two)) for a in self.grid.span(one)
        ]

    def third(self, number):
        one, two, three = self.chunks[number][2]
        return [joined(a, b, c) for a in self.grid.span(one) for b in self.grid.span(two) for c in self.grid.steps(three)]

    def pass_first(self, number, d, j):
        order = self.chunks[number][2]
        self.arrive(number, d)
        if order[0] == "z":
            self.relay(number, d, j)
        for axis in order[1:]:
            self.send(number, d, axis)

    def pass_second(self, number, d, j):
        order = self.chunks[number][2]
        self.arrive(number, d)
        if order[1] == "z":
            self.relay(number, d, j)
        self.send(number, d, order[2])

    def finish(self, number):
        for d in self.third(number):
            self.arrive(number, d)

    def drain(self):
        for allowed, args in self.sent:
            if allowed is None:
                self._copy(*args).wait_send()
            else:
                pl.when(allowed)(lambda args=args: self._copy(*args).wait_send())
        self.sent = []


class Scatter:
    def __init__(self, grid, rows, chunks, send, recv):
        self.grid, self.rows, self.chunks = grid, rows, chunks
        self.send_sem, self.recv_sem = send, recv
        self.sent = []
        self.far_first = [2, 1, 3] if grid.nz == 4 else list(range(1, grid.nz))
        self.second, self.line, self.crossing = 2 * grid.nz, 3 * grid.nz - 1, 4 * grid.nz - 2

    def part(self, number, d):
        return self.chunks[number][0].at[pl.ds(pl.multiple_of(self.grid.at(*d) * self.rows, self.rows), self.rows)]

    def box(self, number, slot):
        return self.chunks[number][3].at[slot]

    def other(self, number):
        return "y" if self.chunks[number][2][0] == "x" else "x"

    def place(self, number, dz, e):
        return (dz, e, 0) if self.other(number) == "y" else (dz, 0, e)

    def _copy(self, number, kind, dz, e=0):
        grid = self.grid
        if kind == "own":
            move = grid.steps(self.chunks[number][2][0])[0]
            source, slot = self.part(number, joined(self.place(number, dz, e), move)), dz * 2 + e
        elif kind == "side":
            move = grid.steps(self.other(number))[0]
            source, slot = self.box(number, dz * 2 + 1), self.second + dz
        elif kind == "cross":
            move = grid.steps(self.other(number))[0]
            source, slot = self.box(number, 1), self.crossing
        elif kind == "middle":
            move = (dz, 0, 0)
            source, slot = self.box(number, dz * 2 + e), self.middle_slot(dz, e)
        else:
            move = (dz, 0, 0)
            source, slot = self.box(number, dz * 2), self.line + dz
        return remote(
            source, self.box(number, slot), self.send_sem.at[number, slot], self.recv_sem.at[number, slot], dp=grid.at(*move)
        )

    def _send(self, *args):
        self._copy(*args).start()
        self.sent.append(args)

    def _arrive(self, number, slot):
        box = self.box(number, slot)
        remote(box, box, self.send_sem.at[number, slot], self.recv_sem.at[number, slot], dp=0).wait_recv()

    def begin(self, number, *halves):
        for e in halves or (1, 0):
            for dz in self.far_first + [0]:
                self._send(number, "own", dz, e)

    def held(self, number, dz, e):
        slot = dz * 2 + e
        self._arrive(number, slot)
        return self.part(number, self.place(number, dz, e))[...].astype(jnp.float32) + self.box(number, slot)[...].astype(jnp.float32)

    def side(self, number, dz):
        self.box(number, dz * 2 + 1)[...] = self.held(number, dz, 1).astype(jnp.bfloat16)
        self._send(number, "side", dz)

    def both(self, number, dz):
        value = self.held(number, dz, 0)
        self._arrive(number, self.second + dz)
        return value + self.box(number, self.second + dz)[...].astype(jnp.float32)

    def along(self, number, dz):
        self.box(number, dz * 2)[...] = self.both(number, dz).astype(jnp.bfloat16)
        self._send(number, "line", dz)

    def middle_slot(self, dz, e):
        return self.second + e * (self.grid.nz - 1) + dz - 1

    def middle(self, number, dz, e):
        self.box(number, dz * 2 + e)[...] = self.held(number, dz, e).astype(jnp.bfloat16)
        self._send(number, "middle", dz, e)

    def line_total(self, number, e):
        total = self.held(number, 0, e)
        for dz in self.far_first:
            slot = self.middle_slot(dz, e)
            self._arrive(number, slot)
            total = total + self.box(number, slot)[...].astype(jnp.float32)
        return total

    def cross(self, number):
        self.box(number, 1)[...] = self.line_total(number, 1).astype(jnp.bfloat16)
        self._send(number, "cross", 0)

    def z_second(self, number):
        return self.chunks[number][2][1] == "z"

    def sides(self, *numbers):
        if self.z_second(numbers[0]):
            return [(self.middle, n, dz, e) for e in (1, 0) for dz in self.far_first for n in numbers]
        return [(self.side, n, dz) for dz in self.far_first + [0] for n in numbers]

    def lines(self, *numbers):
        if self.z_second(numbers[0]):
            return [(self.cross, n) for n in numbers]
        return [(self.along, n, dz) for dz in self.far_first for n in numbers]

    def lasts(self, *numbers):
        return [(self.last, n) for n in numbers]

    def last(self, number):
        if self.z_second(number):
            total = self.line_total(number, 0)
            self._arrive(number, self.crossing)
            total = total + self.box(number, self.crossing)[...].astype(jnp.float32)
        else:
            total = self.both(number, 0)
            for dz in self.far_first:
                self._arrive(number, self.line + dz)
                total = total + self.box(number, self.line + dz)[...].astype(jnp.float32)
        self.chunks[number][1](total)

    def drain(self):
        for args in self.sent:
            self._copy(*args).wait_send()
        self.sent = []


def scatter_slots(grid):
    return 4 * grid.nz - 1
bf16, f32 = jnp.bfloat16, jnp.float32
NORM_EPSILON = 1e-06
EARLY = 12
AFTER_PROJECTION = 4
GATHER_STEPS = 4
AFTER_OUT = 4
AFTER_NORM = 4
ROOT_HALF = 0.7071067811865476
PHI_SCALE = 0.3989422804014327


def nn(a, b):
    return jnp.dot(a, b, preferred_element_type=f32)


def nt(a, b):
    return lax.dot_general(a, b, (((1,), (1,)), ((), ())), preferred_element_type=f32)


def aligned(start, size):
    return pl.ds(pl.multiple_of(start, size), size)


def unit_rows(values):
    centred = values - jnp.mean(values, axis=-1, keepdims=True)
    variance = jnp.mean(centred * centred, axis=-1, keepdims=True)
    scale = lax.rsqrt(variance + NORM_EPSILON)
    return centred * scale, scale


def unit_back(grad_unit, unit, scale):
    inner = (
        grad_unit
        - jnp.mean(grad_unit, axis=-1, keepdims=True)
        - unit * jnp.mean(grad_unit * unit, axis=-1, keepdims=True)
    )
    return inner * scale


def fold(rows):
    return jnp.sum(rows.reshape(rows.shape[0] // 8, 8, rows.shape[1]), axis=0)


def merged(*lists):
    return [entry for row in itertools.zip_longest(*lists) for entry in row if entry is not None]


class Pump:
    def __init__(self, steps=()):
        self.steps = list(steps)

    def take(self, count=None):
        count = len(self.steps) if count is None else min(count, len(self.steps))
        taken, self.steps = self.steps[:count], self.steps[count:]
        return taken

    def run(self, count=None):
        for function, *args in self.take(count):
            function(*args)


def at_trips(*shares):
    def run(index):
        for trip, share in enumerate(shares):

            @pl.when(index == trip)
            def _(share=share):
                Pump(share).run()

    return run


def layer_body(
    grid, rows,
    tokens, cotangent, length, qkv_part, out_part, in_part, down_part, gains_part, offsets_part, qv_bias, in_bias,
    output, grad_tokens, to_qkv, to_out, to_in, to_down, to_gains, to_offsets, to_qv_bias, to_in_bias, probs_far,
    w_qv, w_ko, w_gate, w_up, w_low, w_high, small_mine, small_pair, small_tiles, every_small, small_box, small_grads,
    x, qkv, inverse, mixed, work, key_aug, value_aug, query_aug,
    rows_f32, attended_low, branch_rows, outgoing, incoming, turned,
    grad_t, pair_b, grad_value_t, grad_key_t,
    g_qv, g_ko, g_gate, g_up, g_low, g_high, box_qv, box_ko, box_gate, box_up, box_low, box_high,
    gather_send, gather_recv, scatter_send, scatter_recv, small_send, small_recv, own_sem, swap_send, swap_recv, local_sem, prob_sem,
):
    grid.here()
    side = lax.axis_index("tensor")
    other = 1 - side
    half = tokens.shape[0]
    slots = 2 * half
    width = tokens.shape[1]
    heads_wide = mixed.shape[1]
    units = w_gate.shape[1]
    mine = aligned(side * half, half)
    count = length[0]
    attended, unit_one = rows_f32.at[:, pl.ds(0, width)], rows_f32.at[:, pl.ds(width, width)]
    scale_one = rows_f32.at[:, pl.ds(2 * width, 128)]
    block = 256
    span = 2 * slots - block
    bias = rows_f32.at[pl.ds(0, block), pl.ds(0, span)]

    own_rows = aligned(grid.at(0, 0, 0) * rows, rows)
    low, high = pl.ds(0, units // 2), pl.ds(units // 2, units // 2)
    one_head, two_head = pl.ds(0, heads_wide), pl.ds(heads_wide, heads_wide)
    own_copies = [
        pltpu.make_async_copy(source, target, own_sem.at[n])
        for n, (source, target) in enumerate(
            [
                (qkv_part.at[0], w_qv.at[own_rows, one_head]),
                (qkv_part.at[2], w_qv.at[own_rows, two_head]),
                (qkv_part.at[1], w_ko.at[own_rows, one_head]),
                (out_part, w_ko.at[own_rows, two_head]),
                (in_part.at[0], w_gate.at[own_rows]),
                (in_part.at[1], w_up.at[own_rows]),
                (down_part.at[:, low], w_low.at[own_rows]),
                (down_part.at[:, high], w_high.at[own_rows]),
            ]
        )
    ]
    for copy in own_copies:
        copy.start()
    greet(grid, other)

    gather = Gather(grid, [
        (w_qv.at[own_rows], w_qv, "zyx"),
        (w_ko.at[own_rows], w_ko, "zxy"),
        (w_gate.at[own_rows], w_gate, "yzx"),
        (w_up.at[own_rows], w_up, "xzy"),
        (w_low.at[own_rows], w_low, "zyx"),
        (w_high.at[own_rows], w_high, "zxy"),
        (small_pair, small_tiles, "zyx"),
    ], gather_send, gather_recv)
    def sink_qv(total):
        to_qkv[0], to_qkv[2] = total[:, :heads_wide], total[:, heads_wide:]

    def sink_ko(total):
        to_qkv[1] = total[:, :heads_wide]
        to_out[...] = total[:, heads_wide:]

    def sink_gate(total):
        to_in[0] = total

    def sink_up(total):
        to_in[1] = total

    def sink_low(total):
        to_down[:, : units // 2] = total

    def sink_high(total):
        to_down[:, units // 2 :] = total

    scatter = Scatter(grid, rows, [
        (g_qv, sink_qv, "xyz", box_qv),
        (g_ko, sink_ko, "yxz", box_ko),
        (g_gate, sink_gate, "xyz", box_gate),
        (g_up, sink_up, "yxz", box_up),
        (g_low, sink_low, "xzy", box_low),
        (g_high, sink_high, "yzx", box_high),
    ], scatter_send, scatter_recv)
    QV, KO, GATE, UP, LOW, HIGH, SMALL = range(7)

    def swap(source, target, slot):
        copy = remote(source, target, swap_send.at[slot], swap_recv.at[slot], tensor=other)
        copy.start()
        return copy

    token_swap = swap(tokens, x.at[mine], 0)
    token_copy = pltpu.make_async_copy(tokens, x.at[mine], local_sem.at[0])
    token_copy.start()
    cot_copy = pltpu.make_async_copy(cotangent, output, local_sem.at[1])
    cot_copy.start()
    my_lanes = pl.ds(pl.multiple_of(side * 128, 128), 128)
    small_mine[...] = jnp.zeros_like(small_mine)
    small_mine[0:2, 0 : gains_part.shape[1]] = gains_part[...]
    small_mine[2:6, 0 : offsets_part.shape[1]] = offsets_part[...]
    small_mine[8:10, 0 : in_bias.shape[1]] = in_bias[...].astype(f32)
    small_mine[10:12, 0 : qv_bias.shape[1]] = qv_bias[...].astype(f32)
    small_pair[:, my_lanes] = small_mine[...]
    small_swap = swap(small_mine, small_pair.at[:, my_lanes], 8)
    pieces = {QV: (0, 1), KO: (2, 3), GATE: (4,), UP: (5,), LOW: (6,), HIGH: (7,)}
    for n in pieces:
        for piece in pieces[n]:
            own_copies[piece].wait()
        for axis in gather.chunks[n][2]:
            gather.send(n, (0, 0, 0), axis)
        if n == KO:
            small_swap.wait()
            for axis in gather.chunks[SMALL][2]:
                gather.send(SMALL, (0, 0, 0), axis)
            small_tiles[aligned(grid.at(0, 0, 0) * 16, 16), :] = small_pair[...]
    near_units = merged(gather.second(GATE), gather.second(UP))
    ends_first = merged(gather.first(LOW), gather.first(HIGH))
    ends_second = merged(gather.second(LOW), gather.second(HIGH))
    early = (
        merged(gather.first(QV), gather.first(SMALL), gather.first(KO))
        + merged(gather.first(GATE), gather.first(UP))
        + merged(merged(gather.second(QV), gather.second(SMALL), gather.second(KO)), near_units[:EARLY])
    )
    pump = Pump(early)
    pump.run()
    pump = Pump(merged(near_units[EARLY:], ends_first) + ends_second)
    token_copy.wait()
    token_swap.wait()
    for number in (SMALL, QV, KO):
        gather.finish(number)

    norm_rows = jnp.zeros((8, width), f32)
    head_rows = jnp.zeros((8, heads_wide), f32)
    unit_rows_in = jnp.zeros((8, units), f32)

    def at_lanes(tile, lanes, start):
        wide = jnp.concatenate([tile, jnp.zeros((8, lanes - 128), f32)], axis=1)
        return pltpu.roll(wide, start, 1) if start else wide

    for i in range(grid.slots):
        pair_tile = [small_tiles[16 * i : 16 * i + 8, 128 * s : 128 * s + 128] for s in range(2)]
        unit_tile = [small_tiles[16 * i + 8 : 16 * i + 16, 128 * s : 128 * s + 128] for s in range(2)]
        for s in range(2):
            norm_rows = norm_rows + at_lanes(pair_tile[s], width, (2 * i + s) * (rows // 2))
        units_here = jnp.where(side == 0, unit_tile[0], unit_tile[1])
        unit_rows_in = unit_rows_in + at_lanes(units_here, units, i * (units // grid.slots))
        head_rows = head_rows + at_lanes(pltpu.roll(units_here, 6, 0), heads_wide, i * (heads_wide // grid.slots))
    every_small[0:8, :] = norm_rows
    every_small[8:9, pl.ds(0, heads_wide)] = head_rows[0:1, :]
    every_small[8:9, pl.ds(heads_wide, heads_wide)] = head_rows[1:2, :]
    turned[0:8, :] = unit_rows_in

    q_cols, v_cols, k_cols = (pl.ds(i * heads_wide, heads_wide) for i in range(3))
    side_cols = pl.ds(pl.multiple_of(side * heads_wide, 128), heads_wide)
    row_bias = every_small[8:9, :]
    row_scale = jnp.where(lax.broadcasted_iota(jnp.int32, (1, 2 * heads_wide), 1) < heads_wide, 0.125, 1.0)

    @pl.loop(0, slots // 256)
    def _(i):
        r = aligned(i * 256, 256)
        raw = (nn(x[r, :], w_qv[...]) + row_bias).astype(bf16)
        qkv[r, pl.ds(0, 2 * heads_wide)] = (raw.astype(f32) * row_scale).astype(bf16)
        qkv[r, k_cols] = nn(x[r, :], w_ko[:, pl.ds(0, heads_wide)]).astype(bf16)

    pump.run(AFTER_PROJECTION)

    lane = lax.broadcasted_iota(jnp.int32, (slots, 128), 1)
    slot = lax.broadcasted_iota(jnp.int32, (slots, 128), 0)
    key_mask = jnp.where(slot < count, 0.0, -1e30).astype(bf16)
    zero, one = jnp.zeros((), bf16), jnp.ones((), bf16)
    block_lane = lax.broadcasted_iota(jnp.int32, (block, 128), 1)
    pairs = heads_wide // 128
    slopes = [2.0 ** (-8.0 * (h + 1) / (4 * pairs)) for h in range(4 * pairs)]

    def prob_slot(upper):
        return work.at[:, pl.ds(upper * slots, slots)]

    def prob_out(pair, upper):
        return pltpu.make_async_copy(prob_slot(upper), probs_far.at[2 * pair + upper], prob_sem.at[upper])

    def prob_in(pair, upper):
        return pltpu.make_async_copy(probs_far.at[2 * pair + upper], prob_slot(upper), prob_sem.at[upper])

    def pair_cols(pair, start=0):
        return pl.ds(pl.multiple_of(start + pair * 128, 128), 128)

    def attend_pair(pair):
        cols = pair_cols(pair)
        for upper in (0, 1):
            own = (lane >= 64) == (upper == 1)
            spare = 0 if upper else 64
            gap = jnp.abs(
                lax.broadcasted_iota(jnp.int32, (block, span), 0)
                - (lax.broadcasted_iota(jnp.int32, (block, span), 1) - (span - slots))
            )
            slope = sum(
                jnp.where(pair == p, jnp.where(side == 0, slopes[2 * p + upper], slopes[2 * (pairs + p) + upper]), 0.0)
                for p in range(pairs)
            )
            bias[...] = gap.astype(f32) * slope
            key_aug[...] = jnp.where(own, qkv[:, pair_cols(pair, 2 * heads_wide)], jnp.where(lane == spare, key_mask, zero))
            value_aug[...] = jnp.where(own, qkv[:, pair_cols(pair, heads_wide)], one)
            query_aug[...] = jnp.where(own, qkv[:, cols], jnp.where(lane == spare, one, zero))

            @pl.when(pair > 0)
            def _(upper=upper):
                prob_out(pair - 1, upper).wait()

            def attend(i, inner_carry, upper=upper):
                r = aligned(i * block, block)
                scores = nt(query_aug[r, :], key_aug[...]) - bias[:, pl.ds(pl.multiple_of(span - slots - i * block, block), slots)]
                top = jnp.max(scores, axis=1, keepdims=True)
                weights = jnp.exp(scores - top).astype(bf16)
                work[r, pl.ds(upper * slots, slots)] = weights
                product = nn(weights, value_aug[...])
                scale = 1.0 / (product[:, 0:1] if upper else product[:, 64:65])
                result = (product * scale).astype(bf16)
                inverse[r, :] = jnp.where(block_lane == 2 * pair + upper, scale, inverse[r, :])
                mixed[r, cols] = jnp.where(block_lane < 64, mixed[r, cols], result) if upper else result
                return inner_carry

            lax.fori_loop(0, slots // block, attend, 0, unroll=2)
            prob_out(pair, upper).start()
        between_pairs(pair)

    inverse[...] = jnp.zeros_like(inverse)
    between_pairs = at_trips(*(pump.take(GATHER_STEPS) for _ in range(pairs)))
    pl.loop(0, pairs)(attend_pair)

    def project(source, weights, target_rows, sink):
        @pl.loop(0, half // 256)
        def _(i):
            r = aligned(target_rows * half + i * 256, 256)
            sink(i, nt(source[r, :], weights[...]))

    def to_outgoing(i, value):
        outgoing[aligned(i * 256, 256), :] = value.astype(bf16)

    def to_attended(i, value):
        attended[aligned(i * 256, 256), :] = value

    w_out = w_ko.at[:, pl.ds(heads_wide, heads_wide)]
    project(mixed, w_out, other, to_outgoing)
    first_swap = swap(outgoing, incoming.at[0], 1)
    pump.run(AFTER_OUT)
    project(mixed, w_out, side, to_attended)
    first_swap.wait()
    gain_one, gain_two = every_small[0:1, :], every_small[1:2, :]
    step = 64

    @pl.loop(0, half // step)
    def _(i):
        r = aligned(i * step, step)
        own = pl.ds(pl.multiple_of(side * half + i * step, step), step)
        total = x[own, :].astype(f32) + attended[r, :] + incoming[0, r, :].astype(f32) + every_small[2:3, :]
        unit, scale = unit_rows(total)
        result = unit * gain_one + every_small[3:4, :]
        unit_one[r, :] = unit
        scale_one[r, :] = jnp.broadcast_to(scale, (step, 128))
        attended[r, :] = result
        attended_low[own, :] = result.astype(bf16)

    low_swap = swap(attended_low.at[mine], attended_low.at[mine], 2)
    for upper in (0, 1):
        prob_out(pairs - 1, upper).wait()
    pump.run(AFTER_NORM)
    gather.finish(GATE)
    gather.finish(UP)

    def feed(rows_side):
        r = aligned(rows_side * half, half)

        @pl.loop(0, units // 256)
        def _(j):
            c = aligned(j * 256, 256)
            c_up = pl.ds(pl.multiple_of(units + j * 256, 256), 256)
            c_hidden = pl.ds(pl.multiple_of(2 * units + j * 256, 256), 256)
            gate = nn(attended_low[r, :], w_gate[:, c]) + turned[0:1, c]
            up = nn(attended_low[r, :], w_up[:, c]) + turned[1:2, c]
            below = 0.5 * (1.0 + lax.erf(gate * ROOT_HALF))
            density = PHI_SCALE * jnp.exp(-0.5 * gate * gate)
            bent = gate * below
            work[r, c_hidden] = (bent * up).astype(bf16)
            work[r, c] = (up * (below + gate * density)).astype(bf16)
            work[r, c_up] = bent.astype(bf16)

    feed(side)
    pump.run()
    low_swap.wait()
    feed(other)
    pump.run()
    gather.finish(LOW)
    gather.finish(HIGH)

    hidden_low, hidden_high = pl.ds(2 * units, units // 2), pl.ds(2 * units + units // 2, units // 2)

    def down(rows_side, sink):
        @pl.loop(0, half // 256)
        def _(i):
            r = aligned(rows_side * half + i * 256, 256)
            sink(i, nt(work[r, hidden_low], w_low[...]) + nt(work[r, hidden_high], w_high[...]))

    def add_attended(i, value):
        r = aligned(i * 256, 256)
        attended[r, :] = attended[r, :] + value

    down(other, to_outgoing)
    second_swap = swap(outgoing, incoming.at[1], 3)
    down(side, add_attended)
    cot_copy.wait()
    second_swap.wait()
    nothing = jnp.zeros((8, width), f32)

    def second_norm(i, carry):
        sum_gain, sum_shift, sum_branch = carry
        r = aligned(i * step, step)
        own = pl.ds(pl.multiple_of(side * half + i * step, step), step)
        position = side * half + i * step + lax.broadcasted_iota(jnp.int32, (step, 1), 0)
        valid = jnp.where(position < count, 1.0, 0.0)
        unit, scale = unit_rows(attended[r, :] + incoming[1, r, :].astype(f32) + every_small[4:5, :])
        grad = output[r, :].astype(f32) * valid
        output[r, :] = ((unit * gain_two + every_small[5:6, :]) * valid).astype(bf16)
        back = unit_back(grad * gain_two, unit, scale)
        attended[r, :] = back
        branch_rows[own, :] = back.astype(bf16)
        return sum_gain + fold(grad * unit), sum_shift + fold(grad), sum_branch + fold(back)

    gain_two_sum, shift_two_sum, down_bias_sum = lax.fori_loop(0, half // step, second_norm, (nothing,) * 3)
    branch_swap = swap(branch_rows.at[mine], branch_rows.at[mine], 4)
    small_grads[...] = jnp.zeros_like(small_grads)
    small_grads[1:2, :] = jnp.sum(gain_two_sum, axis=0, keepdims=True)
    small_grads[5:6, :] = jnp.sum(shift_two_sum, axis=0, keepdims=True)
    small_grads[4:5, :] = jnp.sum(down_bias_sum, axis=0, keepdims=True)
    branch_swap.wait()

    def turn(source):
        @pl.loop(0, slots // 256)
        def _(i):
            r = aligned(i * 256, 256)
            grad_t[:, r] = source[r, :].T

    def weight_grad(sink, source, source_start, tile):
        @pl.loop(0, sink.shape[1] // tile)
        def _(j):
            sink[:, aligned(j * tile, tile)] = nn(
                grad_t[...], source[:, pl.ds(pl.multiple_of(source_start + j * tile, tile), tile)]
            ).astype(bf16)

    turn(branch_rows)
    weight_grad(g_low, work, 2 * units, 256)
    scatter.begin(LOW)
    weight_grad(g_high, work, 2 * units + units // 2, 256)
    scatter.begin(HIGH)

    turned[8:24, :] = jnp.zeros((16, units), f32)
    for index, weights in enumerate((w_low, w_high)):
        @pl.loop(0, units // 2 // 256)
        def _(j, index=index, weights=weights):
            c = pl.ds(pl.multiple_of(index * (units // 2) + j * 256, 256), 256)
            c_up = pl.ds(pl.multiple_of(units + index * (units // 2) + j * 256, 256), 256)
            for part in range(2):
                r = pl.ds(part * half, half)
                grad = nn(branch_rows[r, :], weights[:, aligned(j * 256, 256)])
                gate_grad = (grad * work[r, c].astype(f32)).astype(bf16)
                up_grad = (grad * work[r, c_up].astype(f32)).astype(bf16)
                work[r, c] = gate_grad
                work[r, c_up] = up_grad
                turned[8:16, c] = turned[8:16, c] + fold(gate_grad.astype(f32))
                turned[16:24, c] = turned[16:24, c] + fold(up_grad.astype(f32))

    for index in range(2):
        total = jnp.sum(turned[8 + 8 * index : 16 + 8 * index, :], axis=0, keepdims=True)
        for j in range(units // width):
            small_grads[pl.ds(8 + 4 * index + 2 * side + j, 1), :] = total[:, j * width : (j + 1) * width]

    sides_ends = Pump(scatter.sides(LOW, HIGH))
    sides_ends.run(6)
    turn(attended_low)
    weight_grad(g_gate, work, 0, 512)
    scatter.begin(GATE, 1)
    weight_grad(g_up, work, units, 512)
    scatter.begin(UP, 1)
    scatter.begin(GATE, 0)
    sides_ends.run()

    gate_cols, up_cols = pl.ds(0, units), pl.ds(units, units)

    def units_back(rows_side, sink):
        @pl.loop(0, half // 256)
        def _(i):
            r = aligned(rows_side * half + i * 256, 256)
            sink(i, nt(work[r, gate_cols], w_gate[...]) + nt(work[r, up_cols], w_up[...]))

    units_back(other, to_outgoing)
    third_swap = swap(outgoing, incoming.at[0], 5)
    units_back(side, add_attended)
    Pump(scatter.lines(LOW, HIGH)).run()
    third_swap.wait()

    def first_norm_back(i, carry):
        sum_gain, sum_shift, sum_branch = carry
        r = aligned(i * step, step)
        own = pl.ds(pl.multiple_of(side * half + i * step, step), step)
        grad = attended[r, :] + incoming[0, r, :].astype(f32)
        unit = unit_one[r, :]
        back = unit_back(grad * gain_one, unit, scale_one[r, 0:1])
        attended[r, :] = back
        branch_rows[own, :] = back.astype(bf16)
        return sum_gain + fold(grad * unit), sum_shift + fold(grad), sum_branch + fold(back)

    prob_in(0, 0).start()
    prob_in(0, 1).start()
    gain_one_sum, shift_one_sum, out_bias_sum = lax.fori_loop(0, half // step, first_norm_back, (nothing,) * 3)
    attn_swap = swap(branch_rows.at[mine], branch_rows.at[mine], 6)
    small_grads[0:1, :] = jnp.sum(gain_one_sum, axis=0, keepdims=True)
    small_grads[3:4, :] = jnp.sum(shift_one_sum, axis=0, keepdims=True)
    small_grads[2:3, :] = jnp.sum(out_bias_sum, axis=0, keepdims=True)
    attn_swap.wait()

    grad_mixed = attended_low.at[:, pl.ds(0, heads_wide)]
    turn(branch_rows)
    g_ko[:, pl.ds(heads_wide, heads_wide)] = nn(grad_t[...], mixed[...]).astype(bf16)
    sides_gate = Pump(scatter.sides(GATE))
    sides_gate.run(2)

    @pl.loop(0, slots // 256)
    def _(i):
        r = aligned(i * 256, 256)
        grad_mixed[r, :] = nn(branch_rows[r, :], w_out[...]).astype(bf16)

    sides_gate.run()
    scatter.begin(UP, 0)

    mixed_t, query_t = pair_b.at[0], pair_b.at[1]

    def pair_back(pair):
        cols, key_cols, value_cols = pair_cols(pair), pair_cols(pair, 2 * heads_wide), pair_cols(pair, heads_wide)
        scales = inverse[...]
        shrink = jnp.where(
            lane < 64,
            jnp.sum(jnp.where(lane == 2 * pair, scales, 0.0), axis=1, keepdims=True),
            jnp.sum(jnp.where(lane == 2 * pair + 1, scales, 0.0), axis=1, keepdims=True),
        )
        scaled = (grad_mixed[:, cols].astype(f32) * shrink).astype(bf16)
        mixed_t[...] = scaled.T
        query_t[...] = qkv[:, cols].T
        outgoing_pair[...] = scaled
        for upper in (0, 1):
            own = (lane >= 64) == (upper == 1)
            spare = 0 if upper else 64
            scaled = outgoing_pair[...]
            dots = jnp.sum(jnp.where(own, scaled.astype(f32) * mixed[:, cols].astype(f32), 0.0), axis=1, keepdims=True)
            dots_high = dots.astype(bf16)
            dots_low = (dots - dots_high.astype(f32)).astype(bf16)
            ones = (lane == spare) | (lane == spare + 1)
            value_aug[...] = jnp.where(own, qkv[:, value_cols], jnp.where(ones, one, zero))
            query_aug[...] = jnp.where(
                own, scaled, jnp.where(lane == spare, -dots_high, jnp.where(lane == spare + 1, -dots_low, zero))
            )
            part = pl.ds(64 * upper, 64)
            base = upper * slots
            prob_in(pair, upper).wait()
            for j in range(slots // 512):
                c = pl.ds(j * 512, 512)
                grad_value_t[part, c] = nn(mixed_t[part, :], work[:, pl.ds(base + j * 512, 512)]).astype(bf16)

            def attend_back(i, inner_carry, upper=upper, base=base):
                r = aligned(i * block, block)
                inner = nt(query_aug[r, :], value_aug[...])
                grads = (work[r, pl.ds(base, slots)].astype(f32) * inner).astype(bf16)
                work[r, pl.ds(base, slots)] = grads
                result = (nn(grads, qkv[:, key_cols]) * 0.125).astype(bf16)
                qkv[r, cols] = jnp.where(block_lane < 64, qkv[r, cols], result) if upper else result
                return inner_carry

            lax.fori_loop(0, slots // block, attend_back, 0, unroll=2)
            for j in range(slots // 512):
                c = pl.ds(j * 512, 512)
                grad_key_t[part, c] = nn(query_t[part, :], work[:, pl.ds(base + j * 512, 512)]).astype(bf16)

            @pl.when(pair + 1 < pairs)
            def _(upper=upper):
                prob_in(pair + 1, upper).start()

        qkv[:, value_cols] = grad_value_t[...].T
        qkv[:, key_cols] = grad_key_t[...].T
        between_pairs(pair)

    outgoing_pair = key_aug
    between_pairs = at_trips(scatter.sides(UP), scatter.lasts(LOW, HIGH), scatter.lines(GATE))
    pl.loop(0, pairs)(pair_back)

    turn(x)
    g_qv[...] = nn(grad_t[...], qkv[:, pl.ds(0, 2 * heads_wide)]).astype(bf16)
    scatter.begin(QV, 1)
    g_ko[:, pl.ds(0, heads_wide)] = nn(grad_t[...], qkv[:, k_cols]).astype(bf16)
    scatter.begin(KO, 1)
    scatter.begin(QV, 0)
    scatter.begin(KO, 0)
    def column_sum(cols):
        def add(i, carry):
            return carry + fold(qkv[aligned(i * 128, 128), cols].astype(f32))

        return jnp.sum(lax.fori_loop(0, slots // 128, add, jnp.zeros((8, heads_wide), f32)), axis=0, keepdims=True)

    small_grads[6:7, side_cols] = column_sum(q_cols)
    small_grads[7:8, side_cols] = column_sum(v_cols)
    sums = SmallSum(grid, small_grads, small_grads, small_box, small_send, small_recv)
    sums.stage(0)

    def inputs_back(rows_side, sink):
        @pl.loop(0, half // 256)
        def _(i):
            r = aligned(rows_side * half + i * 256, 256)
            sink(
                i,
                nt(qkv[r, pl.ds(0, 2 * heads_wide)], w_qv[...]) + nt(qkv[r, k_cols], w_ko[:, pl.ds(0, heads_wide)]),
            )

    inputs_back(other, to_outgoing)
    fourth_swap = swap(outgoing, incoming.at[1], 7)
    sums.stage(1)
    inputs_back(side, add_attended)
    sums.stage(2)
    Pump(scatter.lines(UP)).run()
    fourth_swap.wait()

    @pl.loop(0, half // step)
    def _(i):
        r = aligned(i * step, step)
        attended[r, :] = attended[r, :] + incoming[1, r, :].astype(f32)

    tokens_copy = pltpu.make_async_copy(attended, grad_tokens, local_sem.at[3])
    tokens_copy.start()
    Pump(scatter.sides(QV, KO)).run()
    sums.stage(3)
    Pump(scatter.lines(QV, KO) + scatter.lasts(GATE, UP) + scatter.lasts(QV, KO)).run()
    sums.stage(4)

    def turn_to(rows_block, start):
        return pltpu.roll(rows_block, (width - start) % width, 1)

    dp = lax.axis_index("dp")
    piece = to_gains.shape[1]
    low_rows, high_rows = small_grads[0:8, :], small_grads[8:16, :]
    norm_part = turn_to(low_rows, (2 * dp + side) * piece)
    to_gains[...] = norm_part[0:2, :piece]
    to_offsets[...] = norm_part[2:6, :piece]
    to_qv_bias[...] = turn_to(low_rows, side * heads_wide + dp * to_qv_bias.shape[1])[6:8, : to_qv_bias.shape[1]]
    unit_piece = to_in_bias.shape[1]
    first_lane = dp * unit_piece
    unit_part = turn_to(high_rows, first_lane % width)
    per_half = units // width
    row = side * per_half + first_lane // width
    for index in range(2):
        chosen = sum(
            jnp.where(row == r, unit_part[2 * per_half * index + r : 2 * per_half * index + r + 1, :], 0.0)
            for r in range(2 * per_half)
        )
        to_in_bias[index : index + 1, :] = chosen[:, :unit_piece]
    tokens_copy.wait()
    gather.drain()
    scatter.drain()


def layer_call(grid, tokens, cotangent, lengths, qkv_part, out_part, in_part, down_part, smalls_in):
    rows, heads_wide = out_part.shape
    wide = 2 * heads_wide
    width = rows * grid.nz * 4
    half = tokens.shape[0]
    slots = 2 * half
    units = in_part.shape[2]
    heads = heads_wide // HEAD
    shapes = [
        jax.ShapeDtypeStruct((half, width), bf16),
        jax.ShapeDtypeStruct((half, width), f32),
        jax.ShapeDtypeStruct((3, rows, heads_wide), f32),
        jax.ShapeDtypeStruct((rows, heads_wide), f32),
        jax.ShapeDtypeStruct(in_part.shape, f32),
        jax.ShapeDtypeStruct((rows, units), f32),
        *(jax.ShapeDtypeStruct(part.shape, f32) for part in smalls_in),
        jax.ShapeDtypeStruct((heads, slots, slots), bf16),
    ]
    vmem = pl.BlockSpec(memory_space=pltpu.VMEM)
    smem = pl.BlockSpec(memory_space=pltpu.SMEM)
    anywhere = pl.BlockSpec(memory_space=pl.ANY)
    smalls = small_slots(grid)
    dma = pltpu.SemaphoreType.DMA
    wides = (wide, wide, units, units, units // 2, units // 2)
    scratch = (
        [pltpu.VMEM((width, w), bf16) for w in wides]
        + [
            pltpu.VMEM((16, 128), f32),
            pltpu.VMEM((16, 256), f32),
            pltpu.VMEM((16 * grid.slots, 256), f32),
            pltpu.VMEM((16, width), f32),
            pltpu.VMEM((smalls, 16, width), f32),
            pltpu.VMEM((16, width), f32),
            pltpu.VMEM((slots, width), bf16),
            pltpu.VMEM((slots, 3 * heads_wide), bf16),
            pltpu.VMEM((slots, 128), f32),
            pltpu.VMEM((slots, heads_wide), bf16),
            pltpu.VMEM((slots, 3 * units), bf16),
            pltpu.VMEM((slots, 128), bf16),
            pltpu.VMEM((slots, 128), bf16),
            pltpu.VMEM((slots, 128), bf16),
            pltpu.VMEM((half, max(2 * slots - 256, 2 * width + 128)), f32),
            pltpu.VMEM((slots, width), bf16),
            pltpu.VMEM((slots, width), bf16),
            pltpu.VMEM((half, width), bf16),
            pltpu.VMEM((2, half, width), bf16),
            pltpu.VMEM((24, units), f32),
            pltpu.VMEM((width, slots), bf16),
            pltpu.VMEM((2, 128, slots), bf16),
            pltpu.VMEM((128, slots), bf16),
            pltpu.VMEM((128, slots), bf16),
        ]
        + [pltpu.VMEM((width, w), bf16) for w in wides]
        + [pltpu.VMEM((scatter_slots(grid), rows, w), bf16) for w in wides]
        + [
            dma((7, grid.slots)),
            dma((7, grid.slots)),
            dma((6, scatter_slots(grid))),
            dma((6, scatter_slots(grid))),
            dma((smalls,)),
            dma((smalls,)),
            dma((8,)),
            dma((9,)),
            dma((9,)),
            dma((5,)),
            dma((2,)),
        ]
    )
    results = pl.pallas_call(
        functools.partial(layer_body, grid, rows),
        out_shape=shapes,
        in_specs=[anywhere, anywhere, smem] + [anywhere] * 4 + [vmem] * 4,
        out_specs=[vmem, anywhere] + [vmem] * 8 + [anywhere],
        scratch_shapes=scratch,
        compiler_params=pltpu.CompilerParams(collective_id=0, has_side_effects=True, vmem_limit_bytes=VMEM_LIMIT),
        name="layer",
    )(tokens, cotangent, lengths, qkv_part, out_part, in_part, down_part, *smalls_in)
    return results[:10]


norm_epsilon = 1e-06


def norm_forward(values, gain_row, shift_row):
    centred = values - jnp.mean(values, axis=-1, keepdims=True)
    variance = jnp.mean(centred * centred, axis=-1, keepdims=True)
    inv_scale = lax.rsqrt(variance + norm_epsilon)
    unit_vals = centred * inv_scale
    return (unit_vals * gain_row + shift_row, unit_vals, inv_scale)


def norm_backward(grad_out, unit_vals, inv_scale, gain_row):
    grad_unit = grad_out * gain_row
    inner_term = (
        grad_unit
        - jnp.mean(grad_unit, axis=-1, keepdims=True)
        - unit_vals * jnp.mean(grad_unit * unit_vals, axis=-1, keepdims=True)
    )
    return (
        inner_term * inv_scale,
        jnp.sum(grad_out * unit_vals, axis=0),
        jnp.sum(grad_out, axis=0),
    )


def score_block(query_block, first_row, key_heads, slopes, key_valid):
    block_size = query_block.shape[0]
    heads_here = slopes.shape[0]
    query_heads = query_block.reshape(block_size, heads_here, HEAD)
    raw_scores = jnp.einsum(
        "qhc,khc->hqk", query_heads, key_heads, preferred_element_type=jnp.float32
    )
    query_pos = first_row + lax.iota(jnp.int32, block_size)
    key_pos = lax.iota(jnp.int32, key_heads.shape[0])
    distance = jnp.abs(query_pos[:, None] - key_pos[None, :]).astype(jnp.float32)
    scores = 0.125 * raw_scores - slopes[:, None, None] * distance[None, :, :]
    return (jnp.where(key_valid[None, None, :], scores, -1e30), query_heads)


def attend(queries, key_rows, value_rows, slopes, key_valid):
    slot_count, width_here = queries.shape
    heads_here = width_here // HEAD
    block_size = min(512, slot_count)
    key_heads = key_rows.reshape(slot_count, heads_here, HEAD)
    value_heads = value_rows.reshape(slot_count, heads_here, HEAD)

    def one_block(first_row):
        query_block = lax.dynamic_slice_in_dim(queries, first_row, block_size, 0)
        scores, query_heads = score_block(query_block, first_row, key_heads, slopes, key_valid)
        row_max = jnp.max(scores, axis=-1, keepdims=True)
        exp_scores = jnp.exp(scores - row_max)
        row_total = jnp.sum(exp_scores, axis=-1, keepdims=True)
        weights = (exp_scores / row_total).astype(jnp.bfloat16)
        mixed_block = jnp.einsum(
            "hqk,khc->qhc", weights, value_heads, preferred_element_type=jnp.float32
        )
        return (
            mixed_block.reshape(block_size, width_here).astype(jnp.bfloat16),
            (row_max + jnp.log(row_total))[..., 0],
        )

    first_rows = lax.iota(jnp.int32, slot_count // block_size) * block_size
    mixed_heads, logsum = lax.map(one_block, first_rows)
    return (mixed_heads.reshape(slot_count, width_here), logsum)


def attend_back(queries, key_rows, value_rows, grad_mixed, logsum, slopes, key_valid):
    slot_count, width_here = queries.shape
    heads_here = width_here // HEAD
    block_size = min(512, slot_count)
    key_heads = key_rows.reshape(slot_count, heads_here, HEAD)
    value_heads = value_rows.reshape(slot_count, heads_here, HEAD)

    def one_block(running, block_item):
        grad_keys, grad_values = running
        first_row, block_lse = block_item
        query_block = lax.dynamic_slice_in_dim(queries, first_row, block_size, 0)
        grad_block = lax.dynamic_slice_in_dim(grad_mixed, first_row, block_size, 0)
        scores, query_heads = score_block(query_block, first_row, key_heads, slopes, key_valid)
        probs = jnp.exp(scores - block_lse[..., None])
        grad_heads = grad_block.reshape(block_size, heads_here, HEAD)
        grad_probs = jnp.einsum(
            "qhc,khc->hqk", grad_heads, value_heads, preferred_element_type=jnp.float32
        )
        row_dot = jnp.sum(probs * grad_probs, axis=-1, keepdims=True)
        grad_scores = (probs * (grad_probs - row_dot)).astype(jnp.bfloat16)
        grad_query = 0.125 * jnp.einsum(
            "hqk,khc->qhc", grad_scores, key_heads, preferred_element_type=jnp.float32
        )
        grad_keys = grad_keys + 0.125 * jnp.einsum(
            "hqk,qhc->khc", grad_scores, query_heads, preferred_element_type=jnp.float32
        )
        grad_values = grad_values + jnp.einsum(
            "hqk,qhc->khc",
            probs.astype(jnp.bfloat16),
            grad_heads,
            preferred_element_type=jnp.float32,
        )
        return ((grad_keys, grad_values), grad_query.reshape(block_size, width_here))

    first_rows = lax.iota(jnp.int32, slot_count // block_size) * block_size
    zero_grads = jnp.zeros((slot_count, heads_here, HEAD), jnp.float32)
    (grad_keys, grad_values), grad_queries = lax.scan(
        one_block, (zero_grads, zero_grads), (first_rows, logsum)
    )
    return (
        grad_queries.reshape(slot_count, width_here),
        grad_keys.reshape(slot_count, width_here),
        grad_values.reshape(slot_count, width_here),
    )


def spread(part, index, count):
    wide = jnp.tile(part, (1, count))
    owner = lax.broadcasted_iota(jnp.int32, wide.shape, 1) // part.shape[1]
    return jnp.where(owner == index, wide.astype(jnp.float32), 0.0)


def pick(whole, index, count):
    size = whole.shape[1] // count
    return lax.dynamic_slice_in_dim(whole, index * size, size, 1)


def pack_small(biases_qv, biases_in, rows_all, piece, pieces):
    width = rows_all.shape[1]
    halves = [b if pieces == 1 else spread(b, piece, pieces) for b in (biases_qv, biases_in)]
    rows = [rows_all] + [h.reshape(-1, width) for h in halves]
    packed = jnp.concatenate(rows, axis=0)
    return jnp.pad(packed, ((0, -packed.shape[0] % 8), (0, 0)))


def unpack_small(packed, width_qv, width_in, piece, pieces):
    width = packed.shape[1]
    count_qv = 2 * width_qv * pieces // width
    count_in = 2 * width_in * pieces // width
    whole_qv = packed[6 : 6 + count_qv].reshape(2, -1)
    whole_in = packed[6 + count_qv : 6 + count_qv + count_in].reshape(2, -1)
    return packed[:6], pick(whole_qv, piece, pieces), pick(whole_in, piece, pieces)


def per_device(
    direct,
    tokens,
    lengths,
    qkv_weight,
    qv_bias,
    out_weight,
    in_weight,
    in_bias,
    down_weight,
    norm_gains,
    offsets,
    cotangent,
):
    row_count = tokens.shape[0]
    dp = lax.axis_size("dp")
    pieces = lax.axis_size("tensor")
    piece_index = lax.axis_index("tensor")
    dp_index = lax.axis_index("dp")
    flat_index = dp_index * pieces + piece_index
    grid = Grid3(dp)
    if direct:
        output, grad_tokens, to_qkv, to_out, to_in, to_down, to_gains, to_offsets, to_qv_bias, to_in_bias = layer_call(
            grid,
            tokens,
            cotangent,
            lengths,
            qkv_weight,
            out_weight.T,
            in_weight,
            down_weight.T,
            (norm_gains, offsets, qv_bias, in_bias),
        )
        return output, grad_tokens, to_qkv, to_qv_bias, to_out.T, to_in, to_in_bias, to_down.T, to_gains, to_offsets
    slot_count = row_count * pieces
    length = lengths[0]
    heads_here = qkv_weight.shape[2] // HEAD
    head_ids = (piece_index * heads_here + lax.iota(jnp.int32, heads_here)).astype(jnp.float32)
    slopes = jnp.exp2(-8.0 * (head_ids + 1.0) / (heads_here * pieces))
    key_valid = lax.iota(jnp.int32, slot_count) < length
    row_valid = (piece_index * row_count + lax.iota(jnp.int32, row_count) < length).astype(
        jnp.float32
    )[:, None]

    width_qv, width_in = qkv_weight.shape[2], in_weight.shape[2]
    parts = (qkv_weight, out_weight.T, in_weight, down_weight.T)
    small = pack_small(
        spread(qv_bias, dp_index, dp),
        spread(in_bias, dp_index, dp),
        jnp.concatenate([spread(norm_gains, flat_index, dp * pieces), spread(offsets, flat_index, dp * pieces)]),
        piece_index,
        pieces,
    )
    whole_qkv, whole_out_t, whole_in, whole_down_t = (
        lax.all_gather(p, "dp", axis=p.ndim - 2, tiled=True) for p in parts
    )
    small = lax.psum(small, ("dp", "tensor"))
    rows_all, whole_bqv, whole_bin = unpack_small(small, width_qv, width_in, piece_index, pieces)
    gains, shift_rows = rows_all[:2], rows_all[2:6]

    gathered = lax.all_gather(tokens, "tensor", axis=0, tiled=True)
    projected = jnp.einsum("sd,kdc->ksc", gathered, whole_qkv, preferred_element_type=jnp.float32)
    queries = (projected[0] + whole_bqv[0]).astype(jnp.bfloat16)
    key_rows = projected[1].astype(jnp.bfloat16)
    value_rows = (projected[2] + whole_bqv[1]).astype(jnp.bfloat16)
    mixed_heads, logsum = attend(queries, key_rows, value_rows, slopes, key_valid)
    attn_part = jnp.einsum("sc,dc->sd", mixed_heads, whole_out_t, preferred_element_type=jnp.float32)
    attn_total = lax.psum_scatter(
        attn_part.astype(jnp.bfloat16), "tensor", scatter_dimension=0, tiled=True
    ).astype(jnp.float32)
    first_in = tokens.astype(jnp.float32) + attn_total + shift_rows[0]
    attended, unit_one, scale_one = norm_forward(first_in, gains[0], shift_rows[1])
    attended_low = attended.astype(jnp.bfloat16)
    gathered_ff = lax.all_gather(attended_low, "tensor", axis=0, tiled=True)
    pre_acts = jnp.einsum("sd,kdc->ksc", gathered_ff, whole_in, preferred_element_type=jnp.float32)
    pre_acts = pre_acts + whole_bin[:, None, :]
    hidden = (jax.nn.gelu(pre_acts[0], approximate=False) * pre_acts[1]).astype(jnp.bfloat16)
    ff_part = jnp.einsum("sf,df->sd", hidden, whole_down_t, preferred_element_type=jnp.float32)
    ff_total = lax.psum_scatter(
        ff_part.astype(jnp.bfloat16), "tensor", scatter_dimension=0, tiled=True
    ).astype(jnp.float32)
    second_in = attended + ff_total + shift_rows[2]
    final_norm, unit_two, scale_two = norm_forward(second_in, gains[1], shift_rows[3])
    output = (final_norm * row_valid).astype(jnp.bfloat16)
    grad_final = cotangent.astype(jnp.float32) * row_valid
    grad_second, grad_gain_two, grad_shift_two = norm_backward(
        grad_final, unit_two, scale_two, gains[1]
    )
    grad_bdown = jnp.sum(grad_second, axis=0)
    grad_ff_rows = lax.all_gather(grad_second.astype(jnp.bfloat16), "tensor", axis=0, tiled=True)
    grad_down_t = jnp.einsum("sd,sf->df", grad_ff_rows, hidden, preferred_element_type=jnp.float32)
    grad_hidden = jnp.einsum("sd,df->sf", grad_ff_rows, whole_down_t, preferred_element_type=jnp.float32)
    pullback = jax.vjp(
        lambda gate_pre, up_pre: jax.nn.gelu(gate_pre, approximate=False) * up_pre,
        pre_acts[0],
        pre_acts[1],
    )[1]
    grad_gate, grad_up = pullback(grad_hidden)
    grad_pre = jnp.stack([grad_gate, grad_up]).astype(jnp.bfloat16)
    grad_bin = jnp.sum(grad_pre, axis=1, dtype=jnp.float32)
    grad_in = jnp.einsum("sd,ksc->kdc", gathered_ff, grad_pre, preferred_element_type=jnp.float32)
    ff_back = jnp.einsum("ksc,kdc->sd", grad_pre, whole_in, preferred_element_type=jnp.float32)
    grad_attended = grad_second + lax.psum_scatter(
        ff_back.astype(jnp.bfloat16), "tensor", scatter_dimension=0, tiled=True
    ).astype(jnp.float32)
    grad_first, grad_gain_one, grad_shift_one = norm_backward(
        grad_attended, unit_one, scale_one, gains[0]
    )
    grad_bout = jnp.sum(grad_first, axis=0)
    grad_attn_rows = lax.all_gather(grad_first.astype(jnp.bfloat16), "tensor", axis=0, tiled=True)
    grad_out_t = jnp.einsum("sd,sc->dc", grad_attn_rows, mixed_heads, preferred_element_type=jnp.float32)
    grad_mixed = jnp.einsum(
        "sd,dc->sc", grad_attn_rows, whole_out_t, preferred_element_type=jnp.float32
    ).astype(jnp.bfloat16)
    grad_queries, grad_keys, grad_values = attend_back(
        queries, key_rows, value_rows, grad_mixed, logsum, slopes, key_valid
    )
    grad_qkv = jnp.stack([grad_queries, grad_keys, grad_values]).astype(jnp.bfloat16)
    grad_wqkv = jnp.einsum("sd,ksc->kdc", gathered, grad_qkv, preferred_element_type=jnp.float32)
    grad_bqv = jnp.stack(
        [
            jnp.sum(grad_qkv[0], axis=0, dtype=jnp.float32),
            jnp.sum(grad_qkv[2], axis=0, dtype=jnp.float32),
        ]
    )
    input_back = jnp.einsum("ksc,kdc->sd", grad_qkv, whole_qkv, preferred_element_type=jnp.float32)
    grad_tokens = grad_first + lax.psum_scatter(
        input_back.astype(jnp.bfloat16), "tensor", scatter_dimension=0, tiled=True
    ).astype(jnp.float32)

    small_grads = pack_small(
        grad_bqv,
        grad_bin,
        jnp.stack([grad_gain_one, grad_gain_two, grad_bout, grad_shift_one, grad_bdown, grad_shift_two]),
        piece_index,
        pieces,
    )
    grads = tuple(g.astype(jnp.bfloat16) for g in (grad_wqkv, grad_out_t, grad_in, grad_down_t))
    shard_wqkv, shard_out_t, shard_in, shard_down_t = (
        lax.psum_scatter(g.astype(jnp.float32), "dp", scatter_dimension=g.ndim - 2, tiled=True) for g in grads
    )
    small_grads = lax.psum(small_grads, ("dp", "tensor"))
    row_grads, bqv_grads, bin_grads = unpack_small(small_grads, width_qv, width_in, piece_index, pieces)
    own_rows = pick(row_grads, flat_index, dp * pieces)
    return (
        output,
        grad_tokens,
        shard_wqkv,
        pick(bqv_grads, dp_index, dp),
        shard_out_t.T,
        shard_in,
        pick(bin_grads, dp_index, dp),
        shard_down_t.T,
        own_rows[:2],
        own_rows[2:],
    )


def solution(mesh):
    placed = (
        P(("dp", "tensor"), None),
        P("dp"),
        P(None, "dp", "tensor"),
        P(None, ("tensor", "dp")),
        P("tensor", "dp"),
        P(None, "dp", "tensor"),
        P(None, ("tensor", "dp")),
        P("tensor", "dp"),
        P(None, ("dp", "tensor")),
        P(None, ("dp", "tensor")),
        P(("dp", "tensor"), None),
    )

    def run(*args):
        dp = mesh.shape["dp"]
        direct = dp % 4 == 0 and (args[2].shape[1] // dp) % 16 == 0 and mesh.shape["tensor"] == 2
        return jax.shard_map(
            functools.partial(per_device, direct),
            mesh=mesh,
            in_specs=placed,
            out_specs=(
                P(("dp", "tensor"), None),
                P(("dp", "tensor"), None),
                P(None, "dp", "tensor"),
                P(None, ("tensor", "dp")),
                P("tensor", "dp"),
                P(None, "dp", "tensor"),
                P(None, ("tensor", "dp")),
                P("tensor", "dp"),
                P(None, ("dp", "tensor")),
                P(None, ("dp", "tensor")),
            ),
            check_vma=False,
        )(*args)

    return run
```

```python
import functools
import itertools

import jax
import jax.numpy as jnp
from jax import lax
from jax.experimental import pallas as pl
from jax.experimental.pallas import tpu as pltpu
from jax.sharding import PartitionSpec as P

HEAD = 64
MESH = pl.DeviceIdType.MESH
VMEM_LIMIT = 64 * 1024 * 1024 - 65536


class Grid3:
    def __init__(self, dp):
        self.nz = dp // 4
        self.slots = dp

    def here(self):
        me = lax.axis_index("dp")
        self.z, self.y, self.x = me // 4, (me // 2) % 2, me % 2
        z, nz = self.z, self.nz
        self.low, self.high = z > 0, z < nz - 1
        near = [sorted(range(1, nz), key=lambda k: (abs((p + k) % nz - p), k)) for p in range(nz)]
        self.by_distance = [(sum(jnp.where(z == p, near[p][j], 0) for p in range(nz)), 0, 0) for j in range(nz - 1)]
        self.line = []
        for d in self.by_distance:
            above = (z + d[0]) % nz > z
            self.line.append((above, jnp.where(above, z, nz - 1 - z) > 0))

    def at(self, dz, dy, dx):
        y = 1 - self.y if dy else self.y
        x = 1 - self.x if dx else self.x
        return (((self.z + dz) % self.nz) * 2 + y) * 2 + x

    def slot(self, d):
        return (d[0] % self.nz) * 4 + d[1] * 2 + d[2]

    def steps(self, axis):
        if axis == "z":
            return [(k, 0, 0) for k in range(1, self.nz)]
        return [(0, 1, 0)] if axis == "y" else [(0, 0, 1)]

    def seen_from(self, d, move):
        return ((d[0] - move[0] + self.nz) % self.nz, d[1] ^ move[1], d[2] ^ move[2])

    def span(self, axis):
        if axis == "z":
            return [(k, 0, 0) for k in range(self.nz)]
        return [(0, 0, 0), (0, 1, 0)] if axis == "y" else [(0, 0, 0), (0, 0, 1)]


def joined(*ds):
    return tuple(sum(part) for part in zip(*ds))


def remote(src, dst, send_sem, recv_sem, **device):
    return pltpu.make_async_remote_copy(
        src_ref=src, dst_ref=dst, send_sem=send_sem, recv_sem=recv_sem, device_id=device, device_id_type=MESH
    )


def greet(grid, partner):
    barrier = pltpu.get_barrier_semaphore()
    moves = [m for axis in "zyx" for m in grid.steps(axis)]
    for move in moves:
        pl.semaphore_signal(barrier, inc=1, device_id={"dp": grid.at(*move)}, device_id_type=MESH)
    pl.semaphore_signal(barrier, inc=1, device_id={"tensor": partner}, device_id_type=MESH)
    pl.semaphore_wait(barrier, len(moves) + 1)


class SmallSum:
    def __init__(self, grid, value, out, box, send, recv):
        self.grid = grid
        self.value, self.out, self.box, self.send, self.recv = value, out, box, send, recv
        self.copies = []

    def _post(self, slot, **device):
        copy = remote(self.out, self.box.at[slot], self.send.at[slot], self.recv.at[slot], **device)
        copy.start()
        self.copies.append(copy)

    def stage(self, number):
        grid = self.grid
        if number == 0:
            self.out[...] = self.value[...]
            self._post(0, tensor=1 - lax.axis_index("tensor"))
            return
        for copy in self.copies:
            copy.wait()
        self.copies = []
        if number == 1:
            self.out[...] = self.out[...] + self.box[0]
            for k in range(1, grid.nz):
                self._post(2 + k, dp=grid.at(k, 0, 0))
        elif number == 2:
            total = self.out[...]
            for k in range(1, grid.nz):
                total = total + self.box[2 + k]
            self.out[...] = total
            self._post(1, dp=grid.at(0, 0, 1))
        elif number == 3:
            self.out[...] = self.out[...] + self.box[1]
            self._post(2, dp=grid.at(0, 1, 0))
        else:
            self.out[...] = self.out[...] + self.box[2]


def small_slots(grid):
    return 2 + grid.nz


class Gather:
    def __init__(self, grid, chunks, send, recv):
        self.grid, self.chunks = grid, chunks
        self.send_sem, self.recv_sem = send, recv
        self.sent = []

    def _dst(self, number, d):
        rows = self.chunks[number][0].shape[0]
        return self.chunks[number][1].at[pl.ds(pl.multiple_of(self.grid.at(*d) * rows, rows), rows)]

    def _copy(self, number, d, move):
        dst = self._dst(number, d)
        if isinstance(move, int):
            move = (jnp.where(self.grid.line[move][0], -1, 1), 0, 0)
        source = self.chunks[number][0] if isinstance(d[0], int) and d == (0, 0, 0) else dst
        slot = self.grid.slot(self.grid.seen_from(d, move))
        return remote(source, dst, self.send_sem.at[number, slot], self.recv_sem.at[number, slot], dp=self.grid.at(*move))

    def _start(self, allowed, *args):
        if allowed is None:
            self._copy(*args).start()
        else:
            pl.when(allowed)(lambda: self._copy(*args).start())
        self.sent.append((allowed, args))

    def send(self, number, d, axis):
        if axis == "z":
            self._start(self.grid.low, number, d, (-1, 0, 0))
            self._start(self.grid.high, number, d, (1, 0, 0))
        else:
            self._start(None, number, d, self.grid.steps(axis)[0])

    def relay(self, number, d, j):
        self._start(self.grid.line[j][1], number, d, j)

    def arrive(self, number, d):
        dst, slot = self._dst(number, d), self.grid.slot(d)
        remote(dst, dst, self.send_sem.at[number, slot], self.recv_sem.at[number, slot], dp=self.grid.at(*d)).wait_recv()

    def moved(self, axis):
        return self.grid.by_distance if axis == "z" else self.grid.steps(axis)

    def first(self, number):
        return [(self.pass_first, number, d, j) for j, d in enumerate(self.moved(self.chunks[number][2][0]))]

    def second(self, number):
        one, two = self.chunks[number][2][:2]
        return [
            (self.pass_second, number, joined(a, b), j) for j, b in enumerate(self.moved(two)) for a in self.grid.span(one)
        ]

    def third(self, number):
        one, two, three = self.chunks[number][2]
        return [joined(a, b, c) for a in self.grid.span(one) for b in self.grid.span(two) for c in self.grid.steps(three)]

    def pass_first(self, number, d, j):
        order = self.chunks[number][2]
        self.arrive(number, d)
        if order[0] == "z":
            self.relay(number, d, j)
        for axis in order[1:]:
            self.send(number, d, axis)

    def pass_second(self, number, d, j):
        order = self.chunks[number][2]
        self.arrive(number, d)
        if order[1] == "z":
            self.relay(number, d, j)
        self.send(number, d, order[2])

    def finish(self, number):
        for d in self.third(number):
            self.arrive(number, d)

    def drain(self):
        for allowed, args in self.sent:
            if allowed is None:
                self._copy(*args).wait_send()
            else:
                pl.when(allowed)(lambda args=args: self._copy(*args).wait_send())
        self.sent = []


class Scatter:
    def __init__(self, grid, rows, chunks, send, recv):
        self.grid, self.rows, self.chunks = grid, rows, chunks
        self.send_sem, self.recv_sem = send, recv
        self.sent = []
        self.far_first = [2, 1, 3] if grid.nz == 4 else list(range(1, grid.nz))
        self.second, self.line, self.crossing = 2 * grid.nz, 3 * grid.nz - 1, 4 * grid.nz - 2

    def part(self, number, d):
        return self.chunks[number][0].at[pl.ds(pl.multiple_of(self.grid.at(*d) * self.rows, self.rows), self.rows)]

    def box(self, number, slot):
        return self.chunks[number][3].at[slot]

    def other(self, number):
        return "y" if self.chunks[number][2][0] == "x" else "x"

    def place(self, number, dz, e):
        return (dz, e, 0) if self.other(number) == "y" else (dz, 0, e)

    def _copy(self, number, kind, dz, e=0):
        grid = self.grid
        if kind == "own":
            move = grid.steps(self.chunks[number][2][0])[0]
            source, slot = self.part(number, joined(self.place(number, dz, e), move)), dz * 2 + e
        elif kind == "side":
            move = grid.steps(self.other(number))[0]
            source, slot = self.box(number, dz * 2 + 1), self.second + dz
        elif kind == "cross":
            move = grid.steps(self.other(number))[0]
            source, slot = self.box(number, 1), self.crossing
        elif kind == "middle":
            move = (dz, 0, 0)
            source, slot = self.box(number, dz * 2 + e), self.middle_slot(dz, e)
        else:
            move = (dz, 0, 0)
            source, slot = self.box(number, dz * 2), self.line + dz
        return remote(
            source, self.box(number, slot), self.send_sem.at[number, slot], self.recv_sem.at[number, slot], dp=grid.at(*move)
        )

    def _send(self, *args):
        self._copy(*args).start()
        self.sent.append(args)

    def _arrive(self, number, slot):
        box = self.box(number, slot)
        remote(box, box, self.send_sem.at[number, slot], self.recv_sem.at[number, slot], dp=0).wait_recv()

    def begin(self, number, *halves):
        for e in halves or (1, 0):
            for dz in self.far_first + [0]:
                self._send(number, "own", dz, e)

    def held(self, number, dz, e):
        slot = dz * 2 + e
        self._arrive(number, slot)
        return self.part(number, self.place(number, dz, e))[...].astype(jnp.float32) + self.box(number, slot)[...].astype(jnp.float32)

    def side(self, number, dz):
        self.box(number, dz * 2 + 1)[...] = self.held(number, dz, 1).astype(jnp.bfloat16)
        self._send(number, "side", dz)

    def both(self, number, dz):
        value = self.held(number, dz, 0)
        self._arrive(number, self.second + dz)
        return value + self.box(number, self.second + dz)[...].astype(jnp.float32)

    def along(self, number, dz):
        self.box(number, dz * 2)[...] = self.both(number, dz).astype(jnp.bfloat16)
        self._send(number, "line", dz)

    def middle_slot(self, dz, e):
        return self.second + e * (self.grid.nz - 1) + dz - 1

    def middle(self, number, dz, e):
        self.box(number, dz * 2 + e)[...] = self.held(number, dz, e).astype(jnp.bfloat16)
        self._send(number, "middle", dz, e)

    def line_total(self, number, e):
        total = self.held(number, 0, e)
        for dz in self.far_first:
            slot = self.middle_slot(dz, e)
            self._arrive(number, slot)
            total = total + self.box(number, slot)[...].astype(jnp.float32)
        return total

    def cross(self, number):
        self.box(number, 1)[...] = self.line_total(number, 1).astype(jnp.bfloat16)
        self._send(number, "cross", 0)

    def z_second(self, number):
        return self.chunks[number][2][1] == "z"

    def sides(self, *numbers):
        if self.z_second(numbers[0]):
            return [(self.middle, n, dz, e) for e in (1, 0) for dz in self.far_first for n in numbers]
        return [(self.side, n, dz) for dz in self.far_first + [0] for n in numbers]

    def lines(self, *numbers):
        if self.z_second(numbers[0]):
            return [(self.cross, n) for n in numbers]
        return [(self.along, n, dz) for dz in self.far_first for n in numbers]

    def lasts(self, *numbers):
        return [(self.last, n) for n in numbers]

    def last(self, number):
        if self.z_second(number):
            total = self.line_total(number, 0)
            self._arrive(number, self.crossing)
            total = total + self.box(number, self.crossing)[...].astype(jnp.float32)
        else:
            total = self.both(number, 0)
            for dz in self.far_first:
                self._arrive(number, self.line + dz)
                total = total + self.box(number, self.line + dz)[...].astype(jnp.float32)
        self.chunks[number][1](total)

    def drain(self):
        for args in self.sent:
            self._copy(*args).wait_send()
        self.sent = []


def scatter_slots(grid):
    return 4 * grid.nz - 1
bf16, f32 = jnp.bfloat16, jnp.float32
NORM_EPSILON = 1e-06
EARLY = 12
AFTER_PROJECTION = 4
GATHER_STEPS = 4
AFTER_OUT = 4
AFTER_NORM = 4
ROOT_HALF = 0.7071067811865476
PHI_SCALE = 0.3989422804014327


def nn(a, b):
    return jnp.dot(a, b, preferred_element_type=f32)


def nt(a, b):
    return lax.dot_general(a, b, (((1,), (1,)), ((), ())), preferred_element_type=f32)


def aligned(start, size):
    return pl.ds(pl.multiple_of(start, size), size)


def unit_rows(values):
    centred = values - jnp.mean(values, axis=-1, keepdims=True)
    variance = jnp.mean(centred * centred, axis=-1, keepdims=True)
    scale = lax.rsqrt(variance + NORM_EPSILON)
    return centred * scale, scale


def unit_back(grad_unit, unit, scale):
    inner = (
        grad_unit
        - jnp.mean(grad_unit, axis=-1, keepdims=True)
        - unit * jnp.mean(grad_unit * unit, axis=-1, keepdims=True)
    )
    return inner * scale


def fold(rows):
    return jnp.sum(rows.reshape(rows.shape[0] // 8, 8, rows.shape[1]), axis=0)


def merged(*lists):
    return [entry for row in itertools.zip_longest(*lists) for entry in row if entry is not None]


class Pump:
    def __init__(self, steps=()):
        self.steps = list(steps)

    def take(self, count=None):
        count = len(self.steps) if count is None else min(count, len(self.steps))
        taken, self.steps = self.steps[:count], self.steps[count:]
        return taken

    def run(self, count=None):
        for function, *args in self.take(count):
            function(*args)


def at_trips(*shares):
    def run(index):
        for trip, share in enumerate(shares):

            @pl.when(index == trip)
            def _(share=share):
                Pump(share).run()

    return run


def layer_body(
    grid, rows,
    tokens, cotangent, length, qkv_part, out_part, in_part, down_part, gains_part, offsets_part, qv_bias, in_bias,
    output, grad_tokens, to_qkv, to_out, to_in, to_down, to_gains, to_offsets, to_qv_bias, to_in_bias, probs_far,
    w_qv, w_ko, w_gate, w_up, w_low, w_high, small_mine, small_pair, small_tiles, every_small, small_box, small_grads,
    x, qkv, inverse, mixed, work, key_aug, value_aug, query_aug,
    rows_f32, attended_low, branch_rows, outgoing, incoming, turned,
    grad_t, pair_b, grad_value_t, grad_key_t,
    g_qv, g_ko, g_gate, g_up, g_low, g_high, box_qv, box_ko, box_gate, box_up, box_low, box_high,
    gather_send, gather_recv, scatter_send, scatter_recv, small_send, small_recv, own_sem, swap_send, swap_recv, local_sem, prob_sem,
):
    grid.here()
    side = lax.axis_index("tensor")
    other = 1 - side
    half = tokens.shape[0]
    slots = 2 * half
    width = tokens.shape[1]
    heads_wide = mixed.shape[1]
    units = w_gate.shape[1]
    mine = aligned(side * half, half)
    count = length[0]
    attended, unit_one = rows_f32.at[:, pl.ds(0, width)], rows_f32.at[:, pl.ds(width, width)]
    scale_one = rows_f32.at[:, pl.ds(2 * width, 128)]
    block = 256
    span = 2 * slots - block
    bias = rows_f32.at[pl.ds(0, block), pl.ds(0, span)]

    own_rows = aligned(grid.at(0, 0, 0) * rows, rows)
    low, high = pl.ds(0, units // 2), pl.ds(units // 2, units // 2)
    one_head, two_head = pl.ds(0, heads_wide), pl.ds(heads_wide, heads_wide)
    own_copies = [
        pltpu.make_async_copy(source, target, own_sem.at[n])
        for n, (source, target) in enumerate(
            [
                (qkv_part.at[0], w_qv.at[own_rows, one_head]),
                (qkv_part.at[2], w_qv.at[own_rows, two_head]),
                (qkv_part.at[1], w_ko.at[own_rows, one_head]),
                (out_part, w_ko.at[own_rows, two_head]),
                (in_part.at[0], w_gate.at[own_rows]),
                (in_part.at[1], w_up.at[own_rows]),
                (down_part.at[:, low], w_low.at[own_rows]),
                (down_part.at[:, high], w_high.at[own_rows]),
            ]
        )
    ]
    for copy in own_copies:
        copy.start()
    greet(grid, other)

    gather = Gather(grid, [
        (w_qv.at[own_rows], w_qv, "zyx"),
        (w_ko.at[own_rows], w_ko, "zxy"),
        (w_gate.at[own_rows], w_gate, "yzx"),
        (w_up.at[own_rows], w_up, "xzy"),
        (w_low.at[own_rows], w_low, "zyx"),
        (w_high.at[own_rows], w_high, "zxy"),
        (small_pair, small_tiles, "zyx"),
    ], gather_send, gather_recv)
    def sink_qv(total):
        to_qkv[0], to_qkv[2] = total[:, :heads_wide], total[:, heads_wide:]

    def sink_ko(total):
        to_qkv[1] = total[:, :heads_wide]
        to_out[...] = total[:, heads_wide:]

    def sink_gate(total):
        to_in[0] = total

    def sink_up(total):
        to_in[1] = total

    def sink_low(total):
        to_down[:, : units // 2] = total

    def sink_high(total):
        to_down[:, units // 2 :] = total

    scatter = Scatter(grid, rows, [
        (g_qv, sink_qv, "xyz", box_qv),
        (g_ko, sink_ko, "yxz", box_ko),
        (g_gate, sink_gate, "xyz", box_gate),
        (g_up, sink_up, "yxz", box_up),
        (g_low, sink_low, "xzy", box_low),
        (g_high, sink_high, "yzx", box_high),
    ], scatter_send, scatter_recv)
    QV, KO, GATE, UP, LOW, HIGH, SMALL = range(7)

    def swap(source, target, slot):
        copy = remote(source, target, swap_send.at[slot], swap_recv.at[slot], tensor=other)
        copy.start()
        return copy

    token_swap = swap(tokens, x.at[mine], 0)
    token_copy = pltpu.make_async_copy(tokens, x.at[mine], local_sem.at[0])
    token_copy.start()
    cot_copy = pltpu.make_async_copy(cotangent, output, local_sem.at[1])
    cot_copy.start()
    my_lanes = pl.ds(pl.multiple_of(side * 128, 128), 128)
    small_mine[...] = jnp.zeros_like(small_mine)
    small_mine[0:2, 0 : gains_part.shape[1]] = gains_part[...]
    small_mine[2:6, 0 : offsets_part.shape[1]] = offsets_part[...]
    small_mine[8:10, 0 : in_bias.shape[1]] = in_bias[...].astype(f32)
    small_mine[10:12, 0 : qv_bias.shape[1]] = qv_bias[...].astype(f32)
    small_pair[:, my_lanes] = small_mine[...]
    small_swap = swap(small_mine, small_pair.at[:, my_lanes], 8)
    pieces = {QV: (0, 1), KO: (2, 3), GATE: (4,), UP: (5,), LOW: (6,), HIGH: (7,)}
    for n in pieces:
        for piece in pieces[n]:
            own_copies[piece].wait()
        for axis in gather.chunks[n][2]:
            gather.send(n, (0, 0, 0), axis)
        if n == KO:
            small_swap.wait()
            for axis in gather.chunks[SMALL][2]:
                gather.send(SMALL, (0, 0, 0), axis)
            small_tiles[aligned(grid.at(0, 0, 0) * 16, 16), :] = small_pair[...]
    near_units = merged(gather.second(GATE), gather.second(UP))
    ends_first = merged(gather.first(LOW), gather.first(HIGH))
    ends_second = merged(gather.second(LOW), gather.second(HIGH))
    early = (
        merged(gather.first(QV), gather.first(SMALL), gather.first(KO))
        + merged(gather.first(GATE), gather.first(UP))
        + merged(merged(gather.second(QV), gather.second(SMALL), gather.second(KO)), near_units[:EARLY])
    )
    pump = Pump(early)
    pump.run()
    pump = Pump(merged(near_units[EARLY:], ends_first) + ends_second)
    token_copy.wait()
    token_swap.wait()
    for number in (SMALL, QV, KO):
        gather.finish(number)

    norm_rows = jnp.zeros((8, width), f32)
    head_rows = jnp.zeros((8, heads_wide), f32)
    unit_rows_in = jnp.zeros((8, units), f32)

    def at_lanes(tile, lanes, start):
        wide = jnp.concatenate([tile, jnp.zeros((8, lanes - 128), f32)], axis=1)
        return pltpu.roll(wide, start, 1) if start else wide

    for i in range(grid.slots):
        pair_tile = [small_tiles[16 * i : 16 * i + 8, 128 * s : 128 * s + 128] for s in range(2)]
        unit_tile = [small_tiles[16 * i + 8 : 16 * i + 16, 128 * s : 128 * s + 128] for s in range(2)]
        for s in range(2):
            norm_rows = norm_rows + at_lanes(pair_tile[s], width, (2 * i + s) * (rows // 2))
        units_here = jnp.where(side == 0, unit_tile[0], unit_tile[1])
        unit_rows_in = unit_rows_in + at_lanes(units_here, units, i * (units // grid.slots))
        head_rows = head_rows + at_lanes(pltpu.roll(units_here, 6, 0), heads_wide, i * (heads_wide // grid.slots))
    every_small[0:8, :] = norm_rows
    every_small[8:9, pl.ds(0, heads_wide)] = head_rows[0:1, :]
    every_small[8:9, pl.ds(heads_wide, heads_wide)] = head_rows[1:2, :]
    turned[0:8, :] = unit_rows_in

    q_cols, v_cols, k_cols = (pl.ds(i * heads_wide, heads_wide) for i in range(3))
    side_cols = pl.ds(pl.multiple_of(side * heads_wide, 128), heads_wide)
    row_bias = every_small[8:9, :]
    row_scale = jnp.where(lax.broadcasted_iota(jnp.int32, (1, 2 * heads_wide), 1) < heads_wide, 0.125, 1.0)

    @pl.loop(0, slots // 256)
    def _(i):
        r = aligned(i * 256, 256)
        raw = (nn(x[r, :], w_qv[...]) + row_bias).astype(bf16)
        qkv[r, pl.ds(0, 2 * heads_wide)] = (raw.astype(f32) * row_scale).astype(bf16)
        qkv[r, k_cols] = nn(x[r, :], w_ko[:, pl.ds(0, heads_wide)]).astype(bf16)

    pump.run(AFTER_PROJECTION)

    lane = lax.broadcasted_iota(jnp.int32, (slots, 128), 1)
    slot = lax.broadcasted_iota(jnp.int32, (slots, 128), 0)
    key_mask = jnp.where(slot < count, 0.0, -1e30).astype(bf16)
    zero, one = jnp.zeros((), bf16), jnp.ones((), bf16)
    block_lane = lax.broadcasted_iota(jnp.int32, (block, 128), 1)
    pairs = heads_wide // 128
    slopes = [2.0 ** (-8.0 * (h + 1) / (4 * pairs)) for h in range(4 * pairs)]

    def prob_slot(upper):
        return work.at[:, pl.ds(upper * slots, slots)]

    def prob_out(pair, upper):
        return pltpu.make_async_copy(prob_slot(upper), probs_far.at[2 * pair + upper], prob_sem.at[upper])

    def prob_in(pair, upper):
        return pltpu.make_async_copy(probs_far.at[2 * pair + upper], prob_slot(upper), prob_sem.at[upper])

    def pair_cols(pair, start=0):
        return pl.ds(pl.multiple_of(start + pair * 128, 128), 128)

    def attend_pair(pair):
        cols = pair_cols(pair)
        for upper in (0, 1):
            own = (lane >= 64) == (upper == 1)
            spare = 0 if upper else 64
            gap = jnp.abs(
                lax.broadcasted_iota(jnp.int32, (block, span), 0)
                - (lax.broadcasted_iota(jnp.int32, (block, span), 1) - (span - slots))
            )
            slope = sum(
                jnp.where(pair == p, jnp.where(side == 0, slopes[2 * p + upper], slopes[2 * (pairs + p) + upper]), 0.0)
                for p in range(pairs)
            )
            bias[...] = gap.astype(f32) * slope
            key_aug[...] = jnp.where(own, qkv[:, pair_cols(pair, 2 * heads_wide)], jnp.where(lane == spare, key_mask, zero))
            value_aug[...] = jnp.where(own, qkv[:, pair_cols(pair, heads_wide)], one)
            query_aug[...] = jnp.where(own, qkv[:, cols], jnp.where(lane == spare, one, zero))

            @pl.when(pair > 0)
            def _(upper=upper):
                prob_out(pair - 1, upper).wait()

            def attend(i, inner_carry, upper=upper):
                r = aligned(i * block, block)
                scores = nt(query_aug[r, :], key_aug[...]) - bias[:, pl.ds(pl.multiple_of(span - slots - i * block, block), slots)]
                top = jnp.max(scores, axis=1, keepdims=True)
                weights = jnp.exp(scores - top).astype(bf16)
                work[r, pl.ds(upper * slots, slots)] = weights
                product = nn(weights, value_aug[...])
                scale = 1.0 / (product[:, 0:1] if upper else product[:, 64:65])
                result = (product * scale).astype(bf16)
                inverse[r, :] = jnp.where(block_lane == 2 * pair + upper, scale, inverse[r, :])
                mixed[r, cols] = jnp.where(block_lane < 64, mixed[r, cols], result) if upper else result
                return inner_carry

            lax.fori_loop(0, slots // block, attend, 0, unroll=2)
            prob_out(pair, upper).start()
        between_pairs(pair)

    inverse[...] = jnp.zeros_like(inverse)
    between_pairs = at_trips(*(pump.take(GATHER_STEPS) for _ in range(pairs)))
    pl.loop(0, pairs)(attend_pair)

    def project(source, weights, target_rows, sink):
        @pl.loop(0, half // 256)
        def _(i):
            r = aligned(target_rows * half + i * 256, 256)
            sink(i, nt(source[r, :], weights[...]))

    def to_outgoing(i, value):
        outgoing[aligned(i * 256, 256), :] = value.astype(bf16)

    def to_attended(i, value):
        attended[aligned(i * 256, 256), :] = value

    w_out = w_ko.at[:, pl.ds(heads_wide, heads_wide)]
    project(mixed, w_out, other, to_outgoing)
    first_swap = swap(outgoing, incoming.at[0], 1)
    pump.run(AFTER_OUT)
    project(mixed, w_out, side, to_attended)
    first_swap.wait()
    gain_one, gain_two = every_small[0:1, :], every_small[1:2, :]
    step = 128

    @pl.loop(0, half // step)
    def _(i):
        r = aligned(i * step, step)
        own = pl.ds(pl.multiple_of(side * half + i * step, step), step)
        total = x[own, :].astype(f32) + attended[r, :] + incoming[0, r, :].astype(f32) + every_small[2:3, :]
        unit, scale = unit_rows(total)
        result = unit * gain_one + every_small[3:4, :]
        unit_one[r, :] = unit
        scale_one[r, :] = jnp.broadcast_to(scale, (step, 128))
        attended[r, :] = result
        attended_low[own, :] = result.astype(bf16)

    low_swap = swap(attended_low.at[mine], attended_low.at[mine], 2)
    for upper in (0, 1):
        prob_out(pairs - 1, upper).wait()
    pump.run(AFTER_NORM)
    gather.finish(GATE)
    gather.finish(UP)

    def feed(rows_side):
        r = aligned(rows_side * half, half)

        @pl.loop(0, units // 256)
        def _(j):
            c = aligned(j * 256, 256)
            c_up = pl.ds(pl.multiple_of(units + j * 256, 256), 256)
            c_hidden = pl.ds(pl.multiple_of(2 * units + j * 256, 256), 256)
            gate = nn(attended_low[r, :], w_gate[:, c]) + turned[0:1, c]
            up = nn(attended_low[r, :], w_up[:, c]) + turned[1:2, c]
            below = 0.5 * (1.0 + lax.erf(gate * ROOT_HALF))
            density = PHI_SCALE * jnp.exp(-0.5 * gate * gate)
            bent = gate * below
            work[r, c_hidden] = (bent * up).astype(bf16)
            work[r, c] = (up * (below + gate * density)).astype(bf16)
            work[r, c_up] = bent.astype(bf16)

    feed(side)
    pump.run()
    low_swap.wait()
    feed(other)
    pump.run()
    gather.finish(LOW)
    gather.finish(HIGH)

    hidden_low, hidden_high = pl.ds(2 * units, units // 2), pl.ds(2 * units + units // 2, units // 2)

    def down(rows_side, sink):
        @pl.loop(0, half // 256)
        def _(i):
            r = aligned(rows_side * half + i * 256, 256)
            sink(i, nt(work[r, hidden_low], w_low[...]) + nt(work[r, hidden_high], w_high[...]))

    def add_attended(i, value):
        r = aligned(i * 256, 256)
        attended[r, :] = attended[r, :] + value

    down(other, to_outgoing)
    second_swap = swap(outgoing, incoming.at[1], 3)
    down(side, add_attended)
    cot_copy.wait()
    second_swap.wait()
    nothing = jnp.zeros((8, width), f32)

    def second_norm(i, carry):
        sum_gain, sum_shift, sum_branch = carry
        r = aligned(i * step, step)
        own = pl.ds(pl.multiple_of(side * half + i * step, step), step)
        position = side * half + i * step + lax.broadcasted_iota(jnp.int32, (step, 1), 0)
        valid = jnp.where(position < count, 1.0, 0.0)
        unit, scale = unit_rows(attended[r, :] + incoming[1, r, :].astype(f32) + every_small[4:5, :])
        grad = output[r, :].astype(f32) * valid
        output[r, :] = ((unit * gain_two + every_small[5:6, :]) * valid).astype(bf16)
        back = unit_back(grad * gain_two, unit, scale)
        attended[r, :] = back
        branch_rows[own, :] = back.astype(bf16)
        return sum_gain + fold(grad * unit), sum_shift + fold(grad), sum_branch + fold(back)

    gain_two_sum, shift_two_sum, down_bias_sum = lax.fori_loop(0, half // step, second_norm, (nothing,) * 3)
    branch_swap = swap(branch_rows.at[mine], branch_rows.at[mine], 4)
    small_grads[...] = jnp.zeros_like(small_grads)
    small_grads[1:2, :] = jnp.sum(gain_two_sum, axis=0, keepdims=True)
    small_grads[5:6, :] = jnp.sum(shift_two_sum, axis=0, keepdims=True)
    small_grads[4:5, :] = jnp.sum(down_bias_sum, axis=0, keepdims=True)
    branch_swap.wait()

    def turn(source):
        @pl.loop(0, slots // 256)
        def _(i):
            r = aligned(i * 256, 256)
            grad_t[:, r] = source[r, :].T

    def weight_grad(sink, source, source_start, tile):
        @pl.loop(0, sink.shape[1] // tile)
        def _(j):
            sink[:, aligned(j * tile, tile)] = nn(
                grad_t[...], source[:, pl.ds(pl.multiple_of(source_start + j * tile, tile), tile)]
            ).astype(bf16)

    turn(branch_rows)
    weight_grad(g_low, work, 2 * units, 256)
    scatter.begin(LOW)
    weight_grad(g_high, work, 2 * units + units // 2, 256)
    scatter.begin(HIGH)

    turned[8:24, :] = jnp.zeros((16, units), f32)
    for index, weights in enumerate((w_low, w_high)):
        @pl.loop(0, units // 2 // 256)
        def _(j, index=index, weights=weights):
            c = pl.ds(pl.multiple_of(index * (units // 2) + j * 256, 256), 256)
            c_up = pl.ds(pl.multiple_of(units + index * (units // 2) + j * 256, 256), 256)
            for part in range(2):
                r = pl.ds(part * half, half)
                grad = nn(branch_rows[r, :], weights[:, aligned(j * 256, 256)])
                gate_grad = (grad * work[r, c].astype(f32)).astype(bf16)
                up_grad = (grad * work[r, c_up].astype(f32)).astype(bf16)
                work[r, c] = gate_grad
                work[r, c_up] = up_grad
                turned[8:16, c] = turned[8:16, c] + fold(gate_grad.astype(f32))
                turned[16:24, c] = turned[16:24, c] + fold(up_grad.astype(f32))

    for index in range(2):
        total = jnp.sum(turned[8 + 8 * index : 16 + 8 * index, :], axis=0, keepdims=True)
        for j in range(units // width):
            small_grads[pl.ds(8 + 4 * index + 2 * side + j, 1), :] = total[:, j * width : (j + 1) * width]

    sides_ends = Pump(scatter.sides(LOW, HIGH))
    sides_ends.run(6)
    turn(attended_low)
    weight_grad(g_gate, work, 0, 512)
    scatter.begin(GATE, 1)
    weight_grad(g_up, work, units, 512)
    scatter.begin(UP, 1)
    scatter.begin(GATE, 0)
    sides_ends.run()

    gate_cols, up_cols = pl.ds(0, units), pl.ds(units, units)

    def units_back(rows_side, sink):
        @pl.loop(0, half // 256)
        def _(i):
            r = aligned(rows_side * half + i * 256, 256)
            sink(i, nt(work[r, gate_cols], w_gate[...]) + nt(work[r, up_cols], w_up[...]))

    units_back(other, to_outgoing)
    third_swap = swap(outgoing, incoming.at[0], 5)
    units_back(side, add_attended)
    Pump(scatter.lines(LOW, HIGH)).run()
    third_swap.wait()

    def first_norm_back(i, carry):
        sum_gain, sum_shift, sum_branch = carry
        r = aligned(i * step, step)
        own = pl.ds(pl.multiple_of(side * half + i * step, step), step)
        grad = attended[r, :] + incoming[0, r, :].astype(f32)
        unit = unit_one[r, :]
        back = unit_back(grad * gain_one, unit, scale_one[r, 0:1])
        attended[r, :] = back
        branch_rows[own, :] = back.astype(bf16)
        return sum_gain + fold(grad * unit), sum_shift + fold(grad), sum_branch + fold(back)

    prob_in(0, 0).start()
    prob_in(0, 1).start()
    gain_one_sum, shift_one_sum, out_bias_sum = lax.fori_loop(0, half // step, first_norm_back, (nothing,) * 3)
    attn_swap = swap(branch_rows.at[mine], branch_rows.at[mine], 6)
    small_grads[0:1, :] = jnp.sum(gain_one_sum, axis=0, keepdims=True)
    small_grads[3:4, :] = jnp.sum(shift_one_sum, axis=0, keepdims=True)
    small_grads[2:3, :] = jnp.sum(out_bias_sum, axis=0, keepdims=True)
    attn_swap.wait()

    grad_mixed = attended_low.at[:, pl.ds(0, heads_wide)]
    turn(branch_rows)
    g_ko[:, pl.ds(heads_wide, heads_wide)] = nn(grad_t[...], mixed[...]).astype(bf16)
    sides_gate = Pump(scatter.sides(GATE))
    sides_gate.run(2)

    @pl.loop(0, slots // 256)
    def _(i):
        r = aligned(i * 256, 256)
        grad_mixed[r, :] = nn(branch_rows[r, :], w_out[...]).astype(bf16)

    sides_gate.run()
    scatter.begin(UP, 0)

    mixed_t, query_t = pair_b.at[0], pair_b.at[1]

    def pair_back(pair):
        cols, key_cols, value_cols = pair_cols(pair), pair_cols(pair, 2 * heads_wide), pair_cols(pair, heads_wide)
        scales = inverse[...]
        shrink = jnp.where(
            lane < 64,
            jnp.sum(jnp.where(lane == 2 * pair, scales, 0.0), axis=1, keepdims=True),
            jnp.sum(jnp.where(lane == 2 * pair + 1, scales, 0.0), axis=1, keepdims=True),
        )
        scaled = (grad_mixed[:, cols].astype(f32) * shrink).astype(bf16)
        mixed_t[...] = scaled.T
        query_t[...] = qkv[:, cols].T
        outgoing_pair[...] = scaled
        for upper in (0, 1):
            own = (lane >= 64) == (upper == 1)
            spare = 0 if upper else 64
            scaled = outgoing_pair[...]
            dots = jnp.sum(jnp.where(own, scaled.astype(f32) * mixed[:, cols].astype(f32), 0.0), axis=1, keepdims=True)
            dots_high = dots.astype(bf16)
            dots_low = (dots - dots_high.astype(f32)).astype(bf16)
            ones = (lane == spare) | (lane == spare + 1)
            value_aug[...] = jnp.where(own, qkv[:, value_cols], jnp.where(ones, one, zero))
            query_aug[...] = jnp.where(
                own, scaled, jnp.where(lane == spare, -dots_high, jnp.where(lane == spare + 1, -dots_low, zero))
            )
            part = pl.ds(64 * upper, 64)
            base = upper * slots
            prob_in(pair, upper).wait()
            for j in range(slots // 512):
                c = pl.ds(j * 512, 512)
                grad_value_t[part, c] = nn(mixed_t[part, :], work[:, pl.ds(base + j * 512, 512)]).astype(bf16)

            def attend_back(i, inner_carry, upper=upper, base=base):
                r = aligned(i * block, block)
                inner = nt(query_aug[r, :], value_aug[...])
                grads = (work[r, pl.ds(base, slots)].astype(f32) * inner).astype(bf16)
                work[r, pl.ds(base, slots)] = grads
                result = (nn(grads, qkv[:, key_cols]) * 0.125).astype(bf16)
                qkv[r, cols] = jnp.where(block_lane < 64, qkv[r, cols], result) if upper else result
                return inner_carry

            lax.fori_loop(0, slots // block, attend_back, 0, unroll=4)
            for j in range(slots // 512):
                c = pl.ds(j * 512, 512)
                grad_key_t[part, c] = nn(query_t[part, :], work[:, pl.ds(base + j * 512, 512)]).astype(bf16)

            @pl.when(pair + 1 < pairs)
            def _(upper=upper):
                prob_in(pair + 1, upper).start()

        qkv[:, value_cols] = grad_value_t[...].T
        qkv[:, key_cols] = grad_key_t[...].T
        between_pairs(pair)

    outgoing_pair = key_aug
    between_pairs = at_trips(scatter.sides(UP), scatter.lasts(LOW, HIGH), scatter.lines(GATE))
    pl.loop(0, pairs)(pair_back)

    turn(x)
    g_qv[...] = nn(grad_t[...], qkv[:, pl.ds(0, 2 * heads_wide)]).astype(bf16)
    scatter.begin(QV, 1)
    g_ko[:, pl.ds(0, heads_wide)] = nn(grad_t[...], qkv[:, k_cols]).astype(bf16)
    scatter.begin(KO, 1)
    scatter.begin(QV, 0)
    scatter.begin(KO, 0)
    def column_sum(cols):
        def add(i, carry):
            return carry + fold(qkv[aligned(i * 128, 128), cols].astype(f32))

        return jnp.sum(lax.fori_loop(0, slots // 128, add, jnp.zeros((8, heads_wide), f32)), axis=0, keepdims=True)

    small_grads[6:7, side_cols] = column_sum(q_cols)
    small_grads[7:8, side_cols] = column_sum(v_cols)
    sums = SmallSum(grid, small_grads, small_grads, small_box, small_send, small_recv)
    sums.stage(0)

    def inputs_back(rows_side, sink):
        @pl.loop(0, half // 256)
        def _(i):
            r = aligned(rows_side * half + i * 256, 256)
            sink(
                i,
                nt(qkv[r, pl.ds(0, 2 * heads_wide)], w_qv[...]) + nt(qkv[r, k_cols], w_ko[:, pl.ds(0, heads_wide)]),
            )

    inputs_back(other, to_outgoing)
    fourth_swap = swap(outgoing, incoming.at[1], 7)
    sums.stage(1)
    inputs_back(side, add_attended)
    sums.stage(2)
    Pump(scatter.lines(UP)).run()
    fourth_swap.wait()

    @pl.loop(0, half // step)
    def _(i):
        r = aligned(i * step, step)
        attended[r, :] = attended[r, :] + incoming[1, r, :].astype(f32)

    tokens_copy = pltpu.make_async_copy(attended, grad_tokens, local_sem.at[3])
    tokens_copy.start()
    Pump(scatter.sides(QV, KO)).run()
    sums.stage(3)
    Pump(scatter.lines(QV, KO) + scatter.lasts(GATE, UP) + scatter.lasts(QV, KO)).run()
    sums.stage(4)

    def turn_to(rows_block, start):
        return pltpu.roll(rows_block, (width - start) % width, 1)

    dp = lax.axis_index("dp")
    piece = to_gains.shape[1]
    low_rows, high_rows = small_grads[0:8, :], small_grads[8:16, :]
    norm_part = turn_to(low_rows, (2 * dp + side) * piece)
    to_gains[...] = norm_part[0:2, :piece]
    to_offsets[...] = norm_part[2:6, :piece]
    to_qv_bias[...] = turn_to(low_rows, side * heads_wide + dp * to_qv_bias.shape[1])[6:8, : to_qv_bias.shape[1]]
    unit_piece = to_in_bias.shape[1]
    first_lane = dp * unit_piece
    unit_part = turn_to(high_rows, first_lane % width)
    per_half = units // width
    row = side * per_half + first_lane // width
    for index in range(2):
        chosen = sum(
            jnp.where(row == r, unit_part[2 * per_half * index + r : 2 * per_half * index + r + 1, :], 0.0)
            for r in range(2 * per_half)
        )
        to_in_bias[index : index + 1, :] = chosen[:, :unit_piece]
    tokens_copy.wait()
    gather.drain()
    scatter.drain()


def layer_call(grid, tokens, cotangent, lengths, qkv_part, out_part, in_part, down_part, smalls_in):
    rows, heads_wide = out_part.shape
    wide = 2 * heads_wide
    width = rows * grid.nz * 4
    half = tokens.shape[0]
    slots = 2 * half
    units = in_part.shape[2]
    heads = heads_wide // HEAD
    shapes = [
        jax.ShapeDtypeStruct((half, width), bf16),
        jax.ShapeDtypeStruct((half, width), f32),
        jax.ShapeDtypeStruct((3, rows, heads_wide), f32),
        jax.ShapeDtypeStruct((rows, heads_wide), f32),
        jax.ShapeDtypeStruct(in_part.shape, f32),
        jax.ShapeDtypeStruct((rows, units), f32),
        *(jax.ShapeDtypeStruct(part.shape, f32) for part in smalls_in),
        jax.ShapeDtypeStruct((heads, slots, slots), bf16),
    ]
    vmem = pl.BlockSpec(memory_space=pltpu.VMEM)
    smem = pl.BlockSpec(memory_space=pltpu.SMEM)
    anywhere = pl.BlockSpec(memory_space=pl.ANY)
    smalls = small_slots(grid)
    dma = pltpu.SemaphoreType.DMA
    wides = (wide, wide, units, units, units // 2, units // 2)
    scratch = (
        [pltpu.VMEM((width, w), bf16) for w in wides]
        + [
            pltpu.VMEM((16, 128), f32),
            pltpu.VMEM((16, 256), f32),
            pltpu.VMEM((16 * grid.slots, 256), f32),
            pltpu.VMEM((16, width), f32),
            pltpu.VMEM((smalls, 16, width), f32),
            pltpu.VMEM((16, width), f32),
            pltpu.VMEM((slots, width), bf16),
            pltpu.VMEM((slots, 3 * heads_wide), bf16),
            pltpu.VMEM((slots, 128), f32),
            pltpu.VMEM((slots, heads_wide), bf16),
            pltpu.VMEM((slots, 3 * units), bf16),
            pltpu.VMEM((slots, 128), bf16),
            pltpu.VMEM((slots, 128), bf16),
            pltpu.VMEM((slots, 128), bf16),
            pltpu.VMEM((half, max(2 * slots - 256, 2 * width + 128)), f32),
            pltpu.VMEM((slots, width), bf16),
            pltpu.VMEM((slots, width), bf16),
            pltpu.VMEM((half, width), bf16),
            pltpu.VMEM((2, half, width), bf16),
            pltpu.VMEM((24, units), f32),
            pltpu.VMEM((width, slots), bf16),
            pltpu.VMEM((2, 128, slots), bf16),
            pltpu.VMEM((128, slots), bf16),
            pltpu.VMEM((128, slots), bf16),
        ]
        + [pltpu.VMEM((width, w), bf16) for w in wides]
        + [pltpu.VMEM((scatter_slots(grid), rows, w), bf16) for w in wides]
        + [
            dma((7, grid.slots)),
            dma((7, grid.slots)),
            dma((6, scatter_slots(grid))),
            dma((6, scatter_slots(grid))),
            dma((smalls,)),
            dma((smalls,)),
            dma((8,)),
            dma((9,)),
            dma((9,)),
            dma((5,)),
            dma((2,)),
        ]
    )
    results = pl.pallas_call(
        functools.partial(layer_body, grid, rows),
        out_shape=shapes,
        in_specs=[anywhere, anywhere, smem] + [anywhere] * 4 + [vmem] * 4,
        out_specs=[vmem, anywhere] + [vmem] * 8 + [anywhere],
        scratch_shapes=scratch,
        compiler_params=pltpu.CompilerParams(collective_id=0, has_side_effects=True, vmem_limit_bytes=VMEM_LIMIT),
        name="layer",
    )(tokens, cotangent, lengths, qkv_part, out_part, in_part, down_part, *smalls_in)
    return results[:10]


norm_epsilon = 1e-06


def norm_forward(values, gain_row, shift_row):
    centred = values - jnp.mean(values, axis=-1, keepdims=True)
    variance = jnp.mean(centred * centred, axis=-1, keepdims=True)
    inv_scale = lax.rsqrt(variance + norm_epsilon)
    unit_vals = centred * inv_scale
    return (unit_vals * gain_row + shift_row, unit_vals, inv_scale)


def norm_backward(grad_out, unit_vals, inv_scale, gain_row):
    grad_unit = grad_out * gain_row
    inner_term = (
        grad_unit
        - jnp.mean(grad_unit, axis=-1, keepdims=True)
        - unit_vals * jnp.mean(grad_unit * unit_vals, axis=-1, keepdims=True)
    )
    return (
        inner_term * inv_scale,
        jnp.sum(grad_out * unit_vals, axis=0),
        jnp.sum(grad_out, axis=0),
    )


def score_block(query_block, first_row, key_heads, slopes, key_valid):
    block_size = query_block.shape[0]
    heads_here = slopes.shape[0]
    query_heads = query_block.reshape(block_size, heads_here, HEAD)
    raw_scores = jnp.einsum(
        "qhc,khc->hqk", query_heads, key_heads, preferred_element_type=jnp.float32
    )
    query_pos = first_row + lax.iota(jnp.int32, block_size)
    key_pos = lax.iota(jnp.int32, key_heads.shape[0])
    distance = jnp.abs(query_pos[:, None] - key_pos[None, :]).astype(jnp.float32)
    scores = 0.125 * raw_scores - slopes[:, None, None] * distance[None, :, :]
    return (jnp.where(key_valid[None, None, :], scores, -1e30), query_heads)


def attend(queries, key_rows, value_rows, slopes, key_valid):
    slot_count, width_here = queries.shape
    heads_here = width_here // HEAD
    block_size = min(512, slot_count)
    key_heads = key_rows.reshape(slot_count, heads_here, HEAD)
    value_heads = value_rows.reshape(slot_count, heads_here, HEAD)

    def one_block(first_row):
        query_block = lax.dynamic_slice_in_dim(queries, first_row, block_size, 0)
        scores, query_heads = score_block(query_block, first_row, key_heads, slopes, key_valid)
        row_max = jnp.max(scores, axis=-1, keepdims=True)
        exp_scores = jnp.exp(scores - row_max)
        row_total = jnp.sum(exp_scores, axis=-1, keepdims=True)
        weights = (exp_scores / row_total).astype(jnp.bfloat16)
        mixed_block = jnp.einsum(
            "hqk,khc->qhc", weights, value_heads, preferred_element_type=jnp.float32
        )
        return (
            mixed_block.reshape(block_size, width_here).astype(jnp.bfloat16),
            (row_max + jnp.log(row_total))[..., 0],
        )

    first_rows = lax.iota(jnp.int32, slot_count // block_size) * block_size
    mixed_heads, logsum = lax.map(one_block, first_rows)
    return (mixed_heads.reshape(slot_count, width_here), logsum)


def attend_back(queries, key_rows, value_rows, grad_mixed, logsum, slopes, key_valid):
    slot_count, width_here = queries.shape
    heads_here = width_here // HEAD
    block_size = min(512, slot_count)
    key_heads = key_rows.reshape(slot_count, heads_here, HEAD)
    value_heads = value_rows.reshape(slot_count, heads_here, HEAD)

    def one_block(running, block_item):
        grad_keys, grad_values = running
        first_row, block_lse = block_item
        query_block = lax.dynamic_slice_in_dim(queries, first_row, block_size, 0)
        grad_block = lax.dynamic_slice_in_dim(grad_mixed, first_row, block_size, 0)
        scores, query_heads = score_block(query_block, first_row, key_heads, slopes, key_valid)
        probs = jnp.exp(scores - block_lse[..., None])
        grad_heads = grad_block.reshape(block_size, heads_here, HEAD)
        grad_probs = jnp.einsum(
            "qhc,khc->hqk", grad_heads, value_heads, preferred_element_type=jnp.float32
        )
        row_dot = jnp.sum(probs * grad_probs, axis=-1, keepdims=True)
        grad_scores = (probs * (grad_probs - row_dot)).astype(jnp.bfloat16)
        grad_query = 0.125 * jnp.einsum(
            "hqk,khc->qhc", grad_scores, key_heads, preferred_element_type=jnp.float32
        )
        grad_keys = grad_keys + 0.125 * jnp.einsum(
            "hqk,qhc->khc", grad_scores, query_heads, preferred_element_type=jnp.float32
        )
        grad_values = grad_values + jnp.einsum(
            "hqk,qhc->khc",
            probs.astype(jnp.bfloat16),
            grad_heads,
            preferred_element_type=jnp.float32,
        )
        return ((grad_keys, grad_values), grad_query.reshape(block_size, width_here))

    first_rows = lax.iota(jnp.int32, slot_count // block_size) * block_size
    zero_grads = jnp.zeros((slot_count, heads_here, HEAD), jnp.float32)
    (grad_keys, grad_values), grad_queries = lax.scan(
        one_block, (zero_grads, zero_grads), (first_rows, logsum)
    )
    return (
        grad_queries.reshape(slot_count, width_here),
        grad_keys.reshape(slot_count, width_here),
        grad_values.reshape(slot_count, width_here),
    )


def spread(part, index, count):
    wide = jnp.tile(part, (1, count))
    owner = lax.broadcasted_iota(jnp.int32, wide.shape, 1) // part.shape[1]
    return jnp.where(owner == index, wide.astype(jnp.float32), 0.0)


def pick(whole, index, count):
    size = whole.shape[1] // count
    return lax.dynamic_slice_in_dim(whole, index * size, size, 1)


def pack_small(biases_qv, biases_in, rows_all, piece, pieces):
    width = rows_all.shape[1]
    halves = [b if pieces == 1 else spread(b, piece, pieces) for b in (biases_qv, biases_in)]
    rows = [rows_all] + [h.reshape(-1, width) for h in halves]
    packed = jnp.concatenate(rows, axis=0)
    return jnp.pad(packed, ((0, -packed.shape[0] % 8), (0, 0)))


def unpack_small(packed, width_qv, width_in, piece, pieces):
    width = packed.shape[1]
    count_qv = 2 * width_qv * pieces // width
    count_in = 2 * width_in * pieces // width
    whole_qv = packed[6 : 6 + count_qv].reshape(2, -1)
    whole_in = packed[6 + count_qv : 6 + count_qv + count_in].reshape(2, -1)
    return packed[:6], pick(whole_qv, piece, pieces), pick(whole_in, piece, pieces)


def per_device(
    direct,
    tokens,
    lengths,
    qkv_weight,
    qv_bias,
    out_weight,
    in_weight,
    in_bias,
    down_weight,
    norm_gains,
    offsets,
    cotangent,
):
    row_count = tokens.shape[0]
    dp = lax.axis_size("dp")
    pieces = lax.axis_size("tensor")
    piece_index = lax.axis_index("tensor")
    dp_index = lax.axis_index("dp")
    flat_index = dp_index * pieces + piece_index
    grid = Grid3(dp)
    if direct:
        output, grad_tokens, to_qkv, to_out, to_in, to_down, to_gains, to_offsets, to_qv_bias, to_in_bias = layer_call(
            grid,
            tokens,
            cotangent,
            lengths,
            qkv_weight,
            out_weight.T,
            in_weight,
            down_weight.T,
            (norm_gains, offsets, qv_bias, in_bias),
        )
        return output, grad_tokens, to_qkv, to_qv_bias, to_out.T, to_in, to_in_bias, to_down.T, to_gains, to_offsets
    slot_count = row_count * pieces
    length = lengths[0]
    heads_here = qkv_weight.shape[2] // HEAD
    head_ids = (piece_index * heads_here + lax.iota(jnp.int32, heads_here)).astype(jnp.float32)
    slopes = jnp.exp2(-8.0 * (head_ids + 1.0) / (heads_here * pieces))
    key_valid = lax.iota(jnp.int32, slot_count) < length
    row_valid = (piece_index * row_count + lax.iota(jnp.int32, row_count) < length).astype(
        jnp.float32
    )[:, None]

    width_qv, width_in = qkv_weight.shape[2], in_weight.shape[2]
    parts = (qkv_weight, out_weight.T, in_weight, down_weight.T)
    small = pack_small(
        spread(qv_bias, dp_index, dp),
        spread(in_bias, dp_index, dp),
        jnp.concatenate([spread(norm_gains, flat_index, dp * pieces), spread(offsets, flat_index, dp * pieces)]),
        piece_index,
        pieces,
    )
    whole_qkv, whole_out_t, whole_in, whole_down_t = (
        lax.all_gather(p, "dp", axis=p.ndim - 2, tiled=True) for p in parts
    )
    small = lax.psum(small, ("dp", "tensor"))
    rows_all, whole_bqv, whole_bin = unpack_small(small, width_qv, width_in, piece_index, pieces)
    gains, shift_rows = rows_all[:2], rows_all[2:6]

    gathered = lax.all_gather(tokens, "tensor", axis=0, tiled=True)
    projected = jnp.einsum("sd,kdc->ksc", gathered, whole_qkv, preferred_element_type=jnp.float32)
    queries = (projected[0] + whole_bqv[0]).astype(jnp.bfloat16)
    key_rows = projected[1].astype(jnp.bfloat16)
    value_rows = (projected[2] + whole_bqv[1]).astype(jnp.bfloat16)
    mixed_heads, logsum = attend(queries, key_rows, value_rows, slopes, key_valid)
    attn_part = jnp.einsum("sc,dc->sd", mixed_heads, whole_out_t, preferred_element_type=jnp.float32)
    attn_total = lax.psum_scatter(
        attn_part.astype(jnp.bfloat16), "tensor", scatter_dimension=0, tiled=True
    ).astype(jnp.float32)
    first_in = tokens.astype(jnp.float32) + attn_total + shift_rows[0]
    attended, unit_one, scale_one = norm_forward(first_in, gains[0], shift_rows[1])
    attended_low = attended.astype(jnp.bfloat16)
    gathered_ff = lax.all_gather(attended_low, "tensor", axis=0, tiled=True)
    pre_acts = jnp.einsum("sd,kdc->ksc", gathered_ff, whole_in, preferred_element_type=jnp.float32)
    pre_acts = pre_acts + whole_bin[:, None, :]
    hidden = (jax.nn.gelu(pre_acts[0], approximate=False) * pre_acts[1]).astype(jnp.bfloat16)
    ff_part = jnp.einsum("sf,df->sd", hidden, whole_down_t, preferred_element_type=jnp.float32)
    ff_total = lax.psum_scatter(
        ff_part.astype(jnp.bfloat16), "tensor", scatter_dimension=0, tiled=True
    ).astype(jnp.float32)
    second_in = attended + ff_total + shift_rows[2]
    final_norm, unit_two, scale_two = norm_forward(second_in, gains[1], shift_rows[3])
    output = (final_norm * row_valid).astype(jnp.bfloat16)
    grad_final = cotangent.astype(jnp.float32) * row_valid
    grad_second, grad_gain_two, grad_shift_two = norm_backward(
        grad_final, unit_two, scale_two, gains[1]
    )
    grad_bdown = jnp.sum(grad_second, axis=0)
    grad_ff_rows = lax.all_gather(grad_second.astype(jnp.bfloat16), "tensor", axis=0, tiled=True)
    grad_down_t = jnp.einsum("sd,sf->df", grad_ff_rows, hidden, preferred_element_type=jnp.float32)
    grad_hidden = jnp.einsum("sd,df->sf", grad_ff_rows, whole_down_t, preferred_element_type=jnp.float32)
    pullback = jax.vjp(
        lambda gate_pre, up_pre: jax.nn.gelu(gate_pre, approximate=False) * up_pre,
        pre_acts[0],
        pre_acts[1],
    )[1]
    grad_gate, grad_up = pullback(grad_hidden)
    grad_pre = jnp.stack([grad_gate, grad_up]).astype(jnp.bfloat16)
    grad_bin = jnp.sum(grad_pre, axis=1, dtype=jnp.float32)
    grad_in = jnp.einsum("sd,ksc->kdc", gathered_ff, grad_pre, preferred_element_type=jnp.float32)
    ff_back = jnp.einsum("ksc,kdc->sd", grad_pre, whole_in, preferred_element_type=jnp.float32)
    grad_attended = grad_second + lax.psum_scatter(
        ff_back.astype(jnp.bfloat16), "tensor", scatter_dimension=0, tiled=True
    ).astype(jnp.float32)
    grad_first, grad_gain_one, grad_shift_one = norm_backward(
        grad_attended, unit_one, scale_one, gains[0]
    )
    grad_bout = jnp.sum(grad_first, axis=0)
    grad_attn_rows = lax.all_gather(grad_first.astype(jnp.bfloat16), "tensor", axis=0, tiled=True)
    grad_out_t = jnp.einsum("sd,sc->dc", grad_attn_rows, mixed_heads, preferred_element_type=jnp.float32)
    grad_mixed = jnp.einsum(
        "sd,dc->sc", grad_attn_rows, whole_out_t, preferred_element_type=jnp.float32
    ).astype(jnp.bfloat16)
    grad_queries, grad_keys, grad_values = attend_back(
        queries, key_rows, value_rows, grad_mixed, logsum, slopes, key_valid
    )
    grad_qkv = jnp.stack([grad_queries, grad_keys, grad_values]).astype(jnp.bfloat16)
    grad_wqkv = jnp.einsum("sd,ksc->kdc", gathered, grad_qkv, preferred_element_type=jnp.float32)
    grad_bqv = jnp.stack(
        [
            jnp.sum(grad_qkv[0], axis=0, dtype=jnp.float32),
            jnp.sum(grad_qkv[2], axis=0, dtype=jnp.float32),
        ]
    )
    input_back = jnp.einsum("ksc,kdc->sd", grad_qkv, whole_qkv, preferred_element_type=jnp.float32)
    grad_tokens = grad_first + lax.psum_scatter(
        input_back.astype(jnp.bfloat16), "tensor", scatter_dimension=0, tiled=True
    ).astype(jnp.float32)

    small_grads = pack_small(
        grad_bqv,
        grad_bin,
        jnp.stack([grad_gain_one, grad_gain_two, grad_bout, grad_shift_one, grad_bdown, grad_shift_two]),
        piece_index,
        pieces,
    )
    grads = tuple(g.astype(jnp.bfloat16) for g in (grad_wqkv, grad_out_t, grad_in, grad_down_t))
    shard_wqkv, shard_out_t, shard_in, shard_down_t = (
        lax.psum_scatter(g.astype(jnp.float32), "dp", scatter_dimension=g.ndim - 2, tiled=True) for g in grads
    )
    small_grads = lax.psum(small_grads, ("dp", "tensor"))
    row_grads, bqv_grads, bin_grads = unpack_small(small_grads, width_qv, width_in, piece_index, pieces)
    own_rows = pick(row_grads, flat_index, dp * pieces)
    return (
        output,
        grad_tokens,
        shard_wqkv,
        pick(bqv_grads, dp_index, dp),
        shard_out_t.T,
        shard_in,
        pick(bin_grads, dp_index, dp),
        shard_down_t.T,
        own_rows[:2],
        own_rows[2:],
    )


def solution(mesh):
    placed = (
        P(("dp", "tensor"), None),
        P("dp"),
        P(None, "dp", "tensor"),
        P(None, ("tensor", "dp")),
        P("tensor", "dp"),
        P(None, "dp", "tensor"),
        P(None, ("tensor", "dp")),
        P("tensor", "dp"),
        P(None, ("dp", "tensor")),
        P(None, ("dp", "tensor")),
        P(("dp", "tensor"), None),
    )

    def run(*args):
        dp = mesh.shape["dp"]
        direct = dp % 4 == 0 and (args[2].shape[1] // dp) % 16 == 0 and mesh.shape["tensor"] == 2
        return jax.shard_map(
            functools.partial(per_device, direct),
            mesh=mesh,
            in_specs=placed,
            out_specs=(
                P(("dp", "tensor"), None),
                P(("dp", "tensor"), None),
                P(None, "dp", "tensor"),
                P(None, ("tensor", "dp")),
                P("tensor", "dp"),
                P(None, "dp", "tensor"),
                P(None, ("tensor", "dp")),
                P("tensor", "dp"),
                P(None, ("dp", "tensor")),
                P(None, ("dp", "tensor")),
            ),
            check_vma=False,
        )(*args)

    return run
```
